128 devices in a mesh: member: 4 (over z_lo, core), space: 32 (over y, z_hi, x).
Axes of the slice: x: 4, y: 4, z: 4 (z_hi: 2, z_lo: 2; z = z_hi * 2 + z_lo), core: 2. Of those that a mesh axis runs over, the one named last changes fastest.
Arguments:
- members: bfloat16 [64, 32, 512, 384], P('member', None, 'space'), may hold values from -6 to 6
- control: float32 [32, 512, 384], P(None, 'space'), may hold values from -6 to 6
- hybrid_weight: float32 [32], replicated, may hold values from 0.2 to 0.6
- member_weights: int32 [64], replicated, may hold values from 1 to 8
- source_device: int32 [512, 1], P('space'), may hold values from 0 to 31, as said below
- source_row: int32 [512], P('space'), may hold values from 0 to 15
- column_source: int32 [512, 768], P('space'), may hold values from 0 to 382, as said below
- column_code: int32 [512, 768], P('space'), may hold values from 0 to 16
Outputs:
- fine_increment: float32 [512, 32, 2, 768], P('space', 'member')
The draws below stay inside these ranges and needn't reach their ends.
Inputs may be any that keep to these rules, and one draw needn't show every extreme that they name: `source_device`: among the 16 fine blocks of one device no space index is named more than 2 times, and in every draw some device's blocks name some index exactly 2 times. `column_source`: within 2 of (j - 1) // 2 for fine column j, clipped to the range.
All inputs are finite; a program needn't handle non-finite values.
Results may differ from the reference program's by a relative error of at most 0.0022.
Values sent between devices are 32-bit elements; how exact they have to be, the bound alone decides.
No kernel may reach another device: no remote copies, remote signals or barrier semaphores. Data moves between devices by JAX's collectives and lax.ppermute only.
A program may use at most 128 MiB of HBM per device.

```python
import math
import jax
import jax.numpy as jnp
from jax import lax

NX = 384
FX = 768
SWEEPS = 4
ROWS_DEV = 16
C = 32
MEMBERS = 64
NY = 512
CAP = 2
N_SPACE = 32


def block_owners(key):
    order = jax.random.permutation(jax.random.fold_in(key, 7), N_SPACE).astype(jnp.int32)
    blocks = jnp.arange(NY, dtype=jnp.int32)
    return jnp.take(order, blocks // CAP % N_SPACE).astype(jnp.int32)


def draw_source_device(key, part):
    return block_owners(key)[:, None].astype(jnp.int32)


def draw_source_row(key, part):
    blocks = jnp.arange(NY, dtype=jnp.int32)
    random_rows = jax.random.randint(jax.random.fold_in(key, 11), (NY,), 0, ROWS_DEV, dtype=jnp.int32)
    leading = blocks % CAP == 0
    return jnp.where(leading, ROWS_DEV - 1, random_rows).astype(jnp.int32)


def draw_column_source(key, part):
    columns = jnp.arange(FX, dtype=jnp.int32)
    centre = (columns - 1) // 2
    jitter = jax.random.randint(key, (NY, FX), -2, 3, dtype=jnp.int32)
    return jnp.clip(centre[None, :] + jitter, 0, NX - 2).astype(jnp.int32)


def draw_members(key, part):
    rows = jnp.arange(NY, dtype=jnp.float32)[:, None]
    phase = rows * (2.0 * math.pi / 64.0)
    small_shape = (MEMBERS, C, 1, NX)
    full_shape = (MEMBERS, C, NY, NX)
    first = jax.random.normal(jax.random.fold_in(key, 21), small_shape, jnp.float32)
    second = jax.random.normal(jax.random.fold_in(key, 22), small_shape, jnp.float32)
    noise = 0.45 * jax.random.normal(jax.random.fold_in(key, 23), full_shape, jnp.float32)
    common = first * jnp.cos(phase) + second * jnp.sin(phase)
    return jnp.clip(common + noise, -6.0, 6.0).astype(jnp.bfloat16)


def draw_control(key, part):
    local = jnp.arange(NY, dtype=jnp.int32) % ROWS_DEV
    depth = jnp.minimum(local, ROWS_DEV - 1 - local)
    far_rows = ((depth == 2) | (depth == 3))[None, :, None]
    shape = (C, NY, NX)
    signs = jnp.where(jax.random.bernoulli(jax.random.fold_in(key, 31), 0.5, shape), 1.0, -1.0)
    base = jnp.clip(jax.random.normal(jax.random.fold_in(key, 32), shape, jnp.float32), -4.0, 4.0)
    magnitude = jax.random.uniform(jax.random.fold_in(key, 33), shape, jnp.float32, 3.0, 6.0)
    return jnp.where(far_rows, signs * magnitude, base)


def with_ends(drawn, rng, low, high):
    index_at = [jax.random.randint(jax.random.fold_in(rng, axis), (), 0, length) for axis, length in enumerate(drawn.shape)]
    main_axis = drawn.shape.index(max(drawn.shape))
    beside = index_at[:main_axis] + [(index_at[main_axis] + 1) % drawn.shape[main_axis]] + index_at[main_axis + 1:]
    return drawn.at[tuple(index_at)].set(low).at[tuple(beside)].set(high)


def setup_inputs(seed: int = 0) -> dict:
    keys = jax.random.split(jax.random.key(seed), 9)
    return {
        "members": draw_members(jax.random.fold_in(keys[8], 71), 0),
        "control": draw_control(jax.random.fold_in(keys[8], 71), 0),
        "hybrid_weight": jnp.clip(jax.random.uniform(keys[2], (C,), jnp.float32, 0.2, 0.6), 0.2, 0.6),
        "member_weights": with_ends(jax.random.randint(keys[3], (MEMBERS,), 1, 9), jax.random.fold_in(keys[3], 1), 1, 8).astype(jnp.int32),
        "source_device": draw_source_device(jax.random.fold_in(keys[8], 71), 0),
        "source_row": draw_source_row(jax.random.fold_in(keys[8], 71), 0),
        "column_source": draw_column_source(jax.random.fold_in(keys[8], 71), 0),
        "column_code": with_ends(jax.random.randint(keys[7], (NY, FX), 0, 17), jax.random.fold_in(keys[7], 1), 0, 16).astype(jnp.int32),
    }


DIFFUSE = 0.2


def sweep_field(field):
    widths = [(0, 0)] * (field.ndim - 2) + [(1, 1), (1, 1)]
    padded = jnp.pad(field, widths)
    laplace = padded[..., 2:, 1:-1] + padded[..., :-2, 1:-1] + padded[..., 1:-1, 2:] + padded[..., 1:-1, :-2] - 4.0 * field
    return field + DIFFUSE * laplace


def localize(field):
    for repeat in range(SWEEPS):
        field = sweep_field(field)
    return field


def reference(members, control, hybrid_weight, member_weights, source_device, source_row, column_source, column_code):
    weight_codes = member_weights.astype(jnp.float32)
    member_share = weight_codes / jnp.sum(weight_codes)

    def add_member(total, item):
        member, weight = item
        states = member.astype(jnp.float32)
        smooth = localize(states * control)
        return total + weight * (states * smooth), None

    ensemble, unused = lax.scan(add_member, jnp.zeros(control.shape, jnp.float32), (members, member_share))
    static = localize(control)
    blend = hybrid_weight[:, None, None]
    increment = (1.0 - blend) * ensemble + blend * static
    extended = jnp.concatenate([increment, jnp.zeros((control.shape[0], 1, control.shape[2]), jnp.float32)], axis=1)
    global_rows = (source_device[:, 0] * ROWS_DEV + source_row).astype(jnp.int32)
    lower = jnp.take(extended, global_rows, axis=1)
    upper = jnp.take(extended, (global_rows + 1).astype(jnp.int32), axis=1)
    fine_rows = jnp.stack([0.75 * lower + 0.25 * upper, 0.25 * lower + 0.75 * upper], axis=2)
    full_shape = (fine_rows.shape[0], fine_rows.shape[1], 2, column_source.shape[1])
    left_index = jnp.broadcast_to(column_source[None, :, None, :], full_shape).astype(jnp.int32)
    right_index = (left_index + 1).astype(jnp.int32)
    left_value = jnp.take_along_axis(fine_rows, left_index, axis=3)
    right_value = jnp.take_along_axis(fine_rows, right_index, axis=3)
    right_weight = (column_code.astype(jnp.float32) / 16.0)[None, :, None, :]
    fine = (1.0 - right_weight) * left_value + right_weight * right_value
    return jnp.transpose(fine, (1, 0, 2, 3))
```

```python
import jax
import jax.numpy as jnp
from jax import lax
from jax.experimental import pallas as pl
from jax.experimental.pallas import tpu as pltpu
from jax.sharding import PartitionSpec as P

SCALE = 1.0 / 625.0
LANES = 128


def passed_along(x, axis, by):
    length = lax.axis_size(axis)
    pairs = [(i, i + by) for i in range(length) if 0 <= i + by < length]
    return lax.ppermute(x, axis, pairs)


def swapped(x, axis, bit):
    length = lax.axis_size(axis)
    return lax.ppermute(x, axis, [(i, i ^ bit) for i in range(length)])


def split_lanes(x):
    return [x[:, i : i + LANES] for i in range(0, x.shape[-1], LANES)]


def joined(parts):
    return jnp.concatenate(parts, axis=-1)


def side_sum(parts, lane):
    ahead = [pltpu.roll(p, 1, 1) for p in parts]
    behind = [pltpu.roll(p, LANES - 1, 1) for p in parts]
    out = []
    for i in range(len(parts)):
        left = jnp.where(lane == 0, ahead[i - 1] if i else 0.0, ahead[i])
        right = jnp.where(
            lane == LANES - 1, behind[i + 1] if i + 1 < len(parts) else 0.0, behind[i]
        )
        out.append(left + right)
    return out


def plus(a, b):
    return [p + q for p, q in zip(a, b)]


def times(a, b):
    return [p * q for p, q in zip(a, b)]


def scaled(factor, a):
    return [factor * p for p in a]


def widen(parts, lane):
    return plus(parts, side_sum(parts, lane))


def edges_kernel(members_ref, control_ref, top_ref, bottom_ref, scratch):
    step = pl.program_id(0)
    group = members_ref.shape[0]
    chans, rows = members_ref.shape[1:3]

    def rows_out(index):
        for slot in range(2):
            for which, ref in ((slot, top_ref), (rows - 2 + slot, bottom_ref)):
                for part in range(scratch.shape[0]):
                    ref[index, slot, :, part * LANES : (part + 1) * LANES] = scratch[
                        part, pl.ds(which, chans, stride=rows), :
                    ]

    for one in range(group):
        wide = members_ref[one].astype(jnp.float32).reshape(chans * rows, -1)
        for part in range(scratch.shape[0]):
            scratch[part] = wide[:, part * LANES : (part + 1) * LANES]
        rows_out(step * group + one)

    @pl.when(step == pl.num_programs(0) - 1)
    def _():
        wide = control_ref[...].reshape(chans * rows, -1)
        for part in range(scratch.shape[0]):
            scratch[part] = wide[:, part * LANES : (part + 1) * LANES]
        rows_out(pl.num_programs(0) * group)


def edge_rows(members, control, group):
    count, chans, rows, width = members.shape
    shape = (count + 1, 2, chans, width)
    out = jax.ShapeDtypeStruct(shape, jnp.float32)
    return pl.pallas_call(
        edges_kernel,
        grid=(count // group,),
        in_specs=[
            pl.BlockSpec((group, chans, rows, width), lambda i: (i, 0, 0, 0)),
            pl.BlockSpec((chans, rows, width), lambda i: (0, 0, 0)),
        ],
        out_specs=[pl.BlockSpec(shape, lambda i: (0, 0, 0, 0))] * 2,
        out_shape=[out, out],
        scratch_shapes=[pltpu.VMEM((width // LANES, chans * rows, LANES), jnp.float32)],
        name="edge_rows",
    )(members, control)


def own_kernel(
    place_ref, share_ref, members_ref, control_ref, blend_ref, partial_ref, near_ref, scratch, turned
):
    step = pl.program_id(0)
    chans, rows = members_ref.shape[1:3]
    parts = scratch.shape[0]
    lane = lax.broadcasted_iota(jnp.int32, (8, LANES), 1)
    slot_own = place_ref[0]
    keep_low = (place_ref[1] != 0).astype(jnp.float32)
    keep_high = (place_ref[2] != 0).astype(jnp.float32)
    last = pl.num_programs(0) - 1

    def turned_in(wide):
        for part in range(parts):
            scratch[part] = wide[:, part * LANES : (part + 1) * LANES]

    def row_of(group, row):
        return [scratch[part, pl.ds(group * (8 * rows) + row, 8, stride=rows), :] for part in range(parts)]

    @pl.when(step == 0)
    def _():
        turned_in(control_ref[...].reshape(chans * rows, -1))

        def fill(group, carry):
            for row in range(rows):
                for part, value in enumerate(row_of(group, row)):
                    turned[part, row, pl.ds(group * 8, 8), :] = value
            return carry

        lax.fori_loop(0, chans // 8, fill, 0)

    def localized(source):
        total = {0: {}, 1: {}, 2: {}, 3: {}, 4: {}}
        reach = {0: 0, 1: 1, 2: 2, 3: 1, 4: 0}

        def at(level, row):
            return total[level].get(row)

        def advance(level, row):
            if not -reach[level] <= row < rows + reach[level]:
                return
            near = [at(level - 1, row - 1), at(level - 1, row + 1)]
            middle = at(level - 1, row)
            if middle is not None:
                near.append(widen(middle, lane))
            near = [n for n in near if n is not None]
            value = near[0]
            for other in near[1:]:
                value = plus(value, other)
            if row < 0:
                value = scaled(keep_low, value)
            if row >= rows:
                value = scaled(keep_high, value)
            total[level][row] = value

        for row in range(-2, rows + 8):
            if 0 <= row < rows:
                total[0][row] = source(row)
            for level in (1, 2, 3, 4):
                advance(level, row - level)
            done = row - 4
            if 0 <= done < rows:
                yield done, total[4][done]
            for level in range(4):
                total[level].pop(row - level - 3, None)

    @pl.when(step < last)
    def _():
        turned_in(members_ref[0].astype(jnp.float32).reshape(chans * rows, -1))
        share = share_ref[jnp.minimum(step, last - 1)]

        def one_group(group, carry):
            def source(row):
                state = row_of(group, row)
                return times(
                    state, [turned[part, row, pl.ds(group * 8, 8), :] for part in range(parts)]
                )

            slot = jnp.bitwise_xor(group, slot_own)
            for row, value in localized(source):
                state = row_of(group, row)
                for part in range(parts):
                    lanes = slice(part * LANES, (part + 1) * LANES)
                    term = share * (state[part] * value[part])
                    before = jnp.where(step == 0, 0.0, partial_ref[slot, row, :, lanes])
                    partial_ref[slot, row, :, lanes] = before + term
            return carry

        lax.fori_loop(0, chans // 8, one_group, 0)
        for place, row in enumerate((0, 1, 2, 3, rows - 4, rows - 3, rows - 2, rows - 1)):
            for part in range(parts):
                near_ref[0, place, :, part * LANES : (part + 1) * LANES] = scratch[
                    part, pl.ds(row, chans, stride=rows), :
                ].astype(jnp.bfloat16)

    @pl.when(step == last)
    def _():
        def one_group(group, carry):
            def source(row):
                return [turned[part, row, pl.ds(group * 8, 8), :] for part in range(parts)]

            slot = jnp.bitwise_xor(group, slot_own)
            blend = blend_ref[pl.ds(group * 8, 8), :]
            for row, value in localized(source):
                for part in range(parts):
                    lanes = slice(part * LANES, (part + 1) * LANES)
                    before = partial_ref[slot, row, :, lanes]
                    partial_ref[slot, row, :, lanes] = (
                        ((1.0 - blend) * before) + (0.25 * blend) * value[part]
                    ) * SCALE
            return carry

        lax.fori_loop(0, chans // 8, one_group, 0)


def own_part(place, share, members, control, blend):
    count, chans, rows, width = members.shape
    parts = width // LANES
    return pl.pallas_call(
        own_kernel,
        grid=(count + 1,),
        in_specs=[
            pl.BlockSpec(memory_space=pltpu.SMEM),
            pl.BlockSpec(memory_space=pltpu.SMEM),
            pl.BlockSpec(
                (1, chans, rows, width), lambda i: (jnp.minimum(i, count - 1), 0, 0, 0)
            ),
            pl.BlockSpec((chans, rows, width), lambda i: (0, 0, 0)),
            pl.BlockSpec((chans, LANES), lambda i: (0, 0)),
        ],
        out_specs=[
            pl.BlockSpec((chans // 8, rows, 8, width), lambda i: (0, 0, 0, 0)),
            pl.BlockSpec(
                (1, 8, chans, width), lambda i: (jnp.minimum(i, count - 1), 0, 0, 0)
            ),
        ],
        out_shape=[
            jax.ShapeDtypeStruct((chans // 8, rows, 8, width), jnp.float32),
            jax.ShapeDtypeStruct((count, 8, chans, width), jnp.bfloat16),
        ],
        scratch_shapes=[
            pltpu.VMEM((parts, chans * rows, LANES), jnp.float32),
            pltpu.VMEM((parts, rows, chans, LANES), jnp.float32),
        ],
        name="own_part",
    )(place, share, members, control, blend)


def cross_kernel(
    place_ref,
    share_ref,
    low_ref,
    low_control_ref,
    high_ref,
    high_control_ref,
    near_ref,
    control_ref,
    blend_ref,
    out_ref,
    sums,
):
    step = pl.program_id(0)
    group = near_ref.shape[0]
    chans, width = near_ref.shape[2:]
    lane = lax.broadcasted_iota(jnp.int32, (8, LANES), 1)
    slot_own = place_ref[0]
    final = step == pl.num_programs(0) - 1
    sides = (
        (low_ref, low_control_ref, (1, 0), (0, 1, 2, 3)),
        (high_ref, high_control_ref, (0, 1), (7, 6, 5, 4)),
    )

    def terms(y1, y2, y3, y4):
        wide = widen(y1, lane)
        inner = plus(widen(plus(scaled(4.0, wide), scaled(6.0, y2)), lane), scaled(12.0, y1))
        first = plus(widen(inner, lane), scaled(4.0, y2))
        second = plus(
            widen(plus(scaled(6.0, wide), scaled(4.0, y2)), lane), scaled(4.0, y1)
        )
        third = plus(scaled(4.0, wide), y2)
        back_first = plus(scaled(4.0, widen(y3, lane)), y4)
        return first, second, third, y1, back_first, y3

    def per_chans(eight, carry):
        at = pl.ds(pl.multiple_of(eight * 8, 8), 8)
        slot = jnp.bitwise_xor(eight, slot_own)
        blend = blend_ref[at, :]
        for side, (halo, halo_control, order, own) in enumerate(sides):
            c1 = split_lanes(halo_control[0, order[0], at, :])
            c2 = split_lanes(halo_control[0, order[1], at, :])
            c3 = split_lanes(control_ref[own[2], at, :])
            c4 = split_lanes(control_ref[own[3], at, :])
            totals = [None] * 6
            for one in range(group):
                share = share_ref[step * group + one]
                b1 = split_lanes(halo[one, order[0], at, :])
                b2 = split_lanes(halo[one, order[1], at, :])
                a = [
                    split_lanes(near_ref[one, row, at, :].astype(jnp.float32)) for row in own
                ]
                found = terms(times(b1, c1), times(b2, c2), times(a[2], c3), times(a[3], c4))
                for i, (factor, value) in enumerate(zip(a + [b1, b2], found)):
                    term = times(scaled(share, factor), value)
                    totals[i] = term if totals[i] is None else plus(totals[i], term)
            places = [side * 6 + i for i in range(6)]
            for place, total in zip(places, totals):
                total = joined(total)
                before = jnp.where(step == 0, 0.0, sums[place, at, :])
                sums[place, at, :] = before + total

            @pl.when(final)
            def _():
                found = terms(c1, c2, c3, c4)
                mix = jnp.concatenate([blend] * (width // LANES), axis=-1)
                for place, value in zip(places, found):
                    out_ref[slot, place] = SCALE * (
                        (1.0 - mix) * sums[place, at, :] + (0.25 * mix) * joined(value)
                    )

        return carry

    lax.fori_loop(0, chans // 8, per_chans, 0)


def cross_part(place, share, low, high, near, control_near, blend, group):
    count, rows, chans, width = near.shape
    halo = pl.BlockSpec((group, 2, chans, width), lambda i: (i, 0, 0, 0))
    halo_control = pl.BlockSpec((1, 2, chans, width), lambda i: (count, 0, 0, 0))
    return pl.pallas_call(
        cross_kernel,
        grid=(count // group,),
        in_specs=[
            pl.BlockSpec(memory_space=pltpu.SMEM),
            pl.BlockSpec(memory_space=pltpu.SMEM),
            halo,
            halo_control,
            halo,
            halo_control,
            pl.BlockSpec((group, rows, chans, width), lambda i: (i, 0, 0, 0)),
            pl.BlockSpec((rows, chans, width), lambda i: (0, 0, 0)),
            pl.BlockSpec((chans, LANES), lambda i: (0, 0)),
        ],
        out_specs=pl.BlockSpec((chans // 8, 12, 8, width), lambda i: (0, 0, 0, 0)),
        out_shape=jax.ShapeDtypeStruct((chans // 8, 12, 8, width), jnp.float32),
        scratch_shapes=[pltpu.VMEM((12, chans, width), jnp.float32)],
        name="cross_part",
    )(place, share, low, low, high, high, near, control_near, blend)


def answer_kernel(place_ref, asked_ref, own_ref, cross_ref, below_ref, above_ref, out_ref, rows_ref):
    rows = own_ref.shape[0]
    keep_high = (place_ref[2] != 0).astype(jnp.float32)
    rows_ref[0:rows] = own_ref[...]
    for i in range(4):
        rows_ref[i] += cross_ref[i]
        rows_ref[rows - 1 - i] += cross_ref[6 + i]
    for i in range(2):
        rows_ref[i] += below_ref[i]
        rows_ref[rows - 1 - i] += above_ref[i]
    rows_ref[rows] = keep_high * (above_ref[2] + cross_ref[10])

    def one(index, carry):
        row = asked_ref[index]
        out_ref[index, 0] = rows_ref[row]
        out_ref[index, 1] = rows_ref[row + 1]
        return carry

    lax.fori_loop(0, asked_ref.shape[0], one, 0, unroll=4)


def answers(place, asked, own, cross, below, above):
    rows, chans, width = own.shape
    slots = asked.shape[0]
    smem = pl.BlockSpec(memory_space=pltpu.SMEM)
    vmem = pl.BlockSpec(memory_space=pltpu.VMEM)
    return pl.pallas_call(
        answer_kernel,
        in_specs=[smem, smem, vmem, vmem, vmem, vmem],
        out_specs=vmem,
        out_shape=jax.ShapeDtypeStruct((slots, 2, chans, width), jnp.float32),
        scratch_shapes=[pltpu.VMEM((rows + 1, chans, width), jnp.float32)],
        name="answers",
    )(place, asked, own, cross, below, above)


def fine_kernel(slot_ref, arrived_ref, source_ref, code_ref, out_ref):
    blocks = source_ref.shape[0]
    chans, width = arrived_ref.shape[2:]
    fine = source_ref.shape[1]
    half = LANES // 2
    lane = lax.broadcasted_iota(jnp.int32, (chans, LANES), 1)

    def window(parts, first):
        part, shift = divmod(first, LANES)
        if shift == 0:
            return parts[part]
        zero = jnp.zeros_like(parts[0])
        left = parts[part] if part >= 0 else zero
        right = parts[part + 1] if part + 1 < len(parts) else zero
        return jnp.where(
            lane < LANES - shift,
            pltpu.roll(left, LANES - shift, 1),
            pltpu.roll(right, LANES - shift, 1),
        )

    def eight(group, carry):
        at = pl.ds(pl.multiple_of(group * 8, 8), 8)
        for inner in range(8):
            block = group * 8 + inner
            slot = slot_ref[block]
            lower = arrived_ref[slot, 0]
            upper = arrived_ref[slot, 1]
            pair = [
                split_lanes(0.75 * lower + 0.25 * upper),
                split_lanes(0.25 * lower + 0.75 * upper),
            ]
            for chunk in range(fine // LANES):
                lanes = slice(chunk * LANES, (chunk + 1) * LANES)
                first = chunk * half - half // 2
                index = source_ref[at, lanes][inner : inner + 1] - first
                weight = code_ref[at, lanes][inner : inner + 1].astype(jnp.float32) * (1.0 / 16.0)
                index = jnp.broadcast_to(index, (chans, LANES))
                weight = jnp.broadcast_to(weight, (chans, LANES))
                for t in range(2):
                    near = window(pair[t], first)
                    left = jnp.take_along_axis(near, index, axis=1)
                    right = jnp.take_along_axis(near, index + 1, axis=1)
                    out_ref[block, :, t, lanes] = (1.0 - weight) * left + weight * right
        return carry

    lax.fori_loop(0, blocks // 8, eight, 0)


def fine_part(slot, arrived, source, code):
    blocks, fine = source.shape
    chans = arrived.shape[2]
    smem = pl.BlockSpec(memory_space=pltpu.SMEM)
    vmem = pl.BlockSpec(memory_space=pltpu.VMEM)
    return pl.pallas_call(
        fine_kernel,
        in_specs=[smem, vmem, vmem, vmem],
        out_specs=vmem,
        out_shape=jax.ShapeDtypeStruct((blocks, chans, 2, fine), jnp.float32),
        name="fine_part",
    )(slot, arrived, source, code)


def reduced(partial):
    got = swapped(jnp.stack([partial[1], partial[3]]), "member", 1)
    mine = partial[0] + got[0]
    other = partial[2] + got[1]
    return mine + swapped(other, "member", 2)


def per_device(
    members,
    control,
    hybrid_weight,
    member_weights,
    source_device,
    source_row,
    column_source,
    column_code,
):
    member_count, chans, row_count, width = members.shape
    spaces = lax.axis_size("space")
    space_index = lax.axis_index("space")
    member_slot = lax.axis_index("member")

    top, bottom = edge_rows(members, control, 4)
    high = passed_along(top, "space", -1)
    low = passed_along(bottom, "space", 1)

    place = jnp.stack(
        [
            member_slot,
            (space_index > 0).astype(jnp.int32),
            (space_index < spaces - 1).astype(jnp.int32),
        ]
    ).astype(jnp.int32)
    weight_codes = member_weights.astype(jnp.float32)
    share = lax.dynamic_slice_in_dim(
        weight_codes, member_slot * member_count, member_count
    ) / jnp.sum(weight_codes)
    blend = jnp.broadcast_to(hybrid_weight[:, None], (chans, LANES))
    partial, near = own_part(place, share, members, control, blend)
    own = reduced(partial)

    control_near = jnp.moveaxis(
        jnp.concatenate([control[:, :4], control[:, row_count - 4 :]], axis=1), 1, 0
    )

    source_index = source_device[:, 0]
    capacity = max(2, 2 * row_count // spaces)
    chosen = (source_index[:, None] == jnp.arange(spaces, dtype=jnp.int32)[None, :]).astype(
        jnp.int32
    )
    earlier = jnp.cumsum(chosen, axis=0) - chosen
    rank_within = jnp.sum(earlier * chosen, axis=1)
    slot_index = source_index * capacity + rank_within
    matches = slot_index[None, :] == jnp.arange(spaces * capacity, dtype=jnp.int32)[:, None]
    request = jnp.sum(jnp.where(matches, source_row[None, :], 0), axis=1)
    asked = lax.all_to_all(
        request.reshape(spaces, capacity), "space", split_axis=0, concat_axis=0, tiled=True
    ).reshape(-1)

    cross = reduced(cross_part(place, share, low, high, near, control_near, blend, 4))
    above = passed_along(
        jnp.concatenate([cross[4:6], own[:1] + cross[:1]], axis=0), "space", -1
    )
    below = passed_along(cross[10:12], "space", 1)

    outgoing = answers(place, asked, own, cross, below, above)
    chan_count = outgoing.shape[2]
    arrived = lax.all_to_all(
        outgoing.reshape(spaces, capacity * 2, chan_count, width),
        "space",
        split_axis=0,
        concat_axis=0,
        tiled=True,
    ).reshape(spaces * capacity, 2, chan_count, width)
    return fine_part(slot_index, arrived, column_source, column_code)


def solution(mesh):
    placed = (
        P("member", None, "space", None),
        P(None, "space", None),
        P(),
        P(),
        P("space", None),
        P("space"),
        P("space", None),
        P("space", None),
    )
    return jax.shard_map(
        per_device,
        mesh=mesh,
        in_specs=placed,
        out_specs=P("space", "member", None, None),
        check_vma=False,
    )
```

```python
import jax
import jax.numpy as jnp
import numpy as np
from jax import lax
from jax.experimental import pallas as pl
from jax.experimental.pallas import tpu as pltpu
from jax.sharding import PartitionSpec as P

SCALE = 1.0 / 625.0
LANES = 128
PITCH = 24


def passed_along(x, axis, by):
    length = lax.axis_size(axis)
    pairs = [(i, i + by) for i in range(length) if 0 <= i + by < length]
    return lax.ppermute(x, axis, pairs)


def swapped(x, axis, bit):
    length = lax.axis_size(axis)
    return lax.ppermute(x, axis, [(i, i ^ bit) for i in range(length)])


def split_lanes(x):
    return [x[:, i : i + LANES] for i in range(0, x.shape[-1], LANES)]


def joined(parts):
    return jnp.concatenate(parts, axis=-1)


def side_sum(parts, lane):
    ahead = [pltpu.roll(p, 1, 1) for p in parts]
    behind = [pltpu.roll(p, LANES - 1, 1) for p in parts]
    out = []
    for i in range(len(parts)):
        left = jnp.where(lane == 0, ahead[i - 1] if i else 0.0, ahead[i])
        right = jnp.where(
            lane == LANES - 1, behind[i + 1] if i + 1 < len(parts) else 0.0, behind[i]
        )
        out.append(left + right)
    return out


def plus(a, b):
    return [p + q for p, q in zip(a, b)]


def times(a, b):
    return [p * q for p, q in zip(a, b)]


def scaled(factor, a):
    return [factor * p for p in a]


def widen(parts, lane):
    return plus(parts, side_sum(parts, lane))


def edges_kernel(members_ref, control_ref, top_ref, bottom_ref, scratch, top_out, bottom_out, sems):
    step = pl.program_id(0)
    steps = pl.num_programs(0)
    group = members_ref.shape[0]
    chans, rows = members_ref.shape[1:3]
    parts = scratch.shape[0]

    def copies(first, count, index):
        return [
            pltpu.make_async_copy(
                stage.at[pl.ds(first, count)], ref.at[pl.ds(first, count)], sems.at[side, index]
            )
            for side, (stage, ref) in enumerate(((top_out, top_ref), (bottom_out, bottom_ref)))
        ]

    def rows_out(wide, index):
        for part in range(parts):
            lanes = slice(part * LANES, (part + 1) * LANES)
            for chan in range(chans):
                scratch[part, chan * PITCH : chan * PITCH + rows] = wide[chan, :, lanes]
            for slot in range(2):
                for which, stage in ((slot, top_out), (rows - 2 + slot, bottom_out)):
                    stage[index, slot, :, lanes] = scratch[
                        part, pl.ds(which, chans, stride=PITCH), :
                    ]

    for one in range(group):
        rows_out(members_ref[one].astype(jnp.float32), step * group + one)
    for copy in copies(step * group, group, step):
        copy.start()

    @pl.when(step == steps - 1)
    def _():
        count = top_ref.shape[0] - 1
        rows_out(control_ref[...], count)
        for copy in copies(count, 1, count // group):
            copy.start()
        for index in range(count // group):
            for copy in copies(index * group, group, index):
                copy.wait()
        for copy in copies(count, 1, count // group):
            copy.wait()


def edge_rows(members, control, group):
    count, chans, rows, width = members.shape
    shape = (count + 1, 2, chans, width)
    out = jax.ShapeDtypeStruct(shape, jnp.float32)
    return pl.pallas_call(
        edges_kernel,
        grid=(count // group,),
        in_specs=[
            pl.BlockSpec((group, chans, rows, width), lambda i: (i, 0, 0, 0)),
            pl.BlockSpec((chans, rows, width), lambda i: (0, 0, 0)),
        ],
        out_specs=[pl.BlockSpec(memory_space=pl.ANY)] * 2,
        out_shape=[out, out],
        scratch_shapes=[
            pltpu.VMEM((width // LANES, chans * PITCH, LANES), jnp.float32),
            pltpu.VMEM(shape, jnp.float32),
            pltpu.VMEM(shape, jnp.float32),
            pltpu.SemaphoreType.DMA((2, count // group + 1)),
        ],
        name="edge_rows",
    )(members, control)


def column_operators(width):
    q = np.eye(width) + np.eye(width, k=1) + np.eye(width, k=-1)
    q2 = q @ q
    q3 = q2 @ q
    eye = np.eye(width)
    return q2 @ q2 + 12 * q2 + 6 * eye, 4 * q3 + 12 * q, 6 * q2 + 4 * eye, 4 * q


def windowed(operator):
    first = operator[:256, :256]
    second = operator[128:, 128:].copy()
    second[:128, :128] = 0.0
    return first, second


def stacked(operators):
    first, second = zip(*[windowed(op) for op in operators])
    return np.stack([np.concatenate(first), np.concatenate(second)]).astype(jnp.bfloat16)


def own_kernel(
    place_ref, share_ref, members_ref, control_ref, blend_ref, operator_ref,
    keep_ref, give_ref, near_ref, control_near_ref,
    total, still, field, first, second, mixed, scratch,
):
    step = pl.program_id(0)
    chans, rows, width = members_ref.shape[1:]
    parts = width // LANES
    count = pl.num_programs(0) - 2

    def lanes(part):
        return slice(part * LANES, (part + 1) * LANES)

    @pl.when(step == 0)
    def _():
        field[...] = jnp.zeros(field.shape, jnp.float32)

    @pl.when(step < count)
    def _():
        def fill(chan, carry):
            for part in range(parts):
                state = members_ref[0, chan, :, lanes(part)].astype(jnp.float32)
                field[part, chan, 8 : 8 + rows] = state * control_ref[chan, :, lanes(part)]
                scratch[part, pl.ds(pl.multiple_of(chan * PITCH, 8), rows), :] = state
            return carry

        lax.fori_loop(0, chans, fill, 0, unroll=4)
        for place, row in enumerate((0, 1, 2, 3, rows - 4, rows - 3, rows - 2, rows - 1)):
            for part in range(parts):
                near_ref[0, place, :, lanes(part)] = scratch[
                    part, pl.ds(row, chans, stride=PITCH), :
                ].astype(jnp.bfloat16)

    @pl.when(step >= count)
    def _():
        def fill(chan, carry):
            for part in range(parts):
                block = control_ref[chan, :, lanes(part)]
                rough = block.astype(jnp.bfloat16).astype(jnp.float32)
                field[part, chan, 8 : 8 + rows] = jnp.where(step == count, rough, block - rough)
                scratch[part, pl.ds(pl.multiple_of(chan * PITCH, 8), rows), :] = block
            return carry

        lax.fori_loop(0, chans, fill, 0, unroll=4)

    @pl.when(step == count)
    def _():
        for place, row in enumerate((0, 1, 2, 3, rows - 4, rows - 3, rows - 2, rows - 1)):
            for part in range(parts):
                control_near_ref[place, :, lanes(part)] = scratch[
                    part, pl.ds(row, chans, stride=PITCH), :
                ]

    @pl.when(place_ref[1] == 0)
    def _():
        def image(chan, carry):
            for part in range(parts):
                for row in range(3):
                    field[part, chan, 6 - row : 7 - row] = -field[part, chan, 8 + row : 9 + row]
            return carry

        lax.fori_loop(0, chans, image, 0, unroll=4)

    @pl.when(place_ref[1] == 2)
    def _():
        def image(chan, carry):
            for part in range(parts):
                for row in range(3):
                    field[part, chan, 9 + rows + row : 10 + rows + row] = -field[
                        part, chan, 7 + rows - row : 8 + rows - row
                    ]
            return carry

        lax.fori_loop(0, chans, image, 0, unroll=4)

    def at_distance(part, chan, distance):
        if distance == 0:
            return field[part, chan, 8 : 8 + rows]
        return (
            field[part, chan, 8 - distance : 8 - distance + rows]
            + field[part, chan, 8 + distance : 8 + distance + rows]
        )

    def gather(chan, carry):
        at = pl.ds(pl.multiple_of(chan * rows, rows), rows)
        for distance in range(4):
            base = distance * 2 * LANES
            for part in range(parts):
                value = at_distance(part, chan, distance).astype(jnp.bfloat16)
                if part < 2:
                    first[at, base + part * LANES : base + (part + 1) * LANES] = value
                if part > 0:
                    second[at, base + (part - 1) * LANES : base + part * LANES] = value
        return carry

    lax.fori_loop(0, chans, gather, 0, unroll=4)
    mixed[0] = jnp.dot(first[...], operator_ref[0], preferred_element_type=jnp.float32)
    mixed[1] = jnp.dot(second[...], operator_ref[1], preferred_element_type=jnp.float32)

    def localized(chan):
        at = pl.ds(pl.multiple_of(chan * rows, rows), rows)
        low = [mixed[0, at, lanes(0)], mixed[0, at, lanes(1)]]
        high = [mixed[1, at, lanes(0)], mixed[1, at, lanes(1)]]
        found = [low[0], low[1] + high[0], high[1]]
        return [value + at_distance(part, chan, 4) for part, value in enumerate(found)]

    @pl.when(step < count)
    def _():
        share = share_ref[jnp.minimum(step, count - 1)]

        def one_chan(chan, carry):
            value = localized(chan)
            for part in range(parts):
                state = members_ref[0, chan, :, lanes(part)].astype(jnp.float32)
                term = (share * state) * value[part]
                before = jnp.where(step == 0, 0.0, total[chan, :, lanes(part)])
                total[chan, :, lanes(part)] = before + term
            return carry

        lax.fori_loop(0, chans, one_chan, 0, unroll=4)

    @pl.when(step == count)
    def _():
        def one_chan(chan, carry):
            value = localized(chan)
            for part in range(parts):
                still[chan, :, lanes(part)] = value[part]
            return carry

        lax.fori_loop(0, chans, one_chan, 0, unroll=4)

    @pl.when(step == count + 1)
    def _():
        def one_group(group, carry):
            slot = jnp.bitwise_xor(group, place_ref[0])
            blends = blend_ref[pl.ds(pl.multiple_of(group * 8, 8), 8), :]
            for inner in range(8):
                chan = group * 8 + inner
                blend = jnp.broadcast_to(blends[inner : inner + 1], (rows, LANES))
                value = localized(chan)
                for part in range(parts):
                    whole = value[part] + still[chan, :, lanes(part)]
                    total[chan, :, lanes(part)] = SCALE * (
                        (1.0 - blend) * total[chan, :, lanes(part)] + (0.25 * blend) * whole
                    )
            done = total[pl.ds(pl.multiple_of(group * 8, 8), 8)]

            @pl.when(jnp.bitwise_and(slot, 1) == 0)
            def _():
                keep_ref[slot // 2] = done

            @pl.when(jnp.bitwise_and(slot, 1) == 1)
            def _():
                give_ref[slot // 2] = done

            return carry

        lax.fori_loop(0, chans // 8, one_group, 0)


def own_part(place, share, members, control, blend):
    count, chans, rows, width = members.shape
    parts = width // LANES
    operators = jnp.asarray(stacked(column_operators(width)))
    half = (chans // 16, 8, rows, width)
    return pl.pallas_call(
        own_kernel,
        grid_spec=pltpu.PrefetchScalarGridSpec(
            num_scalar_prefetch=2,
            grid=(count + 2,),
            in_specs=[
                pl.BlockSpec(
                    (1, chans, rows, width),
                    lambda i, place, share: (jnp.minimum(i, count - 1), 0, 0, 0),
                ),
                pl.BlockSpec((chans, rows, width), lambda i, place, share: (0, 0, 0)),
                pl.BlockSpec((chans, LANES), lambda i, place, share: (0, 0)),
                pl.BlockSpec(operators.shape, lambda i, place, share: (0, 0, 0)),
            ],
            out_specs=[
                pl.BlockSpec(half, lambda i, place, share: (0, 0, 0, 0)),
                pl.BlockSpec(half, lambda i, place, share: (0, 0, 0, 0)),
                pl.BlockSpec(
                    (1, 8, chans, width),
                    lambda i, place, share: (jnp.minimum(i, count - 1), 0, 0, 0),
                ),
                pl.BlockSpec((8, chans, width), lambda i, place, share: (0, 0, 0)),
            ],
            scratch_shapes=[
                pltpu.VMEM((chans, rows, width), jnp.float32),
                pltpu.VMEM((chans, rows, width), jnp.float32),
                pltpu.VMEM((parts, chans, rows + 16, LANES), jnp.float32),
                pltpu.VMEM((chans * rows, operators.shape[1]), jnp.bfloat16),
                pltpu.VMEM((chans * rows, operators.shape[1]), jnp.bfloat16),
                pltpu.VMEM((2, chans * rows, 2 * LANES), jnp.float32),
                pltpu.VMEM((parts, chans * PITCH, LANES), jnp.float32),
            ],
        ),
        out_shape=[
            jax.ShapeDtypeStruct(half, jnp.float32),
            jax.ShapeDtypeStruct(half, jnp.float32),
            jax.ShapeDtypeStruct((count, 8, chans, width), jnp.bfloat16),
            jax.ShapeDtypeStruct((8, chans, width), jnp.float32),
        ],
        name="own_part",
    )(place, share, members, control, blend, operators)


def cross_kernel(
    place_ref, share_ref, low_ref, low_control_ref, high_ref, high_control_ref,
    near_ref, control_ref, blend_ref, pair_ref, single_ref,
    keep_ref, give_ref, sums, first, second, third, fourth, mixed, alone,
):
    step = pl.program_id(0)
    group = near_ref.shape[0]
    chans, width = near_ref.shape[2:]
    parts = width // LANES
    lane = lax.broadcasted_iota(jnp.int32, (8, LANES), 1)
    final = step == pl.num_programs(0) - 1
    span = group * chans
    sides = (
        (low_ref, low_control_ref, (1, 0), (0, 1, 2, 3)),
        (high_ref, high_control_ref, (0, 1), (7, 6, 5, 4)),
    )

    def lanes(part, base=0):
        return slice(base + part * LANES, base + (part + 1) * LANES)

    for side, (halo, halo_control, order, own) in enumerate(sides):
        for one in range(group):
            share = share_ref[step * group + one]
            at = slice(side * span + one * chans, side * span + (one + 1) * chans)
            below = slice(2 * span + at.start, 2 * span + at.stop)
            for part in range(parts):
                y1, y2 = [
                    (
                        halo[one, slot, :, lanes(part)]
                        * (share * halo_control[0, slot, :, lanes(part)])
                    ).astype(jnp.bfloat16)
                    for slot in order
                ]
                y3 = (
                    near_ref[one, own[2], :, lanes(part)].astype(jnp.float32)
                    * (share * control_ref[own[2], :, lanes(part)])
                ).astype(jnp.bfloat16)
                if part < 2:
                    first[at, lanes(part)] = y1
                    first[at, lanes(part, 2 * LANES)] = y2
                    third[at, lanes(part)] = y1
                    third[below, lanes(part)] = y3
                if part > 0:
                    second[at, lanes(part - 1)] = y1
                    second[at, lanes(part - 1, 2 * LANES)] = y2
                    fourth[at, lanes(part - 1)] = y1
                    fourth[below, lanes(part - 1)] = y3
    mixed[0] = jnp.dot(first[...], pair_ref[0], preferred_element_type=jnp.float32)
    mixed[1] = jnp.dot(second[...], pair_ref[1], preferred_element_type=jnp.float32)
    alone[0] = jnp.dot(third[...], single_ref[0], preferred_element_type=jnp.float32)
    alone[1] = jnp.dot(fourth[...], single_ref[1], preferred_element_type=jnp.float32)

    def piece(ref, at, part, base):
        if part == 0:
            return ref[0, at, lanes(0, base)]
        if part == parts - 1:
            return ref[1, at, lanes(1, base)]
        return ref[0, at, lanes(1, base)] + ref[1, at, lanes(0, base)]

    def per_chans(eight, carry):
        here = pl.ds(pl.multiple_of(eight * 8, 8), 8)
        for side, (halo, halo_control, order, own) in enumerate(sides):
            for part in range(parts):
                totals = [None] * 6
                c = [
                    halo_control[0, order[0], here, lanes(part)],
                    halo_control[0, order[1], here, lanes(part)],
                    control_ref[own[2], here, lanes(part)],
                    control_ref[own[3], here, lanes(part)],
                ]
                for one in range(group):
                    share = share_ref[step * group + one]
                    start = side * span + one * chans + eight * 8
                    at = pl.ds(pl.multiple_of(start, 8), 8)
                    below = pl.ds(pl.multiple_of(2 * span + start, 8), 8)
                    b1 = halo[one, order[0], here, lanes(part)]
                    b2 = halo[one, order[1], here, lanes(part)]
                    a = [
                        near_ref[one, row, here, lanes(part)].astype(jnp.float32) for row in own
                    ]
                    y = [x * (share * k) for x, k in zip((b1, b2, a[2], a[3]), c)]
                    terms = (
                        a[0] * piece(mixed, at, part, 0),
                        a[1] * piece(mixed, at, part, 2 * LANES),
                        a[2] * (piece(alone, at, part, 0) + y[1]),
                        a[3] * y[0],
                        b1 * (piece(alone, below, part, 0) + y[3]),
                        b2 * y[2],
                    )
                    totals = [t if s is None else s + t for s, t in zip(totals, terms)]
                for i, value in enumerate(totals):
                    place = side * 6 + i
                    before = jnp.where(step == 0, 0.0, sums[place, here, lanes(part)])
                    sums[place, here, lanes(part)] = before + value
        return carry

    lax.fori_loop(0, chans // 8, per_chans, 0)

    def exact(y1, y2, y3, y4):
        wide = scaled(4.0, widen(y1, lane))
        inner = plus(widen(plus(wide, scaled(6.0, y2)), lane), scaled(12.0, y1))
        top = plus(widen(inner, lane), scaled(4.0, y2))
        next_row = plus(
            widen(plus(scaled(1.5, wide), scaled(4.0, y2)), lane), scaled(4.0, y1)
        )
        return top, next_row, plus(wide, y2), y1, plus(scaled(4.0, widen(y3, lane)), y4), y3

    @pl.when(final)
    def _():
        def finish(eight, carry):
            at = pl.ds(pl.multiple_of(eight * 8, 8), 8)
            slot = jnp.bitwise_xor(eight, place_ref[0])
            blend = blend_ref[at, :]
            for side, (halo, halo_control, order, own) in enumerate(sides):
                found = exact(
                    split_lanes(halo_control[0, order[0], at, :]),
                    split_lanes(halo_control[0, order[1], at, :]),
                    split_lanes(control_ref[own[2], at, :]),
                    split_lanes(control_ref[own[3], at, :]),
                )
                for i, value in enumerate(found):
                    place = side * 6 + i
                    for part in range(parts):
                        sums[place, at, lanes(part)] = SCALE * (
                            (1.0 - blend) * sums[place, at, lanes(part)]
                            + (0.25 * blend) * value[part]
                        )

            @pl.when(jnp.bitwise_and(slot, 1) == 0)
            def _():
                keep_ref[slot // 2] = sums[:, at, :]

            @pl.when(jnp.bitwise_and(slot, 1) == 1)
            def _():
                give_ref[slot // 2] = sums[:, at, :]

            return carry

        lax.fori_loop(0, chans // 8, finish, 0, unroll=2)


def cross_part(place, share, low, high, near, control_near, blend, group):
    count, rows, chans, width = near.shape
    halo = pl.BlockSpec((group, 2, chans, width), lambda i: (i, 0, 0, 0))
    halo_control = pl.BlockSpec((1, 2, chans, width), lambda i: (count, 0, 0, 0))
    half = (chans // 16, 12, 8, width)
    _, p1, p2, p3 = column_operators(width)
    left, right = stacked([p1, p2]), stacked([p2, p3])
    pair = jnp.asarray(np.concatenate([left, right], axis=2))
    single = jnp.asarray(stacked([p3]))
    span = 2 * group * chans
    return pl.pallas_call(
        cross_kernel,
        grid=(count // group,),
        in_specs=[
            pl.BlockSpec(memory_space=pltpu.SMEM),
            pl.BlockSpec(memory_space=pltpu.SMEM),
            halo,
            halo_control,
            halo,
            halo_control,
            pl.BlockSpec((group, rows, chans, width), lambda i: (i, 0, 0, 0)),
            pl.BlockSpec((rows, chans, width), lambda i: (0, 0, 0)),
            pl.BlockSpec((chans, LANES), lambda i: (0, 0)),
            pl.BlockSpec(pair.shape, lambda i: (0, 0, 0)),
            pl.BlockSpec(single.shape, lambda i: (0, 0, 0)),
        ],
        out_specs=[pl.BlockSpec(half, lambda i: (0, 0, 0, 0))] * 2,
        out_shape=[jax.ShapeDtypeStruct(half, jnp.float32)] * 2,
        scratch_shapes=[
            pltpu.VMEM((12, chans, width), jnp.float32),
            pltpu.VMEM((span, 4 * LANES), jnp.bfloat16),
            pltpu.VMEM((span, 4 * LANES), jnp.bfloat16),
            pltpu.VMEM((2 * span, 2 * LANES), jnp.bfloat16),
            pltpu.VMEM((2 * span, 2 * LANES), jnp.bfloat16),
            pltpu.VMEM((2, span, 4 * LANES), jnp.float32),
            pltpu.VMEM((2, 2 * span, 2 * LANES), jnp.float32),
        ],
        name="cross_part",
    )(place, share, low, low, high, high, near, control_near, blend, pair, single)


def sent_kernel(own_ref, got_ref, last_ref, cross_ref, cross_got_ref, cross_last_ref, up_ref, down_ref, turned):
    chans, rows, width = last_ref.shape
    whole = own_ref[0] + got_ref[0] + last_ref[...]
    for part in range(width // LANES):
        lanes = slice(part * LANES, (part + 1) * LANES)
        for chan in range(chans):
            turned[chan * PITCH : chan * PITCH + 8] = whole[chan, :8, lanes]
        first = turned[pl.ds(0, chans, stride=PITCH), :]

        def crossed(i):
            return cross_ref[0, i, :, lanes] + cross_got_ref[0, i, :, lanes] + cross_last_ref[i, :, lanes]

        for i in range(2):
            up_ref[i, :, lanes] = crossed(4 + i)
            down_ref[i, :, lanes] = crossed(10 + i)
        up_ref[2, :, lanes] = first + crossed(0)


def sent_rows(own, got, last, cross, cross_got, cross_last):
    chans, rows, width = last.shape
    one = lambda x: pl.BlockSpec((1,) + x.shape[1:], lambda i: (0, 0, 0, 0))
    vmem = pl.BlockSpec(memory_space=pltpu.VMEM)
    return pl.pallas_call(
        sent_kernel,
        grid=(1,),
        in_specs=[one(own), one(got), vmem, one(cross), one(cross_got), vmem],
        out_specs=[vmem, vmem],
        out_shape=[
            jax.ShapeDtypeStruct((3, chans, width), jnp.float32),
            jax.ShapeDtypeStruct((2, chans, width), jnp.float32),
        ],
        scratch_shapes=[pltpu.VMEM((chans * PITCH, LANES), jnp.float32)],
        name="sent_rows",
    )(own, got, last, cross, cross_got, cross_last)


def answer_kernel(
    place_ref, asked_ref, own_ref, got_ref, last_ref, cross_ref, cross_got_ref, cross_last_ref,
    below_ref, above_ref, out_ref, turned, pairs,
):
    chans, rows, width = last_ref.shape
    parts = width // LANES
    capacity = out_ref.shape[0] // asked_ref.shape[0]
    keep_high = (place_ref[2] != 0).astype(jnp.float32)
    whole = own_ref[0] + got_ref[0] + last_ref[...]
    for part in range(parts):
        for chan in range(chans):
            turned[part, chan * PITCH : chan * PITCH + rows] = whole[
                chan, :, part * LANES : (part + 1) * LANES
            ]

    def crossed(i, lanes):
        return cross_ref[0, i, :, lanes] + cross_got_ref[0, i, :, lanes] + cross_last_ref[i, :, lanes]

    for part in range(parts):
        lanes = slice(part * LANES, (part + 1) * LANES)
        for row in range(rows + 1):
            if row < rows:
                value = turned[part, pl.ds(row, chans, stride=PITCH), :]
            else:
                value = keep_high * (above_ref[2, :, lanes] + crossed(10, lanes))
            if row < 4:
                value += crossed(row, lanes)
            if rows - 4 <= row < rows:
                value += crossed(6 + rows - 1 - row, lanes)
            if row < 2:
                value += below_ref[row, :, lanes]
            if rows - 2 <= row < rows:
                value += above_ref[rows - 1 - row, :, lanes]
            if row < rows:
                pairs[part, pl.ds(row * 2 * chans, chans, stride=2), :] = value
            if row > 0:
                pairs[part, pl.ds((row - 1) * 2 * chans + 1, chans, stride=2), :] = value

    def one(device, carry):
        for slot in range(capacity):
            row = asked_ref[device, 0, slot]
            at = pl.ds(pl.multiple_of(row * (2 * chans), 2 * chans), 2 * chans)
            for part in range(parts):
                out_ref[device * capacity + slot, :, part * LANES : (part + 1) * LANES] = pairs[
                    part, at, :
                ]
        return carry

    lax.fori_loop(0, asked_ref.shape[0], one, 0, unroll=4)


def answers(place, asked, capacity, own, got, last, cross, cross_got, cross_last, below, above):
    chans, rows, width = last.shape
    slots = asked.shape[0] * capacity
    smem = pl.BlockSpec(memory_space=pltpu.SMEM)
    vmem = pl.BlockSpec(memory_space=pltpu.VMEM)
    one = lambda x: pl.BlockSpec((1,) + x.shape[1:], lambda i: (0, 0, 0, 0))
    return pl.pallas_call(
        answer_kernel,
        grid=(1,),
        in_specs=[smem, smem, one(own), one(got), vmem, one(cross), one(cross_got), vmem, vmem, vmem],
        out_specs=vmem,
        out_shape=jax.ShapeDtypeStruct((slots, 2 * chans, width), jnp.float32),
        scratch_shapes=[
            pltpu.VMEM((width // LANES, chans * PITCH, LANES), jnp.float32),
            pltpu.VMEM((width // LANES, rows * 2 * chans, LANES), jnp.float32),
        ],
        name="answers",
    )(place, asked, own, got, last, cross, cross_got, cross_last, below, above)


def fine_kernel(slot_ref, arrived_ref, index_ref, weight_ref, out_ref):
    blocks = index_ref.shape[0]
    pairs, width = arrived_ref.shape[1:]
    fine = index_ref.shape[2]
    half = LANES // 2
    quarter = half // 2
    lane = lax.broadcasted_iota(jnp.int32, (8, LANES), 1)
    even = lax.broadcasted_iota(jnp.int32, (8, LANES), 0) % 2 == 0

    def one(block, carry):
        slot = slot_ref[block]
        windows = []
        for group in range(pairs // 8):
            parts = []
            for part in split_lanes(arrived_ref[slot, pl.ds(group * 8, 8), :]):
                other = jnp.where(even, pltpu.roll(part, 7, 0), pltpu.roll(part, 1, 0))
                parts.append(0.75 * part + 0.25 * other)
            turned = {
                shift: [pltpu.roll(p, shift, 1) for p in parts]
                for shift in (quarter, LANES - quarter)
            }
            found = []
            for chunk in range(fine // LANES):
                part, ahead = divmod(chunk * half - quarter, LANES)
                rolled = turned[LANES - ahead]
                if part < 0:
                    found.append(rolled[part + 1])
                elif part + 1 == len(parts):
                    found.append(rolled[part])
                else:
                    found.append(
                        jnp.where(lane < LANES - ahead, rolled[part], rolled[part + 1])
                    )
            windows.append(found)
        for chunk in range(fine // LANES):
            lanes = slice(chunk * LANES, (chunk + 1) * LANES)
            index = index_ref[block, :, lanes]
            weight = weight_ref[block, :, lanes]
            for group in range(pairs // 8):
                near = windows[group][chunk]
                left = jnp.take_along_axis(near, index, axis=1)
                right = jnp.take_along_axis(near, index + 1, axis=1)
                value = (1.0 - weight) * left + weight * right
                out_ref[block, group * 4 : (group + 1) * 4, :, lanes] = value.reshape(4, 2, LANES)
        return carry

    lax.fori_loop(0, blocks, one, 0, unroll=4)


def fine_part(slot, arrived, index, weight):
    blocks, _, fine = index.shape
    chans = arrived.shape[1] // 2
    smem = pl.BlockSpec(memory_space=pltpu.SMEM)
    vmem = pl.BlockSpec(memory_space=pltpu.VMEM)
    return pl.pallas_call(
        fine_kernel,
        in_specs=[smem, vmem, vmem, vmem],
        out_specs=vmem,
        out_shape=jax.ShapeDtypeStruct((blocks, chans, 2, fine), jnp.float32),
        name="fine_part",
    )(slot, arrived, index, weight)


def column_kernel(source_ref, code_ref, index_ref, weight_ref):
    blocks, fine = source_ref.shape
    column = lax.broadcasted_iota(jnp.int32, (1, fine), 1)
    first = (column // LANES) * (LANES // 2) - LANES // 4
    for block in range(blocks):
        shape = index_ref.shape[1:]
        index_ref[block] = jnp.broadcast_to(source_ref[block : block + 1] - first, shape)
        weight_ref[block] = jnp.broadcast_to(
            code_ref[block : block + 1].astype(jnp.float32) * (1.0 / 16.0), shape
        )


def columns(source, code):
    blocks, fine = source.shape
    return pl.pallas_call(
        column_kernel,
        out_shape=[
            jax.ShapeDtypeStruct((blocks, 8, fine), jnp.int32),
            jax.ShapeDtypeStruct((blocks, 8, fine), jnp.float32),
        ],
        name="columns",
    )(source, code)


def per_device(
    members,
    control,
    hybrid_weight,
    member_weights,
    source_device,
    source_row,
    column_source,
    column_code,
):
    member_count, chans, row_count, width = members.shape
    spaces = lax.axis_size("space")
    space_index = lax.axis_index("space")
    member_slot = lax.axis_index("member")

    top, bottom = edge_rows(members, control, 4)
    high = passed_along(top, "space", -1)
    low = passed_along(bottom, "space", 1)

    place = jnp.stack(
        [
            member_slot,
            jnp.where(space_index == 0, 0, jnp.where(space_index == spaces - 1, 2, 1)),
            (space_index < spaces - 1).astype(jnp.int32),
        ]
    ).astype(jnp.int32)
    weight_codes = member_weights.astype(jnp.float32)
    share = lax.dynamic_slice_in_dim(
        weight_codes, member_slot * member_count, member_count
    ) / jnp.sum(weight_codes)
    blend = jnp.broadcast_to(hybrid_weight[:, None], (chans, LANES))
    source_index = source_device[:, 0]
    capacity = max(2, 2 * row_count // spaces)
    chosen = (source_index[:, None] == jnp.arange(spaces, dtype=jnp.int32)[None, :]).astype(
        jnp.int32
    )
    earlier = jnp.cumsum(chosen, axis=0) - chosen
    rank_within = jnp.sum(earlier * chosen, axis=1)
    slot_index = source_index * capacity + rank_within
    spread = slot_index[None, :] - capacity * jnp.arange(spaces, dtype=jnp.int32)[:, None]
    lane = jnp.arange(LANES, dtype=jnp.int32)
    taken = (spread[:, None, :] == lane[None, :, None]) & (lane < capacity)[None, :, None]
    request = jnp.sum(jnp.where(taken, source_row[None, None, :], 0), axis=2)[:, None, :]
    index, weight = columns(column_source, column_code)

    own_keep, own_give, near, control_near = own_part(place, share, members, control, blend)
    own_give, request = lax.optimization_barrier((own_give, request))
    own_got = swapped(own_give, "member", 1)
    own_last = swapped(own_keep[1] + own_got[1], "member", 2)
    asked = lax.all_to_all(request, "space", split_axis=0, concat_axis=0, tiled=True)
    near, asked, own_last, index, weight, slot_index = lax.optimization_barrier(
        (near, asked, own_last, index, weight, slot_index)
    )

    keep, give = cross_part(place, share, low, high, near, control_near, blend, 4)
    got = swapped(give, "member", 1)
    last = swapped(keep[1] + got[1], "member", 2)
    up, down = sent_rows(own_keep, own_got, own_last, keep, got, last)
    above = passed_along(up, "space", -1)
    below = passed_along(down, "space", 1)

    outgoing = answers(
        place, asked, capacity, own_keep, own_got, own_last, keep, got, last, below, above
    )
    pair_rows = outgoing.shape[1]
    arrived = lax.all_to_all(
        outgoing.reshape(spaces, capacity * pair_rows, width),
        "space",
        split_axis=0,
        concat_axis=0,
        tiled=True,
    ).reshape(spaces * capacity, pair_rows, width)
    return fine_part(slot_index, arrived, index, weight)


def solution(mesh):
    placed = (
        P("member", None, "space", None),
        P(None, "space", None),
        P(),
        P(),
        P("space", None),
        P("space"),
        P("space", None),
        P("space", None),
    )
    return jax.shard_map(
        per_device,
        mesh=mesh,
        in_specs=placed,
        out_specs=P("space", "member", None, None),
        check_vma=False,
    )
```

```python
import jax
import jax.numpy as jnp
import numpy as np
from jax import lax
from jax.experimental import pallas as pl
from jax.experimental.pallas import tpu as pltpu
from jax.sharding import PartitionSpec as P

SCALE = 1.0 / 625.0
LANES = 128
PITCH = 24


def passed_along(x, axis, by):
    length = lax.axis_size(axis)
    pairs = [(i, i + by) for i in range(length) if 0 <= i + by < length]
    return lax.ppermute(x, axis, pairs)


def swapped(x, axis, bit):
    length = lax.axis_size(axis)
    return lax.ppermute(x, axis, [(i, i ^ bit) for i in range(length)])


def split_lanes(x):
    return [x[:, i : i + LANES] for i in range(0, x.shape[-1], LANES)]


def joined(parts):
    return jnp.concatenate(parts, axis=-1)


def side_sum(parts, lane):
    ahead = [pltpu.roll(p, 1, 1) for p in parts]
    behind = [pltpu.roll(p, LANES - 1, 1) for p in parts]
    out = []
    for i in range(len(parts)):
        left = jnp.where(lane == 0, ahead[i - 1] if i else 0.0, ahead[i])
        right = jnp.where(
            lane == LANES - 1, behind[i + 1] if i + 1 < len(parts) else 0.0, behind[i]
        )
        out.append(left + right)
    return out


def plus(a, b):
    return [p + q for p, q in zip(a, b)]


def times(a, b):
    return [p * q for p, q in zip(a, b)]


def scaled(factor, a):
    return [factor * p for p in a]


def widen(parts, lane):
    return plus(parts, side_sum(parts, lane))


def edges_kernel(members_ref, control_ref, top_ref, bottom_ref, scratch, top_out, bottom_out, sems):
    step = pl.program_id(0)
    steps = pl.num_programs(0)
    group = members_ref.shape[0]
    chans, rows = members_ref.shape[1:3]
    parts = scratch.shape[0]

    def copies(first, count, index):
        return [
            pltpu.make_async_copy(
                stage.at[pl.ds(first, count)], ref.at[pl.ds(first, count)], sems.at[side, index]
            )
            for side, (stage, ref) in enumerate(((top_out, top_ref), (bottom_out, bottom_ref)))
        ]

    def rows_out(wide, index):
        for part in range(parts):
            lanes = slice(part * LANES, (part + 1) * LANES)
            for chan in range(chans):
                scratch[part, chan * PITCH : chan * PITCH + rows] = wide[chan, :, lanes]
            for slot in range(2):
                for which, stage in ((slot, top_out), (rows - 2 + slot, bottom_out)):
                    stage[index, slot, :, lanes] = scratch[
                        part, pl.ds(which, chans, stride=PITCH), :
                    ]

    for one in range(group):
        rows_out(members_ref[one].astype(jnp.float32), step * group + one)
    for copy in copies(step * group, group, step):
        copy.start()

    @pl.when(step == steps - 1)
    def _():
        count = top_ref.shape[0] - 1
        rows_out(control_ref[...], count)
        for copy in copies(count, 1, count // group):
            copy.start()
        for index in range(count // group):
            for copy in copies(index * group, group, index):
                copy.wait()
        for copy in copies(count, 1, count // group):
            copy.wait()


def edge_rows(members, control, group):
    count, chans, rows, width = members.shape
    shape = (count + 1, 2, chans, width)
    out = jax.ShapeDtypeStruct(shape, jnp.float32)
    return pl.pallas_call(
        edges_kernel,
        grid=(count // group,),
        in_specs=[
            pl.BlockSpec((group, chans, rows, width), lambda i: (i, 0, 0, 0)),
            pl.BlockSpec((chans, rows, width), lambda i: (0, 0, 0)),
        ],
        out_specs=[pl.BlockSpec(memory_space=pl.ANY)] * 2,
        out_shape=[out, out],
        scratch_shapes=[
            pltpu.VMEM((width // LANES, chans * PITCH, LANES), jnp.float32),
            pltpu.VMEM(shape, jnp.float32),
            pltpu.VMEM(shape, jnp.float32),
            pltpu.SemaphoreType.DMA((2, count // group + 1)),
        ],
        name="edge_rows",
    )(members, control)


def column_operators(width):
    q = np.eye(width) + np.eye(width, k=1) + np.eye(width, k=-1)
    q2 = q @ q
    q3 = q2 @ q
    eye = np.eye(width)
    return q2 @ q2 + 12 * q2 + 6 * eye, 4 * q3 + 12 * q, 6 * q2 + 4 * eye, 4 * q


def windowed(operator):
    first = operator[:256, :256]
    second = operator[128:, 128:].copy()
    second[:128, :128] = 0.0
    return first, second


def stacked(operators):
    first, second = zip(*[windowed(op) for op in operators])
    return np.stack([np.concatenate(first), np.concatenate(second)]).astype(jnp.bfloat16)


def own_kernel(
    place_ref, share_ref, members_ref, control_ref, blend_ref, operator_ref,
    keep_ref, give_ref, near_ref, control_near_ref,
    total, scratch, *work,
):
    step = pl.program_id(0)
    both, chans, rows, width = members_ref.shape
    parts = width // LANES
    last = pl.num_programs(0) - 1
    static = step == last
    fields, firsts, seconds, mixes = [work[i * both : (i + 1) * both] for i in range(4)]
    ends = (0, 1, 2, 3, rows - 4, rows - 3, rows - 2, rows - 1)

    def lanes(part):
        return slice(part * LANES, (part + 1) * LANES)

    @pl.when(step == 0)
    def _():
        total[...] = jnp.zeros(total.shape, jnp.float32)
        for field in fields:
            field[...] = jnp.zeros(field.shape, jnp.float32)

    @pl.when(step < last)
    def _():
        for which, field in enumerate(fields):

            def fill(chan, carry):
                for part in range(parts):
                    state = members_ref[which, chan, :, lanes(part)].astype(jnp.float32)
                    field[part, chan, 8 : 8 + rows] = state * control_ref[chan, :, lanes(part)]
                    scratch[part, pl.ds(pl.multiple_of(chan * PITCH, 8), rows), :] = state
                return carry

            lax.fori_loop(0, chans, fill, 0, unroll=4)
            for place, row in enumerate(ends):
                for part in range(parts):
                    near_ref[which, place, :, lanes(part)] = scratch[
                        part, pl.ds(row, chans, stride=PITCH), :
                    ].astype(jnp.bfloat16)

    @pl.when(static)
    def _():
        def fill(chan, carry):
            for part in range(parts):
                block = control_ref[chan, :, lanes(part)]
                for field in fields:
                    field[part, chan, 8 : 8 + rows] = block
                scratch[part, pl.ds(pl.multiple_of(chan * PITCH, 8), rows), :] = block
            return carry

        lax.fori_loop(0, chans, fill, 0, unroll=4)
        for place, row in enumerate(ends):
            for part in range(parts):
                control_near_ref[place, :, lanes(part)] = scratch[
                    part, pl.ds(row, chans, stride=PITCH), :
                ]

    @pl.when(place_ref[1] == 0)
    def _():
        def image(chan, carry):
            for field in fields:
                for part in range(parts):
                    for row in range(3):
                        field[part, chan, 6 - row : 7 - row] = -field[
                            part, chan, 8 + row : 9 + row
                        ]
            return carry

        lax.fori_loop(0, chans, image, 0, unroll=4)

    @pl.when(place_ref[1] == 2)
    def _():
        def image(chan, carry):
            for field in fields:
                for part in range(parts):
                    for row in range(3):
                        field[part, chan, 9 + rows + row : 10 + rows + row] = -field[
                            part, chan, 7 + rows - row : 8 + rows - row
                        ]
            return carry

        lax.fori_loop(0, chans, image, 0, unroll=4)

    def at_distance(field, part, chan, distance):
        if distance == 0:
            return field[part, chan, 8 : 8 + rows]
        return (
            field[part, chan, 8 - distance : 8 - distance + rows]
            + field[part, chan, 8 + distance : 8 + distance + rows]
        )

    refine = jnp.where(static, 1.0, 0.0)

    def gather(which, chan):
        start = chan * rows
        at = pl.ds(start if isinstance(chan, int) else pl.multiple_of(start, rows), rows)
        for distance in range(4):
            base = distance * 2 * LANES
            for part in range(parts):
                value = at_distance(fields[which], part, chan, distance)
                if which:
                    value -= refine * value.astype(jnp.bfloat16).astype(jnp.float32)
                value = value.astype(jnp.bfloat16)
                if part < 2:
                    firsts[which][at, base + part * LANES : base + (part + 1) * LANES] = value
                if part > 0:
                    seconds[which][at, base + (part - 1) * LANES : base + part * LANES] = value

    def multiply(which):
        for window, ref in enumerate((firsts[which], seconds[which])):
            mixes[which][window] = jnp.dot(
                ref[...], operator_ref[window], preferred_element_type=jnp.float32
            )

    def collect(which, chan):
        at = pl.ds(chan * rows, rows)
        mixed = mixes[which]
        low = [mixed[0, at, lanes(0)], mixed[0, at, lanes(1)]]
        high = [mixed[1, at, lanes(0)], mixed[1, at, lanes(1)]]
        found = [low[0], low[1] + high[0], high[1]]
        blend = blend_ref[chan : chan + 1, :]
        share = share_ref[jnp.minimum(step, last - 1) * both + which]
        factor = jnp.where(static, 0.25 * blend, share)
        for part in range(parts):
            far = at_distance(fields[which], part, chan, 4)
            value = found[part] + (far if which == 0 else (1.0 - refine) * far)
            state = members_ref[which, chan, :, lanes(part)].astype(jnp.float32)
            state = jnp.where(static, 1.0, state)
            before = total[chan, :, lanes(part)]
            if which == 0:
                before = jnp.where(static, 1.0 - blend, 1.0) * before
            total[chan, :, lanes(part)] = before + (factor * state) * value

    def gather_four(group, carry):
        for inner in range(4):
            gather(0, group * 4 + inner)
        return carry

    lax.fori_loop(0, chans // 4, gather_four, 0)
    multiply(0)
    for chan in range(chans):
        gather(1, chan)
    multiply(1)
    for chan in range(chans):
        collect(0, chan)
    for chan in range(chans):
        collect(1, chan)

    @pl.when(static)
    def _():
        def one_group(group, carry):
            slot = jnp.bitwise_xor(group, place_ref[0])
            done = SCALE * total[pl.ds(pl.multiple_of(group * 8, 8), 8)]

            @pl.when(jnp.bitwise_and(slot, 1) == 0)
            def _():
                keep_ref[slot // 2] = done

            @pl.when(jnp.bitwise_and(slot, 1) == 1)
            def _():
                give_ref[slot // 2] = done

            return carry

        lax.fori_loop(0, chans // 8, one_group, 0)


def own_part(place, share, members, control, blend):
    count, chans, rows, width = members.shape
    parts = width // LANES
    both = 2
    steps = count // both
    operators = jnp.asarray(stacked(column_operators(width)))
    depth = operators.shape[1]
    half = (chans // 16, 8, rows, width)
    return pl.pallas_call(
        own_kernel,
        grid_spec=pltpu.PrefetchScalarGridSpec(
            num_scalar_prefetch=2,
            grid=(steps + 1,),
            in_specs=[
                pl.BlockSpec(
                    (both, chans, rows, width),
                    lambda i, place, share: (jnp.minimum(i, steps - 1), 0, 0, 0),
                ),
                pl.BlockSpec((chans, rows, width), lambda i, place, share: (0, 0, 0)),
                pl.BlockSpec((chans, LANES), lambda i, place, share: (0, 0)),
                pl.BlockSpec(operators.shape, lambda i, place, share: (0, 0, 0)),
            ],
            out_specs=[
                pl.BlockSpec(half, lambda i, place, share: (0, 0, 0, 0)),
                pl.BlockSpec(half, lambda i, place, share: (0, 0, 0, 0)),
                pl.BlockSpec(
                    (both, 8, chans, width),
                    lambda i, place, share: (jnp.minimum(i, steps - 1), 0, 0, 0),
                ),
                pl.BlockSpec((8, chans, width), lambda i, place, share: (0, 0, 0)),
            ],
            scratch_shapes=[
                pltpu.VMEM((chans, rows, width), jnp.float32),
                pltpu.VMEM((parts, chans * PITCH, LANES), jnp.float32),
            ]
            + [pltpu.VMEM((parts, chans, rows + 16, LANES), jnp.float32)] * both
            + [pltpu.VMEM((chans * rows, depth), jnp.bfloat16)] * (2 * both)
            + [pltpu.VMEM((2, chans * rows, 2 * LANES), jnp.float32)] * both,
        ),
        out_shape=[
            jax.ShapeDtypeStruct(half, jnp.float32),
            jax.ShapeDtypeStruct(half, jnp.float32),
            jax.ShapeDtypeStruct((count, 8, chans, width), jnp.bfloat16),
            jax.ShapeDtypeStruct((8, chans, width), jnp.float32),
        ],
        name="own_part",
    )(place, share, members, control, blend, operators)


def cross_kernel(
    place_ref, share_ref, low_ref, low_control_ref, high_ref, high_control_ref,
    near_ref, control_ref, blend_ref, pair_ref, single_ref,
    keep_ref, give_ref, sums, first, second, third, fourth, mixed, alone,
):
    step = pl.program_id(0)
    group = near_ref.shape[0]
    chans, width = near_ref.shape[2:]
    parts = width // LANES
    lane = lax.broadcasted_iota(jnp.int32, (8, LANES), 1)
    final = step == pl.num_programs(0) - 1
    span = group * chans
    sides = (
        (low_ref, low_control_ref, (1, 0), (0, 1, 2, 3)),
        (high_ref, high_control_ref, (0, 1), (7, 6, 5, 4)),
    )

    def lanes(part, base=0):
        return slice(base + part * LANES, base + (part + 1) * LANES)

    for side, (halo, halo_control, order, own) in enumerate(sides):
        for one in range(group):
            share = share_ref[step * group + one]
            at = slice(side * span + one * chans, side * span + (one + 1) * chans)
            below = slice(2 * span + at.start, 2 * span + at.stop)
            for part in range(parts):
                y1, y2 = [
                    (
                        halo[one, slot, :, lanes(part)]
                        * (share * halo_control[0, slot, :, lanes(part)])
                    ).astype(jnp.bfloat16)
                    for slot in order
                ]
                y3 = (
                    near_ref[one, own[2], :, lanes(part)].astype(jnp.float32)
                    * (share * control_ref[own[2], :, lanes(part)])
                ).astype(jnp.bfloat16)
                if part < 2:
                    first[at, lanes(part)] = y1
                    first[at, lanes(part, 2 * LANES)] = y2
                    third[at, lanes(part)] = y1
                    third[below, lanes(part)] = y3
                if part > 0:
                    second[at, lanes(part - 1)] = y1
                    second[at, lanes(part - 1, 2 * LANES)] = y2
                    fourth[at, lanes(part - 1)] = y1
                    fourth[below, lanes(part - 1)] = y3
    mixed[0] = jnp.dot(first[...], pair_ref[0], preferred_element_type=jnp.float32)
    mixed[1] = jnp.dot(second[...], pair_ref[1], preferred_element_type=jnp.float32)
    alone[0] = jnp.dot(third[...], single_ref[0], preferred_element_type=jnp.float32)
    alone[1] = jnp.dot(fourth[...], single_ref[1], preferred_element_type=jnp.float32)

    def piece(ref, at, part, base):
        if part == 0:
            return ref[0, at, lanes(0, base)]
        if part == parts - 1:
            return ref[1, at, lanes(1, base)]
        return ref[0, at, lanes(1, base)] + ref[1, at, lanes(0, base)]

    def per_chans(eight, carry):
        here = pl.ds(pl.multiple_of(eight * 8, 8), 8)
        for side, (halo, halo_control, order, own) in enumerate(sides):
            for part in range(parts):
                totals = [None] * 6
                c = [
                    halo_control[0, order[0], here, lanes(part)],
                    halo_control[0, order[1], here, lanes(part)],
                    control_ref[own[2], here, lanes(part)],
                    control_ref[own[3], here, lanes(part)],
                ]
                for one in range(group):
                    share = share_ref[step * group + one]
                    start = side * span + one * chans + eight * 8
                    at = pl.ds(pl.multiple_of(start, 8), 8)
                    below = pl.ds(pl.multiple_of(2 * span + start, 8), 8)
                    b1 = halo[one, order[0], here, lanes(part)]
                    b2 = halo[one, order[1], here, lanes(part)]
                    a = [
                        near_ref[one, row, here, lanes(part)].astype(jnp.float32) for row in own
                    ]
                    y = [x * (share * k) for x, k in zip((b1, b2, a[2], a[3]), c)]
                    terms = (
                        a[0] * piece(mixed, at, part, 0),
                        a[1] * piece(mixed, at, part, 2 * LANES),
                        a[2] * (piece(alone, at, part, 0) + y[1]),
                        a[3] * y[0],
                        b1 * (piece(alone, below, part, 0) + y[3]),
                        b2 * y[2],
                    )
                    totals = [t if s is None else s + t for s, t in zip(totals, terms)]
                for i, value in enumerate(totals):
                    place = side * 6 + i
                    before = jnp.where(step == 0, 0.0, sums[place, here, lanes(part)])
                    sums[place, here, lanes(part)] = before + value
        return carry

    lax.fori_loop(0, chans // 8, per_chans, 0)

    def exact(y1, y2, y3, y4):
        wide = scaled(4.0, widen(y1, lane))
        inner = plus(widen(plus(wide, scaled(6.0, y2)), lane), scaled(12.0, y1))
        top = plus(widen(inner, lane), scaled(4.0, y2))
        next_row = plus(
            widen(plus(scaled(1.5, wide), scaled(4.0, y2)), lane), scaled(4.0, y1)
        )
        return top, next_row, plus(wide, y2), y1, plus(scaled(4.0, widen(y3, lane)), y4), y3

    @pl.when(final)
    def _():
        def finish(eight, carry):
            at = pl.ds(pl.multiple_of(eight * 8, 8), 8)
            slot = jnp.bitwise_xor(eight, place_ref[0])
            blend = blend_ref[at, :]
            for side, (halo, halo_control, order, own) in enumerate(sides):
                found = exact(
                    split_lanes(halo_control[0, order[0], at, :]),
                    split_lanes(halo_control[0, order[1], at, :]),
                    split_lanes(control_ref[own[2], at, :]),
                    split_lanes(control_ref[own[3], at, :]),
                )
                for i, value in enumerate(found):
                    place = side * 6 + i
                    for part in range(parts):
                        sums[place, at, lanes(part)] = SCALE * (
                            (1.0 - blend) * sums[place, at, lanes(part)]
                            + (0.25 * blend) * value[part]
                        )

            @pl.when(jnp.bitwise_and(slot, 1) == 0)
            def _():
                keep_ref[slot // 2] = sums[:, at, :]

            @pl.when(jnp.bitwise_and(slot, 1) == 1)
            def _():
                give_ref[slot // 2] = sums[:, at, :]

            return carry

        lax.fori_loop(0, chans // 8, finish, 0, unroll=2)


def cross_part(place, share, low, high, near, control_near, blend, group):
    count, rows, chans, width = near.shape
    halo = pl.BlockSpec((group, 2, chans, width), lambda i: (i, 0, 0, 0))
    halo_control = pl.BlockSpec((1, 2, chans, width), lambda i: (count, 0, 0, 0))
    half = (chans // 16, 12, 8, width)
    _, p1, p2, p3 = column_operators(width)
    left, right = stacked([p1, p2]), stacked([p2, p3])
    pair = jnp.asarray(np.concatenate([left, right], axis=2))
    single = jnp.asarray(stacked([p3]))
    span = 2 * group * chans
    return pl.pallas_call(
        cross_kernel,
        grid=(count // group,),
        in_specs=[
            pl.BlockSpec(memory_space=pltpu.SMEM),
            pl.BlockSpec(memory_space=pltpu.SMEM),
            halo,
            halo_control,
            halo,
            halo_control,
            pl.BlockSpec((group, rows, chans, width), lambda i: (i, 0, 0, 0)),
            pl.BlockSpec((rows, chans, width), lambda i: (0, 0, 0)),
            pl.BlockSpec((chans, LANES), lambda i: (0, 0)),
            pl.BlockSpec(pair.shape, lambda i: (0, 0, 0)),
            pl.BlockSpec(single.shape, lambda i: (0, 0, 0)),
        ],
        out_specs=[pl.BlockSpec(half, lambda i: (0, 0, 0, 0))] * 2,
        out_shape=[jax.ShapeDtypeStruct(half, jnp.float32)] * 2,
        scratch_shapes=[
            pltpu.VMEM((12, chans, width), jnp.float32),
            pltpu.VMEM((span, 4 * LANES), jnp.bfloat16),
            pltpu.VMEM((span, 4 * LANES), jnp.bfloat16),
            pltpu.VMEM((2 * span, 2 * LANES), jnp.bfloat16),
            pltpu.VMEM((2 * span, 2 * LANES), jnp.bfloat16),
            pltpu.VMEM((2, span, 4 * LANES), jnp.float32),
            pltpu.VMEM((2, 2 * span, 2 * LANES), jnp.float32),
        ],
        name="cross_part",
    )(place, share, low, low, high, high, near, control_near, blend, pair, single)


def sent_kernel(own_ref, got_ref, last_ref, cross_ref, cross_got_ref, cross_last_ref, up_ref, down_ref, turned):
    chans, rows, width = last_ref.shape
    whole = own_ref[0] + got_ref[0] + last_ref[...]
    for part in range(width // LANES):
        lanes = slice(part * LANES, (part + 1) * LANES)
        for chan in range(chans):
            turned[chan * PITCH : chan * PITCH + 8] = whole[chan, :8, lanes]
        first = turned[pl.ds(0, chans, stride=PITCH), :]

        def crossed(i):
            return cross_ref[0, i, :, lanes] + cross_got_ref[0, i, :, lanes] + cross_last_ref[i, :, lanes]

        for i in range(2):
            up_ref[i, :, lanes] = crossed(4 + i)
            down_ref[i, :, lanes] = crossed(10 + i)
        up_ref[2, :, lanes] = first + crossed(0)


def sent_rows(own, got, last, cross, cross_got, cross_last):
    chans, rows, width = last.shape
    one = lambda x: pl.BlockSpec((1,) + x.shape[1:], lambda i: (0, 0, 0, 0))
    vmem = pl.BlockSpec(memory_space=pltpu.VMEM)
    return pl.pallas_call(
        sent_kernel,
        grid=(1,),
        in_specs=[one(own), one(got), vmem, one(cross), one(cross_got), vmem],
        out_specs=[vmem, vmem],
        out_shape=[
            jax.ShapeDtypeStruct((3, chans, width), jnp.float32),
            jax.ShapeDtypeStruct((2, chans, width), jnp.float32),
        ],
        scratch_shapes=[pltpu.VMEM((chans * PITCH, LANES), jnp.float32)],
        name="sent_rows",
    )(own, got, last, cross, cross_got, cross_last)


def answer_kernel(
    place_ref, asked_ref, own_ref, got_ref, last_ref, cross_ref, cross_got_ref, cross_last_ref,
    below_ref, above_ref, out_ref, turned, pairs,
):
    chans, rows, width = last_ref.shape
    parts = width // LANES
    capacity = out_ref.shape[0] // asked_ref.shape[0]
    keep_high = (place_ref[2] != 0).astype(jnp.float32)
    whole = own_ref[0] + got_ref[0] + last_ref[...]
    for part in range(parts):
        for chan in range(chans):
            turned[part, chan * PITCH : chan * PITCH + rows] = whole[
                chan, :, part * LANES : (part + 1) * LANES
            ]

    def crossed(i, lanes):
        return cross_ref[0, i, :, lanes] + cross_got_ref[0, i, :, lanes] + cross_last_ref[i, :, lanes]

    for part in range(parts):
        lanes = slice(part * LANES, (part + 1) * LANES)
        for row in range(rows + 1):
            if row < rows:
                value = turned[part, pl.ds(row, chans, stride=PITCH), :]
            else:
                value = keep_high * (above_ref[2, :, lanes] + crossed(10, lanes))
            if row < 4:
                value += crossed(row, lanes)
            if rows - 4 <= row < rows:
                value += crossed(6 + rows - 1 - row, lanes)
            if row < 2:
                value += below_ref[row, :, lanes]
            if rows - 2 <= row < rows:
                value += above_ref[rows - 1 - row, :, lanes]
            if row < rows:
                pairs[part, pl.ds(row * 2 * chans, chans, stride=2), :] = value
            if row > 0:
                pairs[part, pl.ds((row - 1) * 2 * chans + 1, chans, stride=2), :] = value

    def one(device, carry):
        for slot in range(capacity):
            row = asked_ref[device, 0, slot]
            at = pl.ds(pl.multiple_of(row * (2 * chans), 2 * chans), 2 * chans)
            for part in range(parts):
                out_ref[device * capacity + slot, :, part * LANES : (part + 1) * LANES] = pairs[
                    part, at, :
                ]
        return carry

    lax.fori_loop(0, asked_ref.shape[0], one, 0, unroll=4)


def answers(place, asked, capacity, own, got, last, cross, cross_got, cross_last, below, above):
    chans, rows, width = last.shape
    slots = asked.shape[0] * capacity
    smem = pl.BlockSpec(memory_space=pltpu.SMEM)
    vmem = pl.BlockSpec(memory_space=pltpu.VMEM)
    one = lambda x: pl.BlockSpec((1,) + x.shape[1:], lambda i: (0, 0, 0, 0))
    return pl.pallas_call(
        answer_kernel,
        grid=(1,),
        in_specs=[smem, smem, one(own), one(got), vmem, one(cross), one(cross_got), vmem, vmem, vmem],
        out_specs=vmem,
        out_shape=jax.ShapeDtypeStruct((slots, 2 * chans, width), jnp.float32),
        scratch_shapes=[
            pltpu.VMEM((width // LANES, chans * PITCH, LANES), jnp.float32),
            pltpu.VMEM((width // LANES, rows * 2 * chans, LANES), jnp.float32),
        ],
        name="answers",
    )(place, asked, own, got, last, cross, cross_got, cross_last, below, above)


def fine_kernel(slot_ref, arrived_ref, index_ref, weight_ref, out_ref):
    blocks = index_ref.shape[0]
    pairs, width = arrived_ref.shape[1:]
    fine = index_ref.shape[2]
    half = LANES // 2
    quarter = half // 2
    lane = lax.broadcasted_iota(jnp.int32, (8, LANES), 1)
    even = lax.broadcasted_iota(jnp.int32, (8, LANES), 0) % 2 == 0

    def one(block, carry):
        slot = slot_ref[block]
        windows = []
        for group in range(pairs // 8):
            parts = []
            for part in split_lanes(arrived_ref[slot, pl.ds(group * 8, 8), :]):
                other = jnp.where(even, pltpu.roll(part, 7, 0), pltpu.roll(part, 1, 0))
                parts.append(0.75 * part + 0.25 * other)
            turned = {
                shift: [pltpu.roll(p, shift, 1) for p in parts]
                for shift in (quarter, LANES - quarter)
            }
            found = []
            for chunk in range(fine // LANES):
                part, ahead = divmod(chunk * half - quarter, LANES)
                rolled = turned[LANES - ahead]
                if part < 0:
                    found.append(rolled[part + 1])
                elif part + 1 == len(parts):
                    found.append(rolled[part])
                else:
                    found.append(
                        jnp.where(lane < LANES - ahead, rolled[part], rolled[part + 1])
                    )
            windows.append(found)
        for chunk in range(fine // LANES):
            lanes = slice(chunk * LANES, (chunk + 1) * LANES)
            index = index_ref[block, :, lanes]
            weight = weight_ref[block, :, lanes]
            for group in range(pairs // 8):
                near = windows[group][chunk]
                left = jnp.take_along_axis(near, index, axis=1)
                right = jnp.take_along_axis(near, index + 1, axis=1)
                value = (1.0 - weight) * left + weight * right
                out_ref[block, group * 4 : (group + 1) * 4, :, lanes] = value.reshape(4, 2, LANES)
        return carry

    lax.fori_loop(0, blocks, one, 0, unroll=4)


def fine_part(slot, arrived, index, weight):
    blocks, _, fine = index.shape
    chans = arrived.shape[1] // 2
    smem = pl.BlockSpec(memory_space=pltpu.SMEM)
    vmem = pl.BlockSpec(memory_space=pltpu.VMEM)
    return pl.pallas_call(
        fine_kernel,
        in_specs=[smem, vmem, vmem, vmem],
        out_specs=vmem,
        out_shape=jax.ShapeDtypeStruct((blocks, chans, 2, fine), jnp.float32),
        name="fine_part",
    )(slot, arrived, index, weight)


def column_kernel(source_ref, code_ref, index_ref, weight_ref):
    blocks, fine = source_ref.shape
    column = lax.broadcasted_iota(jnp.int32, (1, fine), 1)
    first = (column // LANES) * (LANES // 2) - LANES // 4
    for block in range(blocks):
        shape = index_ref.shape[1:]
        index_ref[block] = jnp.broadcast_to(source_ref[block : block + 1] - first, shape)
        weight_ref[block] = jnp.broadcast_to(
            code_ref[block : block + 1].astype(jnp.float32) * (1.0 / 16.0), shape
        )


def columns(source, code):
    blocks, fine = source.shape
    return pl.pallas_call(
        column_kernel,
        out_shape=[
            jax.ShapeDtypeStruct((blocks, 8, fine), jnp.int32),
            jax.ShapeDtypeStruct((blocks, 8, fine), jnp.float32),
        ],
        name="columns",
    )(source, code)


def per_device(
    members,
    control,
    hybrid_weight,
    member_weights,
    source_device,
    source_row,
    column_source,
    column_code,
):
    member_count, chans, row_count, width = members.shape
    spaces = lax.axis_size("space")
    space_index = lax.axis_index("space")
    member_slot = lax.axis_index("member")

    source_index = source_device[:, 0]
    capacity = max(2, 2 * row_count // spaces)
    chosen = (source_index[:, None] == jnp.arange(spaces, dtype=jnp.int32)[None, :]).astype(
        jnp.int32
    )
    earlier = jnp.cumsum(chosen, axis=0) - chosen
    rank_within = jnp.sum(earlier * chosen, axis=1)
    slot_index = source_index * capacity + rank_within
    spread = slot_index[None, :] - capacity * jnp.arange(spaces, dtype=jnp.int32)[:, None]
    lane = jnp.arange(LANES, dtype=jnp.int32)
    taken = (spread[:, None, :] == lane[None, :, None]) & (lane < capacity)[None, :, None]
    request = jnp.sum(jnp.where(taken, source_row[None, None, :], 0), axis=2)[:, None, :]
    asked = lax.all_to_all(request, "space", split_axis=0, concat_axis=0, tiled=True)
    top, bottom = edge_rows(members, control, 4)
    top, bottom, asked = lax.optimization_barrier((top, bottom, asked))
    high = passed_along(top, "space", -1)
    low = passed_along(bottom, "space", 1)

    place = jnp.stack(
        [
            member_slot,
            jnp.where(space_index == 0, 0, jnp.where(space_index == spaces - 1, 2, 1)),
            (space_index < spaces - 1).astype(jnp.int32),
        ]
    ).astype(jnp.int32)
    weight_codes = member_weights.astype(jnp.float32)
    share = lax.dynamic_slice_in_dim(
        weight_codes, member_slot * member_count, member_count
    ) / jnp.sum(weight_codes)
    blend = jnp.broadcast_to(hybrid_weight[:, None], (chans, LANES))
    index, weight = columns(column_source, column_code)

    own_keep, own_give, near, control_near = own_part(place, share, members, control, blend)
    own_got = swapped(own_give, "member", 1)
    own_last = swapped(own_keep[1] + own_got[1], "member", 2)
    near, own_last, index, weight, slot_index = lax.optimization_barrier(
        (near, own_last, index, weight, slot_index)
    )

    keep, give = cross_part(place, share, low, high, near, control_near, blend, 4)
    got = swapped(give, "member", 1)
    last = swapped(keep[1] + got[1], "member", 2)
    up, down = sent_rows(own_keep, own_got, own_last, keep, got, last)
    above = passed_along(up, "space", -1)
    below = passed_along(down, "space", 1)

    outgoing = answers(
        place, asked, capacity, own_keep, own_got, own_last, keep, got, last, below, above
    )
    pair_rows = outgoing.shape[1]
    arrived = lax.all_to_all(
        outgoing.reshape(spaces, capacity * pair_rows, width),
        "space",
        split_axis=0,
        concat_axis=0,
        tiled=True,
    ).reshape(spaces * capacity, pair_rows, width)
    return fine_part(slot_index, arrived, index, weight)


def solution(mesh):
    placed = (
        P("member", None, "space", None),
        P(None, "space", None),
        P(),
        P(),
        P("space", None),
        P("space"),
        P("space", None),
        P("space", None),
    )
    return jax.shard_map(
        per_device,
        mesh=mesh,
        in_specs=placed,
        out_specs=P("space", "member", None, None),
        check_vma=False,
    )
```

```python
import jax
import jax.numpy as jnp
import numpy as np
from jax import lax
from jax.experimental import pallas as pl
from jax.experimental.pallas import tpu as pltpu
from jax.sharding import PartitionSpec as P

SCALE = 1.0 / 625.0
LANES = 128
PITCH = 24


def passed_along(x, axis, by):
    length = lax.axis_size(axis)
    pairs = [(i, i + by) for i in range(length) if 0 <= i + by < length]
    return lax.ppermute(x, axis, pairs)


def swapped(x, axis, bit):
    length = lax.axis_size(axis)
    return lax.ppermute(x, axis, [(i, i ^ bit) for i in range(length)])


def split_lanes(x):
    return [x[:, i : i + LANES] for i in range(0, x.shape[-1], LANES)]


def side_sum(parts, lane):
    ahead = [pltpu.roll(p, 1, 1) for p in parts]
    behind = [pltpu.roll(p, LANES - 1, 1) for p in parts]
    out = []
    for i in range(len(parts)):
        left = jnp.where(lane == 0, ahead[i - 1] if i else 0.0, ahead[i])
        right = jnp.where(
            lane == LANES - 1, behind[i + 1] if i + 1 < len(parts) else 0.0, behind[i]
        )
        out.append(left + right)
    return out


def plus(a, b):
    return [p + q for p, q in zip(a, b)]


def scaled(factor, a):
    return [factor * p for p in a]


def widen(parts, lane):
    return plus(parts, side_sum(parts, lane))


def edges_kernel(members_ref, control_ref, top_ref, bottom_ref, scratch, top_out, bottom_out, sems):
    step = pl.program_id(0)
    steps = pl.num_programs(0)
    group = members_ref.shape[0]
    chans, rows = members_ref.shape[1:3]
    parts = scratch.shape[0]

    def copies(first, count, index):
        return [
            pltpu.make_async_copy(
                stage.at[pl.ds(first, count)], ref.at[pl.ds(first, count)], sems.at[side, index]
            )
            for side, (stage, ref) in enumerate(((top_out, top_ref), (bottom_out, bottom_ref)))
        ]

    def rows_out(wide, index):
        for part in range(parts):
            lanes = slice(part * LANES, (part + 1) * LANES)
            for chan in range(chans):
                scratch[part, chan * PITCH : chan * PITCH + rows] = wide[chan, :, lanes]
            for slot in range(2):
                for which, stage in ((slot, top_out), (rows - 2 + slot, bottom_out)):
                    stage[index, slot, :, lanes] = scratch[
                        part, pl.ds(which, chans, stride=PITCH), :
                    ]

    for one in range(group):
        rows_out(members_ref[one].astype(jnp.float32), step * group + one)
    for copy in copies(step * group, group, step):
        copy.start()

    @pl.when(step == steps - 1)
    def _():
        count = top_ref.shape[0] - 1
        rows_out(control_ref[...], count)
        for copy in copies(count, 1, count // group):
            copy.start()
        for index in range(count // group):
            for copy in copies(index * group, group, index):
                copy.wait()
        for copy in copies(count, 1, count // group):
            copy.wait()


def edge_rows(members, control, group):
    count, chans, rows, width = members.shape
    shape = (count + 1, 2, chans, width)
    out = jax.ShapeDtypeStruct(shape, jnp.float32)
    return pl.pallas_call(
        edges_kernel,
        grid=(count // group,),
        in_specs=[
            pl.BlockSpec((group, chans, rows, width), lambda i: (i, 0, 0, 0)),
            pl.BlockSpec((chans, rows, width), lambda i: (0, 0, 0)),
        ],
        out_specs=[pl.BlockSpec(memory_space=pl.ANY)] * 2,
        out_shape=[out, out],
        scratch_shapes=[
            pltpu.VMEM((width // LANES, chans * PITCH, LANES), jnp.float32),
            pltpu.VMEM(shape, jnp.float32),
            pltpu.VMEM(shape, jnp.float32),
            pltpu.SemaphoreType.DMA((2, count // group + 1)),
        ],
        name="edge_rows",
    )(members, control)


def column_operators(width):
    q = np.eye(width) + np.eye(width, k=1) + np.eye(width, k=-1)
    q2 = q @ q
    q3 = q2 @ q
    eye = np.eye(width)
    return q2 @ q2 + 12 * q2 + 6 * eye, 4 * q3 + 12 * q, 6 * q2 + 4 * eye, 4 * q


def windowed(operator):
    first = operator[:256, :256]
    second = operator[128:, 128:].copy()
    second[:128, :128] = 0.0
    return first, second


def stacked(operators):
    first, second = zip(*[windowed(op) for op in operators])
    return np.stack([np.concatenate(first), np.concatenate(second)]).astype(jnp.bfloat16)


def own_kernel(
    place_ref, share_ref, members_ref, control_ref, blend_ref, operator_ref,
    keep_ref, give_ref, near_ref, control_near_ref,
    total, scratch, *work,
):
    step = pl.program_id(0)
    both, chans, rows, width = members_ref.shape
    parts = width // LANES
    last = pl.num_programs(0) - 1
    static = step == last
    fields, firsts, seconds, mixes = [work[i * both : (i + 1) * both] for i in range(4)]
    ends = (0, 1, 2, 3, rows - 4, rows - 3, rows - 2, rows - 1)

    def lanes(part):
        return slice(part * LANES, (part + 1) * LANES)

    @pl.when(step == 0)
    def _():
        total[...] = jnp.zeros(total.shape, jnp.float32)
        for field in fields:
            field[...] = jnp.zeros(field.shape, jnp.float32)

    @pl.when(step < last)
    def _():
        for which, field in enumerate(fields):

            def fill(chan, carry):
                for part in range(parts):
                    state = members_ref[which, chan, :, lanes(part)].astype(jnp.float32)
                    field[part, chan, 8 : 8 + rows] = state * control_ref[chan, :, lanes(part)]
                    scratch[part, pl.ds(pl.multiple_of(chan * PITCH, 8), rows), :] = state
                return carry

            lax.fori_loop(0, chans, fill, 0, unroll=4)
            for place, row in enumerate(ends):
                for part in range(parts):
                    near_ref[which, place, :, lanes(part)] = scratch[
                        part, pl.ds(row, chans, stride=PITCH), :
                    ].astype(jnp.bfloat16)

    @pl.when(static)
    def _():
        def fill(chan, carry):
            for part in range(parts):
                block = control_ref[chan, :, lanes(part)]
                for field in fields:
                    field[part, chan, 8 : 8 + rows] = block
                scratch[part, pl.ds(pl.multiple_of(chan * PITCH, 8), rows), :] = block
            return carry

        lax.fori_loop(0, chans, fill, 0, unroll=4)
        for place, row in enumerate(ends):
            for part in range(parts):
                control_near_ref[place, :, lanes(part)] = scratch[
                    part, pl.ds(row, chans, stride=PITCH), :
                ]

    @pl.when(place_ref[1] == 0)
    def _():
        def image(chan, carry):
            for field in fields:
                for part in range(parts):
                    for row in range(3):
                        field[part, chan, 6 - row : 7 - row] = -field[
                            part, chan, 8 + row : 9 + row
                        ]
            return carry

        lax.fori_loop(0, chans, image, 0, unroll=4)

    @pl.when(place_ref[1] == 2)
    def _():
        def image(chan, carry):
            for field in fields:
                for part in range(parts):
                    for row in range(3):
                        field[part, chan, 9 + rows + row : 10 + rows + row] = -field[
                            part, chan, 7 + rows - row : 8 + rows - row
                        ]
            return carry

        lax.fori_loop(0, chans, image, 0, unroll=4)

    def at_distance(field, part, chan, distance):
        if distance == 0:
            return field[part, chan, 8 : 8 + rows]
        return (
            field[part, chan, 8 - distance : 8 - distance + rows]
            + field[part, chan, 8 + distance : 8 + distance + rows]
        )

    refine = jnp.where(static, 1.0, 0.0)

    def gather(which, chan):
        start = chan * rows
        at = pl.ds(start if isinstance(chan, int) else pl.multiple_of(start, rows), rows)
        for distance in range(4):
            base = distance * 2 * LANES
            for part in range(parts):
                value = at_distance(fields[which], part, chan, distance)
                if which:
                    value -= refine * value.astype(jnp.bfloat16).astype(jnp.float32)
                value = value.astype(jnp.bfloat16)
                if part < 2:
                    firsts[which][at, base + part * LANES : base + (part + 1) * LANES] = value
                if part > 0:
                    seconds[which][at, base + (part - 1) * LANES : base + part * LANES] = value

    def multiply(which):
        for window, ref in enumerate((firsts[which], seconds[which])):
            mixes[which][window] = jnp.dot(
                ref[...], operator_ref[window], preferred_element_type=jnp.float32
            )

    def collect(which, chan):
        at = pl.ds(chan * rows, rows)
        mixed = mixes[which]
        low = [mixed[0, at, lanes(0)], mixed[0, at, lanes(1)]]
        high = [mixed[1, at, lanes(0)], mixed[1, at, lanes(1)]]
        found = [low[0], low[1] + high[0], high[1]]
        blend = blend_ref[chan : chan + 1, :]
        share = share_ref[jnp.minimum(step, last - 1) * both + which]
        factor = jnp.where(static, 0.25 * blend, share)
        for part in range(parts):
            far = at_distance(fields[which], part, chan, 4)
            value = found[part] + (far if which == 0 else (1.0 - refine) * far)
            state = members_ref[which, chan, :, lanes(part)].astype(jnp.float32)
            state = jnp.where(static, 1.0, state)
            before = total[chan, :, lanes(part)]
            if which == 0:
                before = jnp.where(static, 1.0 - blend, 1.0) * before
            total[chan, :, lanes(part)] = before + (factor * state) * value

    def gather_four(group, carry):
        for inner in range(4):
            gather(0, group * 4 + inner)
        return carry

    lax.fori_loop(0, chans // 4, gather_four, 0)
    multiply(0)
    for chan in range(chans):
        gather(1, chan)
    multiply(1)
    for chan in range(chans):
        collect(0, chan)
    for chan in range(chans):
        collect(1, chan)

    @pl.when(static)
    def _():
        def one_group(group, carry):
            slot = jnp.bitwise_xor(group, place_ref[0])
            done = SCALE * total[pl.ds(pl.multiple_of(group * 8, 8), 8)]

            @pl.when(jnp.bitwise_and(slot, 1) == 0)
            def _():
                keep_ref[slot // 2] = done

            @pl.when(jnp.bitwise_and(slot, 1) == 1)
            def _():
                give_ref[slot // 2] = done

            return carry

        lax.fori_loop(0, chans // 8, one_group, 0)


def own_part(place, share, members, control, blend):
    count, chans, rows, width = members.shape
    parts = width // LANES
    both = 2
    steps = count // both
    operators = jnp.asarray(stacked(column_operators(width)))
    depth = operators.shape[1]
    half = (chans // 16, 8, rows, width)
    return pl.pallas_call(
        own_kernel,
        grid_spec=pltpu.PrefetchScalarGridSpec(
            num_scalar_prefetch=2,
            grid=(steps + 1,),
            in_specs=[
                pl.BlockSpec(
                    (both, chans, rows, width),
                    lambda i, place, share: (jnp.minimum(i, steps - 1), 0, 0, 0),
                ),
                pl.BlockSpec((chans, rows, width), lambda i, place, share: (0, 0, 0)),
                pl.BlockSpec((chans, LANES), lambda i, place, share: (0, 0)),
                pl.BlockSpec(operators.shape, lambda i, place, share: (0, 0, 0)),
            ],
            out_specs=[
                pl.BlockSpec(half, lambda i, place, share: (0, 0, 0, 0)),
                pl.BlockSpec(half, lambda i, place, share: (0, 0, 0, 0)),
                pl.BlockSpec(
                    (both, 8, chans, width),
                    lambda i, place, share: (jnp.minimum(i, steps - 1), 0, 0, 0),
                ),
                pl.BlockSpec((8, chans, width), lambda i, place, share: (0, 0, 0)),
            ],
            scratch_shapes=[
                pltpu.VMEM((chans, rows, width), jnp.float32),
                pltpu.VMEM((parts, chans * PITCH, LANES), jnp.float32),
            ]
            + [pltpu.VMEM((parts, chans, rows + 16, LANES), jnp.float32)] * both
            + [pltpu.VMEM((chans * rows, depth), jnp.bfloat16)] * (2 * both)
            + [pltpu.VMEM((2, chans * rows, 2 * LANES), jnp.float32)] * both,
        ),
        out_shape=[
            jax.ShapeDtypeStruct(half, jnp.float32),
            jax.ShapeDtypeStruct(half, jnp.float32),
            jax.ShapeDtypeStruct((count, 8, chans, width), jnp.bfloat16),
            jax.ShapeDtypeStruct((8, chans, width), jnp.float32),
        ],
        name="own_part",
    )(place, share, members, control, blend, operators)


def cross_kernel(
    place_ref, share_ref, low_ref, low_control_ref, high_ref, high_control_ref,
    near_ref, control_ref, blend_ref, pair_ref, single_ref,
    keep_ref, give_ref, sums, first, second, third, fourth, mixed, alone,
):
    step = pl.program_id(0)
    group = near_ref.shape[0]
    chans, width = near_ref.shape[2:]
    parts = width // LANES
    lane = lax.broadcasted_iota(jnp.int32, (8, LANES), 1)
    final = step == pl.num_programs(0) - 1
    span = group * chans
    sides = (
        (low_ref, low_control_ref, (1, 0), (0, 1, 2, 3)),
        (high_ref, high_control_ref, (0, 1), (7, 6, 5, 4)),
    )

    def lanes(part, base=0):
        return slice(base + part * LANES, base + (part + 1) * LANES)

    for side, (halo, halo_control, order, own) in enumerate(sides):
        for one in range(group):
            share = share_ref[step * group + one]
            at = slice(side * span + one * chans, side * span + (one + 1) * chans)
            below = slice(2 * span + at.start, 2 * span + at.stop)
            for part in range(parts):
                y1, y2 = [
                    (
                        halo[one, slot, :, lanes(part)]
                        * (share * halo_control[0, slot, :, lanes(part)])
                    ).astype(jnp.bfloat16)
                    for slot in order
                ]
                y3 = (
                    near_ref[one, own[2], :, lanes(part)].astype(jnp.float32)
                    * (share * control_ref[own[2], :, lanes(part)])
                ).astype(jnp.bfloat16)
                if part < 2:
                    first[at, lanes(part)] = y1
                    first[at, lanes(part, 2 * LANES)] = y2
                    third[at, lanes(part)] = y1
                    third[below, lanes(part)] = y3
                if part > 0:
                    second[at, lanes(part - 1)] = y1
                    second[at, lanes(part - 1, 2 * LANES)] = y2
                    fourth[at, lanes(part - 1)] = y1
                    fourth[below, lanes(part - 1)] = y3
    mixed[0] = jnp.dot(first[...], pair_ref[0], preferred_element_type=jnp.float32)
    mixed[1] = jnp.dot(second[...], pair_ref[1], preferred_element_type=jnp.float32)
    alone[0] = jnp.dot(third[...], single_ref[0], preferred_element_type=jnp.float32)
    alone[1] = jnp.dot(fourth[...], single_ref[1], preferred_element_type=jnp.float32)

    def piece(ref, at, part, base):
        if part == 0:
            return ref[0, at, lanes(0, base)]
        if part == parts - 1:
            return ref[1, at, lanes(1, base)]
        return ref[0, at, lanes(1, base)] + ref[1, at, lanes(0, base)]

    def per_chans(eight, carry):
        here = pl.ds(pl.multiple_of(eight * 8, 8), 8)
        for side, (halo, halo_control, order, own) in enumerate(sides):
            for part in range(parts):
                totals = [None] * 6
                c = [
                    halo_control[0, order[0], here, lanes(part)],
                    halo_control[0, order[1], here, lanes(part)],
                    control_ref[own[2], here, lanes(part)],
                    control_ref[own[3], here, lanes(part)],
                ]
                for one in range(group):
                    share = share_ref[step * group + one]
                    start = side * span + one * chans + eight * 8
                    at = pl.ds(pl.multiple_of(start, 8), 8)
                    below = pl.ds(pl.multiple_of(2 * span + start, 8), 8)
                    b1 = halo[one, order[0], here, lanes(part)]
                    b2 = halo[one, order[1], here, lanes(part)]
                    a = [
                        near_ref[one, row, here, lanes(part)].astype(jnp.float32) for row in own
                    ]
                    y = [x * (share * k) for x, k in zip((b1, b2, a[2], a[3]), c)]
                    terms = (
                        a[0] * piece(mixed, at, part, 0),
                        a[1] * piece(mixed, at, part, 2 * LANES),
                        a[2] * (piece(alone, at, part, 0) + y[1]),
                        a[3] * y[0],
                        b1 * (piece(alone, below, part, 0) + y[3]),
                        b2 * y[2],
                    )
                    totals = [t if s is None else s + t for s, t in zip(totals, terms)]
                for i, value in enumerate(totals):
                    place = side * 6 + i
                    before = jnp.where(step == 0, 0.0, sums[place, here, lanes(part)])
                    sums[place, here, lanes(part)] = before + value
        return carry

    lax.fori_loop(0, chans // 8, per_chans, 0)

    def exact(y1, y2, y3, y4):
        wide = scaled(4.0, widen(y1, lane))
        inner = plus(widen(plus(wide, scaled(6.0, y2)), lane), scaled(12.0, y1))
        top = plus(widen(inner, lane), scaled(4.0, y2))
        next_row = plus(
            widen(plus(scaled(1.5, wide), scaled(4.0, y2)), lane), scaled(4.0, y1)
        )
        return top, next_row, plus(wide, y2), y1, plus(scaled(4.0, widen(y3, lane)), y4), y3

    @pl.when(final)
    def _():
        def finish(eight, carry):
            at = pl.ds(pl.multiple_of(eight * 8, 8), 8)
            slot = jnp.bitwise_xor(eight, place_ref[0])
            blend = blend_ref[at, :]
            for side, (halo, halo_control, order, own) in enumerate(sides):
                found = exact(
                    split_lanes(halo_control[0, order[0], at, :]),
                    split_lanes(halo_control[0, order[1], at, :]),
                    split_lanes(control_ref[own[2], at, :]),
                    split_lanes(control_ref[own[3], at, :]),
                )
                for i, value in enumerate(found):
                    place = side * 6 + i
                    for part in range(parts):
                        sums[place, at, lanes(part)] = SCALE * (
                            (1.0 - blend) * sums[place, at, lanes(part)]
                            + (0.25 * blend) * value[part]
                        )

            @pl.when(jnp.bitwise_and(slot, 1) == 0)
            def _():
                keep_ref[slot // 2] = sums[:, at, :]

            @pl.when(jnp.bitwise_and(slot, 1) == 1)
            def _():
                give_ref[slot // 2] = sums[:, at, :]

            return carry

        lax.fori_loop(0, chans // 8, finish, 0, unroll=2)


def cross_part(place, share, low, high, near, control_near, blend, group):
    count, rows, chans, width = near.shape
    halo = pl.BlockSpec((group, 2, chans, width), lambda i: (i, 0, 0, 0))
    halo_control = pl.BlockSpec((1, 2, chans, width), lambda i: (count, 0, 0, 0))
    half = (chans // 16, 12, 8, width)
    _, p1, p2, p3 = column_operators(width)
    left, right = stacked([p1, p2]), stacked([p2, p3])
    pair = jnp.asarray(np.concatenate([left, right], axis=2))
    single = jnp.asarray(stacked([p3]))
    span = 2 * group * chans
    return pl.pallas_call(
        cross_kernel,
        grid=(count // group,),
        in_specs=[
            pl.BlockSpec(memory_space=pltpu.SMEM),
            pl.BlockSpec(memory_space=pltpu.SMEM),
            halo,
            halo_control,
            halo,
            halo_control,
            pl.BlockSpec((group, rows, chans, width), lambda i: (i, 0, 0, 0)),
            pl.BlockSpec((rows, chans, width), lambda i: (0, 0, 0)),
            pl.BlockSpec((chans, LANES), lambda i: (0, 0)),
            pl.BlockSpec(pair.shape, lambda i: (0, 0, 0)),
            pl.BlockSpec(single.shape, lambda i: (0, 0, 0)),
        ],
        out_specs=[pl.BlockSpec(half, lambda i: (0, 0, 0, 0))] * 2,
        out_shape=[jax.ShapeDtypeStruct(half, jnp.float32)] * 2,
        scratch_shapes=[
            pltpu.VMEM((12, chans, width), jnp.float32),
            pltpu.VMEM((span, 4 * LANES), jnp.bfloat16),
            pltpu.VMEM((span, 4 * LANES), jnp.bfloat16),
            pltpu.VMEM((2 * span, 2 * LANES), jnp.bfloat16),
            pltpu.VMEM((2 * span, 2 * LANES), jnp.bfloat16),
            pltpu.VMEM((2, span, 4 * LANES), jnp.float32),
            pltpu.VMEM((2, 2 * span, 2 * LANES), jnp.float32),
        ],
        name="cross_part",
    )(place, share, low, low, high, high, near, control_near, blend, pair, single)


def sent_kernel(own_ref, got_ref, last_ref, cross_ref, cross_got_ref, cross_last_ref, up_ref, down_ref, turned):
    chans, _, width = last_ref.shape
    whole = own_ref[0] + got_ref[0] + last_ref[...]
    for part in range(width // LANES):
        lanes = slice(part * LANES, (part + 1) * LANES)
        for chan in range(chans):
            turned[chan * PITCH : chan * PITCH + 8] = whole[chan, :8, lanes]
        first = turned[pl.ds(0, chans, stride=PITCH), :]

        def crossed(i):
            return cross_ref[0, i, :, lanes] + cross_got_ref[0, i, :, lanes] + cross_last_ref[i, :, lanes]

        for i in range(2):
            up_ref[i, :, lanes] = crossed(4 + i)
            down_ref[i, :, lanes] = crossed(10 + i)
        up_ref[2, :, lanes] = first + crossed(0)


def sent_rows(own, got, last, cross, cross_got, cross_last):
    chans, _, width = last.shape
    one = lambda x: pl.BlockSpec((1,) + x.shape[1:], lambda i: (0, 0, 0, 0))
    vmem = pl.BlockSpec(memory_space=pltpu.VMEM)
    return pl.pallas_call(
        sent_kernel,
        grid=(1,),
        in_specs=[one(own), one(got), vmem, one(cross), one(cross_got), vmem],
        out_specs=[vmem, vmem],
        out_shape=[
            jax.ShapeDtypeStruct((3, chans, width), jnp.float32),
            jax.ShapeDtypeStruct((2, chans, width), jnp.float32),
        ],
        scratch_shapes=[pltpu.VMEM((chans * PITCH, LANES), jnp.float32)],
        name="sent_rows",
    )(own, got, last, cross, cross_got, cross_last)


def answer_kernel(
    place_ref, asked_ref, own_ref, got_ref, last_ref, cross_ref, cross_got_ref, cross_last_ref,
    below_ref, above_ref, out_ref, turned, pairs,
):
    chans, rows, width = last_ref.shape
    parts = width // LANES
    capacity = out_ref.shape[0] // asked_ref.shape[0]
    keep_high = (place_ref[2] != 0).astype(jnp.float32)
    whole = own_ref[0] + got_ref[0] + last_ref[...]
    for part in range(parts):
        for chan in range(chans):
            turned[part, chan * PITCH : chan * PITCH + rows] = whole[
                chan, :, part * LANES : (part + 1) * LANES
            ]

    def crossed(i, lanes):
        return cross_ref[0, i, :, lanes] + cross_got_ref[0, i, :, lanes] + cross_last_ref[i, :, lanes]

    for part in range(parts):
        lanes = slice(part * LANES, (part + 1) * LANES)
        for row in range(rows + 1):
            if row < rows:
                value = turned[part, pl.ds(row, chans, stride=PITCH), :]
            else:
                value = keep_high * (above_ref[2, :, lanes] + crossed(10, lanes))
            if row < 4:
                value += crossed(row, lanes)
            if rows - 4 <= row < rows:
                value += crossed(6 + rows - 1 - row, lanes)
            if row < 2:
                value += below_ref[row, :, lanes]
            if rows - 2 <= row < rows:
                value += above_ref[rows - 1 - row, :, lanes]
            if row < rows:
                pairs[part, pl.ds(row * 2 * chans, chans, stride=2), :] = value
            if row > 0:
                pairs[part, pl.ds((row - 1) * 2 * chans + 1, chans, stride=2), :] = value

    def one(device, carry):
        for slot in range(capacity):
            row = asked_ref[device, 0, slot]
            at = pl.ds(pl.multiple_of(row * (2 * chans), 2 * chans), 2 * chans)
            for part in range(parts):
                out_ref[device * capacity + slot, :, part * LANES : (part + 1) * LANES] = pairs[
                    part, at, :
                ]
        return carry

    lax.fori_loop(0, asked_ref.shape[0], one, 0, unroll=4)


def answers(place, asked, capacity, own, got, last, cross, cross_got, cross_last, below, above):
    chans, rows, width = last.shape
    slots = asked.shape[0] * capacity
    smem = pl.BlockSpec(memory_space=pltpu.SMEM)
    vmem = pl.BlockSpec(memory_space=pltpu.VMEM)
    one = lambda x: pl.BlockSpec((1,) + x.shape[1:], lambda i: (0, 0, 0, 0))
    return pl.pallas_call(
        answer_kernel,
        grid=(1,),
        in_specs=[smem, smem, one(own), one(got), vmem, one(cross), one(cross_got), vmem, vmem, vmem],
        out_specs=vmem,
        out_shape=jax.ShapeDtypeStruct((slots, 2 * chans, width), jnp.float32),
        scratch_shapes=[
            pltpu.VMEM((width // LANES, chans * PITCH, LANES), jnp.float32),
            pltpu.VMEM((width // LANES, rows * 2 * chans, LANES), jnp.float32),
        ],
        name="answers",
    )(place, asked, own, got, last, cross, cross_got, cross_last, below, above)


def fine_kernel(slot_ref, arrived_ref, index_ref, weight_ref, out_ref):
    blocks = index_ref.shape[0]
    pairs, _ = arrived_ref.shape[1:]
    fine = index_ref.shape[2]
    half = LANES // 2
    quarter = half // 2
    lane = lax.broadcasted_iota(jnp.int32, (8, LANES), 1)
    even = lax.broadcasted_iota(jnp.int32, (8, LANES), 0) % 2 == 0

    def one(block, carry):
        slot = slot_ref[block]
        windows = []
        for group in range(pairs // 8):
            parts = []
            for part in split_lanes(arrived_ref[slot, pl.ds(group * 8, 8), :]):
                other = jnp.where(even, pltpu.roll(part, 7, 0), pltpu.roll(part, 1, 0))
                parts.append(0.75 * part + 0.25 * other)
            turned = {
                shift: [pltpu.roll(p, shift, 1) for p in parts]
                for shift in (quarter, LANES - quarter)
            }
            found = []
            for chunk in range(fine // LANES):
                part, ahead = divmod(chunk * half - quarter, LANES)
                rolled = turned[LANES - ahead]
                if part < 0:
                    found.append(rolled[part + 1])
                elif part + 1 == len(parts):
                    found.append(rolled[part])
                else:
                    found.append(
                        jnp.where(lane < LANES - ahead, rolled[part], rolled[part + 1])
                    )
            windows.append(found)
        for chunk in range(fine // LANES):
            lanes = slice(chunk * LANES, (chunk + 1) * LANES)
            index = index_ref[block, :, lanes]
            weight = weight_ref[block, :, lanes]
            for group in range(pairs // 8):
                near = windows[group][chunk]
                left = jnp.take_along_axis(near, index, axis=1)
                right = jnp.take_along_axis(near, index + 1, axis=1)
                value = (1.0 - weight) * left + weight * right
                out_ref[block, group * 4 : (group + 1) * 4, :, lanes] = value.reshape(4, 2, LANES)
        return carry

    lax.fori_loop(0, blocks, one, 0, unroll=4)


def fine_part(slot, arrived, index, weight):
    blocks, _, fine = index.shape
    chans = arrived.shape[1] // 2
    smem = pl.BlockSpec(memory_space=pltpu.SMEM)
    vmem = pl.BlockSpec(memory_space=pltpu.VMEM)
    return pl.pallas_call(
        fine_kernel,
        in_specs=[smem, vmem, vmem, vmem],
        out_specs=vmem,
        out_shape=jax.ShapeDtypeStruct((blocks, chans, 2, fine), jnp.float32),
        name="fine_part",
    )(slot, arrived, index, weight)


def column_kernel(source_ref, code_ref, index_ref, weight_ref):
    blocks, fine = source_ref.shape
    column = lax.broadcasted_iota(jnp.int32, (1, fine), 1)
    first = (column // LANES) * (LANES // 2) - LANES // 4
    for block in range(blocks):
        shape = index_ref.shape[1:]
        index_ref[block] = jnp.broadcast_to(source_ref[block : block + 1] - first, shape)
        weight_ref[block] = jnp.broadcast_to(
            code_ref[block : block + 1].astype(jnp.float32) * (1.0 / 16.0), shape
        )


def columns(source, code):
    blocks, fine = source.shape
    return pl.pallas_call(
        column_kernel,
        out_shape=[
            jax.ShapeDtypeStruct((blocks, 8, fine), jnp.int32),
            jax.ShapeDtypeStruct((blocks, 8, fine), jnp.float32),
        ],
        name="columns",
    )(source, code)


def per_device(
    members,
    control,
    hybrid_weight,
    member_weights,
    source_device,
    source_row,
    column_source,
    column_code,
):
    member_count, chans, row_count, width = members.shape
    spaces = lax.axis_size("space")
    space_index = lax.axis_index("space")
    member_slot = lax.axis_index("member")

    top, bottom = edge_rows(members, control, 4)
    high = passed_along(top, "space", -1)
    low = passed_along(bottom, "space", 1)

    place = jnp.stack(
        [
            member_slot,
            jnp.where(space_index == 0, 0, jnp.where(space_index == spaces - 1, 2, 1)),
            (space_index < spaces - 1).astype(jnp.int32),
        ]
    ).astype(jnp.int32)
    weight_codes = member_weights.astype(jnp.float32)
    share = lax.dynamic_slice_in_dim(
        weight_codes, member_slot * member_count, member_count
    ) / jnp.sum(weight_codes)
    blend = jnp.broadcast_to(hybrid_weight[:, None], (chans, LANES))
    source_index = source_device[:, 0]
    capacity = max(2, 2 * row_count // spaces)
    chosen = (source_index[:, None] == jnp.arange(spaces, dtype=jnp.int32)[None, :]).astype(
        jnp.int32
    )
    earlier = jnp.cumsum(chosen, axis=0) - chosen
    rank_within = jnp.sum(earlier * chosen, axis=1)
    slot_index = source_index * capacity + rank_within
    spread = slot_index[None, :] - capacity * jnp.arange(spaces, dtype=jnp.int32)[:, None]
    lane = jnp.arange(LANES, dtype=jnp.int32)
    taken = (spread[:, None, :] == lane[None, :, None]) & (lane < capacity)[None, :, None]
    request = jnp.sum(jnp.where(taken, source_row[None, None, :], 0), axis=2)[:, None, :]
    index, weight = columns(column_source, column_code)

    own_keep, own_give, near, control_near = own_part(place, share, members, control, blend)
    own_give, request = lax.optimization_barrier((own_give, request))
    asked = lax.all_to_all(request, "space", split_axis=0, concat_axis=0, tiled=True)
    own_got = swapped(own_give, "member", 1)
    own_last = swapped(own_keep[1] + own_got[1], "member", 2)
    near, index, weight, slot_index = lax.optimization_barrier((near, index, weight, slot_index))

    keep, give = cross_part(place, share, low, high, near, control_near, blend, 4)
    got = swapped(give, "member", 1)
    last = swapped(keep[1] + got[1], "member", 2)
    up, down = sent_rows(own_keep, own_got, own_last, keep, got, last)
    above = passed_along(up, "space", -1)
    below = passed_along(down, "space", 1)

    outgoing = answers(
        place, asked, capacity, own_keep, own_got, own_last, keep, got, last, below, above
    )
    pair_rows = outgoing.shape[1]
    arrived = lax.all_to_all(
        outgoing.reshape(spaces, capacity * pair_rows, width),
        "space",
        split_axis=0,
        concat_axis=0,
        tiled=True,
    ).reshape(spaces * capacity, pair_rows, width)
    return fine_part(slot_index, arrived, index, weight)


def solution(mesh):
    placed = (
        P("member", None, "space", None),
        P(None, "space", None),
        P(),
        P(),
        P("space", None),
        P("space"),
        P("space", None),
        P("space", None),
    )

    return jax.shard_map(
        per_device,
        mesh=mesh,
        in_specs=placed,
        out_specs=P("space", "member", None, None),
        check_vma=False,
    )
```

```python
import jax
import jax.numpy as jnp
import numpy as np
from jax import lax
from jax.experimental import pallas as pl
from jax.experimental.pallas import tpu as pltpu
from jax.sharding import PartitionSpec as P

SCALE = 1.0 / 625.0
LANES = 128
PITCH = 24


def paired(x, axis, first):
    length = lax.axis_size(axis)
    pairs = []
    for low in range(first, length - 1, 2):
        pairs += [(low, low + 1), (low + 1, low)]
    return lax.ppermute(x, axis, pairs)


def swapped(x, axis, bit):
    length = lax.axis_size(axis)
    return lax.ppermute(x, axis, [(i, i ^ bit) for i in range(length)])


def split_lanes(x):
    return [x[:, i : i + LANES] for i in range(0, x.shape[-1], LANES)]


def side_sum(parts, lane):
    ahead = [pltpu.roll(p, 1, 1) for p in parts]
    behind = [pltpu.roll(p, LANES - 1, 1) for p in parts]
    out = []
    for i in range(len(parts)):
        left = jnp.where(lane == 0, ahead[i - 1] if i else 0.0, ahead[i])
        right = jnp.where(
            lane == LANES - 1, behind[i + 1] if i + 1 < len(parts) else 0.0, behind[i]
        )
        out.append(left + right)
    return out


def plus(a, b):
    return [p + q for p, q in zip(a, b)]


def scaled(factor, a):
    return [factor * p for p in a]


def widen(parts, lane):
    return plus(parts, side_sum(parts, lane))


def edges_kernel(place_ref, members_ref, control_ref, a_ref, b_ref, scratch, stage, sems):
    step = pl.program_id(0)
    steps = pl.num_programs(0)
    group = members_ref.shape[0]
    chans, rows = members_ref.shape[1:3]
    parts = scratch.shape[0]
    odd = place_ref[3]

    def copies(first, count, index):
        return [
            pltpu.make_async_copy(
                stage.at[side, pl.ds(first, count)], ref.at[pl.ds(first, count)], sems.at[side, index]
            )
            for side, ref in enumerate((a_ref, b_ref))
        ]

    def rows_out(wide, index):
        for part in range(parts):
            lanes = slice(part * LANES, (part + 1) * LANES)
            for chan in range(chans):
                scratch[part, chan * PITCH : chan * PITCH + rows] = wide[chan, :, lanes]
            for slot in range(2):
                for which, side in ((slot, 1 - odd), (rows - 1 - slot, odd)):
                    stage[side, index, slot, :, lanes] = scratch[
                        part, pl.ds(which, chans, stride=PITCH), :
                    ]

    for one in range(group):
        rows_out(members_ref[one].astype(jnp.float32), step * group + one)
    for copy in copies(step * group, group, step):
        copy.start()

    @pl.when(step == steps - 1)
    def _():
        count = a_ref.shape[0] - 1
        rows_out(control_ref[...], count)
        for copy in copies(count, 1, count // group):
            copy.start()
        for index in range(count // group):
            for copy in copies(index * group, group, index):
                copy.wait()
        for copy in copies(count, 1, count // group):
            copy.wait()


def edge_rows(place, members, control, group):
    count, chans, rows, width = members.shape
    shape = (count + 1, 2, chans, width)
    out = jax.ShapeDtypeStruct(shape, jnp.float32)
    return pl.pallas_call(
        edges_kernel,
        grid=(count // group,),
        in_specs=[
            pl.BlockSpec(memory_space=pltpu.SMEM),
            pl.BlockSpec((group, chans, rows, width), lambda i: (i, 0, 0, 0)),
            pl.BlockSpec((chans, rows, width), lambda i: (0, 0, 0)),
        ],
        out_specs=[pl.BlockSpec(memory_space=pl.ANY)] * 2,
        out_shape=[out, out],
        scratch_shapes=[
            pltpu.VMEM((width // LANES, chans * PITCH, LANES), jnp.float32),
            pltpu.VMEM((2,) + shape, jnp.float32),
            pltpu.SemaphoreType.DMA((2, count // group + 1)),
        ],
        name="edge_rows",
    )(place, members, control)


def column_operators(width):
    q = np.eye(width) + np.eye(width, k=1) + np.eye(width, k=-1)
    q2 = q @ q
    q3 = q2 @ q
    eye = np.eye(width)
    return q2 @ q2 + 12 * q2 + 6 * eye, 4 * q3 + 12 * q, 6 * q2 + 4 * eye, 4 * q


def windowed(operator):
    first = operator[:256, :256]
    second = operator[128:, 128:].copy()
    second[:128, :128] = 0.0
    return first, second


def stacked(operators):
    first, second = zip(*[windowed(op) for op in operators])
    return np.stack([np.concatenate(first), np.concatenate(second)]).astype(jnp.bfloat16)


def own_kernel(
    place_ref, share_ref, members_ref, control_ref, blend_ref, operator_ref,
    keep_ref, give_ref, near_ref, control_near_ref,
    total, scratch, *work,
):
    step = pl.program_id(0)
    both, chans, rows, width = members_ref.shape
    parts = width // LANES
    last = pl.num_programs(0) - 1
    static = step == last
    fields, firsts, seconds, mixes = [work[i * both : (i + 1) * both] for i in range(4)]
    odd = place_ref[3]
    ends = [(4 * (1 - odd) + i, i) for i in range(4)]
    ends += [(4 * odd + i, rows - 1 - i) for i in range(4)]

    def lanes(part):
        return slice(part * LANES, (part + 1) * LANES)

    @pl.when(step == 0)
    def _():
        total[...] = jnp.zeros(total.shape, jnp.float32)
        for field in fields:
            field[...] = jnp.zeros(field.shape, jnp.float32)

    @pl.when(step < last)
    def _():
        for which, field in enumerate(fields):

            def fill(chan, carry):
                for part in range(parts):
                    state = members_ref[which, chan, :, lanes(part)].astype(jnp.float32)
                    field[part, chan, 8 : 8 + rows] = state * control_ref[chan, :, lanes(part)]
                    scratch[part, pl.ds(pl.multiple_of(chan * PITCH, 8), rows), :] = state
                return carry

            lax.fori_loop(0, chans, fill, 0, unroll=4)
            for place, row in ends:
                for part in range(parts):
                    near_ref[which, place, :, lanes(part)] = scratch[
                        part, pl.ds(row, chans, stride=PITCH), :
                    ].astype(jnp.bfloat16)

    @pl.when(static)
    def _():
        def fill(chan, carry):
            for part in range(parts):
                block = control_ref[chan, :, lanes(part)]
                for field in fields:
                    field[part, chan, 8 : 8 + rows] = block
                scratch[part, pl.ds(pl.multiple_of(chan * PITCH, 8), rows), :] = block
            return carry

        lax.fori_loop(0, chans, fill, 0, unroll=4)
        for place, row in ends:
            for part in range(parts):
                control_near_ref[place, :, lanes(part)] = scratch[
                    part, pl.ds(row, chans, stride=PITCH), :
                ]

    @pl.when(place_ref[1] == 0)
    def _():
        def image(chan, carry):
            for field in fields:
                for part in range(parts):
                    for row in range(3):
                        field[part, chan, 6 - row : 7 - row] = -field[
                            part, chan, 8 + row : 9 + row
                        ]
            return carry

        lax.fori_loop(0, chans, image, 0, unroll=4)

    @pl.when(place_ref[1] == 2)
    def _():
        def image(chan, carry):
            for field in fields:
                for part in range(parts):
                    for row in range(3):
                        field[part, chan, 9 + rows + row : 10 + rows + row] = -field[
                            part, chan, 7 + rows - row : 8 + rows - row
                        ]
            return carry

        lax.fori_loop(0, chans, image, 0, unroll=4)

    def at_distance(field, part, chan, distance):
        if distance == 0:
            return field[part, chan, 8 : 8 + rows]
        return (
            field[part, chan, 8 - distance : 8 - distance + rows]
            + field[part, chan, 8 + distance : 8 + distance + rows]
        )

    refine = jnp.where(static, 1.0, 0.0)

    def gather(which, chan):
        start = chan * rows
        at = pl.ds(start if isinstance(chan, int) else pl.multiple_of(start, rows), rows)
        for distance in range(4):
            base = distance * 2 * LANES
            for part in range(parts):
                value = at_distance(fields[which], part, chan, distance)
                if which:
                    value -= refine * value.astype(jnp.bfloat16).astype(jnp.float32)
                value = value.astype(jnp.bfloat16)
                if part < 2:
                    firsts[which][at, base + part * LANES : base + (part + 1) * LANES] = value
                if part > 0:
                    seconds[which][at, base + (part - 1) * LANES : base + part * LANES] = value

    def multiply(which):
        for window, ref in enumerate((firsts[which], seconds[which])):
            mixes[which][window] = jnp.dot(
                ref[...], operator_ref[window], preferred_element_type=jnp.float32
            )

    def collect(which, chan):
        at = pl.ds(chan * rows, rows)
        mixed = mixes[which]
        low = [mixed[0, at, lanes(0)], mixed[0, at, lanes(1)]]
        high = [mixed[1, at, lanes(0)], mixed[1, at, lanes(1)]]
        found = [low[0], low[1] + high[0], high[1]]
        blend = blend_ref[chan : chan + 1, :]
        share = share_ref[jnp.minimum(step, last - 1) * both + which]
        factor = jnp.where(static, 0.25 * blend, share)
        for part in range(parts):
            far = at_distance(fields[which], part, chan, 4)
            value = found[part] + (far if which == 0 else (1.0 - refine) * far)
            state = members_ref[which, chan, :, lanes(part)].astype(jnp.float32)
            state = jnp.where(static, 1.0, state)
            before = total[chan, :, lanes(part)]
            if which == 0:
                before = jnp.where(static, 1.0 - blend, 1.0) * before
            total[chan, :, lanes(part)] = before + (factor * state) * value

    def gather_four(group, carry):
        for inner in range(4):
            gather(0, group * 4 + inner)
        return carry

    lax.fori_loop(0, chans // 4, gather_four, 0)
    multiply(0)
    for chan in range(chans):
        gather(1, chan)
    multiply(1)
    for chan in range(chans):
        collect(0, chan)
    for chan in range(chans):
        collect(1, chan)

    @pl.when(static)
    def _():
        def one_group(group, carry):
            slot = jnp.bitwise_xor(group, place_ref[0])
            done = SCALE * total[pl.ds(pl.multiple_of(group * 8, 8), 8)]

            @pl.when(jnp.bitwise_and(slot, 1) == 0)
            def _():
                keep_ref[slot // 2] = done

            @pl.when(jnp.bitwise_and(slot, 1) == 1)
            def _():
                give_ref[slot // 2] = done

            return carry

        lax.fori_loop(0, chans // 8, one_group, 0)


def own_part(place, share, members, control, blend):
    count, chans, rows, width = members.shape
    parts = width // LANES
    both = 2
    steps = count // both
    operators = jnp.asarray(stacked(column_operators(width)))
    depth = operators.shape[1]
    half = (chans // 16, 8, rows, width)
    return pl.pallas_call(
        own_kernel,
        grid_spec=pltpu.PrefetchScalarGridSpec(
            num_scalar_prefetch=2,
            grid=(steps + 1,),
            in_specs=[
                pl.BlockSpec(
                    (both, chans, rows, width),
                    lambda i, place, share: (jnp.minimum(i, steps - 1), 0, 0, 0),
                ),
                pl.BlockSpec((chans, rows, width), lambda i, place, share: (0, 0, 0)),
                pl.BlockSpec((chans, LANES), lambda i, place, share: (0, 0)),
                pl.BlockSpec(operators.shape, lambda i, place, share: (0, 0, 0)),
            ],
            out_specs=[
                pl.BlockSpec(half, lambda i, place, share: (0, 0, 0, 0)),
                pl.BlockSpec(half, lambda i, place, share: (0, 0, 0, 0)),
                pl.BlockSpec(
                    (both, 8, chans, width),
                    lambda i, place, share: (jnp.minimum(i, steps - 1), 0, 0, 0),
                ),
                pl.BlockSpec((8, chans, width), lambda i, place, share: (0, 0, 0)),
            ],
            scratch_shapes=[
                pltpu.VMEM((chans, rows, width), jnp.float32),
                pltpu.VMEM((parts, chans * PITCH, LANES), jnp.float32),
            ]
            + [pltpu.VMEM((parts, chans, rows + 16, LANES), jnp.float32)] * both
            + [pltpu.VMEM((chans * rows, depth), jnp.bfloat16)] * (2 * both)
            + [pltpu.VMEM((2, chans * rows, 2 * LANES), jnp.float32)] * both,
        ),
        out_shape=[
            jax.ShapeDtypeStruct(half, jnp.float32),
            jax.ShapeDtypeStruct(half, jnp.float32),
            jax.ShapeDtypeStruct((count, 8, chans, width), jnp.bfloat16),
            jax.ShapeDtypeStruct((8, chans, width), jnp.float32),
        ],
        name="own_part",
    )(place, share, members, control, blend, operators)


def cross_kernel(
    place_ref, share_ref, a_ref, a_control_ref, b_ref, b_control_ref,
    near_ref, control_ref, blend_ref, pair_ref, single_ref,
    keep_ref, give_ref, sums, first, second, third, fourth, mixed, alone,
):
    step = pl.program_id(0)
    group = near_ref.shape[0]
    chans, width = near_ref.shape[2:]
    parts = width // LANES
    lane = lax.broadcasted_iota(jnp.int32, (8, LANES), 1)
    final = step == pl.num_programs(0) - 1
    span = group * chans
    sides = (
        (a_ref, a_control_ref, (0, 1), (0, 1, 2, 3)),
        (b_ref, b_control_ref, (0, 1), (4, 5, 6, 7)),
    )

    def lanes(part, base=0):
        return slice(base + part * LANES, base + (part + 1) * LANES)

    for side, (halo, halo_control, order, own) in enumerate(sides):
        for one in range(group):
            share = share_ref[step * group + one]
            at = slice(side * span + one * chans, side * span + (one + 1) * chans)
            below = slice(2 * span + at.start, 2 * span + at.stop)
            for part in range(parts):
                y1, y2 = [
                    (
                        halo[one, slot, :, lanes(part)]
                        * (share * halo_control[0, slot, :, lanes(part)])
                    ).astype(jnp.bfloat16)
                    for slot in order
                ]
                y3 = (
                    near_ref[one, own[2], :, lanes(part)].astype(jnp.float32)
                    * (share * control_ref[own[2], :, lanes(part)])
                ).astype(jnp.bfloat16)
                if part < 2:
                    first[at, lanes(part)] = y1
                    first[at, lanes(part, 2 * LANES)] = y2
                    third[at, lanes(part)] = y1
                    third[below, lanes(part)] = y3
                if part > 0:
                    second[at, lanes(part - 1)] = y1
                    second[at, lanes(part - 1, 2 * LANES)] = y2
                    fourth[at, lanes(part - 1)] = y1
                    fourth[below, lanes(part - 1)] = y3
    mixed[0] = jnp.dot(first[...], pair_ref[0], preferred_element_type=jnp.float32)
    mixed[1] = jnp.dot(second[...], pair_ref[1], preferred_element_type=jnp.float32)
    alone[0] = jnp.dot(third[...], single_ref[0], preferred_element_type=jnp.float32)
    alone[1] = jnp.dot(fourth[...], single_ref[1], preferred_element_type=jnp.float32)

    def piece(ref, at, part, base):
        if part == 0:
            return ref[0, at, lanes(0, base)]
        if part == parts - 1:
            return ref[1, at, lanes(1, base)]
        return ref[0, at, lanes(1, base)] + ref[1, at, lanes(0, base)]

    def per_chans(eight, carry):
        here = pl.ds(pl.multiple_of(eight * 8, 8), 8)
        for side, (halo, halo_control, order, own) in enumerate(sides):
            for part in range(parts):
                totals = [None] * 6
                c = [
                    halo_control[0, order[0], here, lanes(part)],
                    halo_control[0, order[1], here, lanes(part)],
                    control_ref[own[2], here, lanes(part)],
                    control_ref[own[3], here, lanes(part)],
                ]
                for one in range(group):
                    share = share_ref[step * group + one]
                    start = side * span + one * chans + eight * 8
                    at = pl.ds(pl.multiple_of(start, 8), 8)
                    below = pl.ds(pl.multiple_of(2 * span + start, 8), 8)
                    b1 = halo[one, order[0], here, lanes(part)]
                    b2 = halo[one, order[1], here, lanes(part)]
                    a = [
                        near_ref[one, row, here, lanes(part)].astype(jnp.float32) for row in own
                    ]
                    y = [x * (share * k) for x, k in zip((b1, b2, a[2], a[3]), c)]
                    terms = (
                        a[0] * piece(mixed, at, part, 0),
                        a[1] * piece(mixed, at, part, 2 * LANES),
                        a[2] * (piece(alone, at, part, 0) + y[1]),
                        a[3] * y[0],
                        b1 * (piece(alone, below, part, 0) + y[3]),
                        b2 * y[2],
                    )
                    totals = [t if s is None else s + t for s, t in zip(totals, terms)]
                for i, value in enumerate(totals):
                    place = side * 6 + i
                    before = jnp.where(step == 0, 0.0, sums[place, here, lanes(part)])
                    sums[place, here, lanes(part)] = before + value
        return carry

    lax.fori_loop(0, chans // 8, per_chans, 0)

    def exact(y1, y2, y3, y4):
        wide = scaled(4.0, widen(y1, lane))
        inner = plus(widen(plus(wide, scaled(6.0, y2)), lane), scaled(12.0, y1))
        top = plus(widen(inner, lane), scaled(4.0, y2))
        next_row = plus(
            widen(plus(scaled(1.5, wide), scaled(4.0, y2)), lane), scaled(4.0, y1)
        )
        return top, next_row, plus(wide, y2), y1, plus(scaled(4.0, widen(y3, lane)), y4), y3

    @pl.when(final)
    def _():
        def finish(eight, carry):
            at = pl.ds(pl.multiple_of(eight * 8, 8), 8)
            slot = jnp.bitwise_xor(eight, place_ref[0])
            blend = blend_ref[at, :]
            for side, (halo, halo_control, order, own) in enumerate(sides):
                found = exact(
                    split_lanes(halo_control[0, order[0], at, :]),
                    split_lanes(halo_control[0, order[1], at, :]),
                    split_lanes(control_ref[own[2], at, :]),
                    split_lanes(control_ref[own[3], at, :]),
                )
                for i, value in enumerate(found):
                    place = side * 6 + i
                    for part in range(parts):
                        sums[place, at, lanes(part)] = SCALE * (
                            (1.0 - blend) * sums[place, at, lanes(part)]
                            + (0.25 * blend) * value[part]
                        )

            @pl.when(jnp.bitwise_and(slot, 1) == 0)
            def _():
                keep_ref[slot // 2] = sums[:, at, :]

            @pl.when(jnp.bitwise_and(slot, 1) == 1)
            def _():
                give_ref[slot // 2] = sums[:, at, :]

            return carry

        lax.fori_loop(0, chans // 8, finish, 0, unroll=2)


def cross_part(place, share, a, b, near, control_near, blend, group):
    count, rows, chans, width = near.shape
    halo = pl.BlockSpec((group, 2, chans, width), lambda i: (i, 0, 0, 0))
    halo_control = pl.BlockSpec((1, 2, chans, width), lambda i: (count, 0, 0, 0))
    half = (chans // 16, 12, 8, width)
    _, p1, p2, p3 = column_operators(width)
    left, right = stacked([p1, p2]), stacked([p2, p3])
    pair = jnp.asarray(np.concatenate([left, right], axis=2))
    single = jnp.asarray(stacked([p3]))
    span = 2 * group * chans
    return pl.pallas_call(
        cross_kernel,
        grid=(count // group,),
        in_specs=[
            pl.BlockSpec(memory_space=pltpu.SMEM),
            pl.BlockSpec(memory_space=pltpu.SMEM),
            halo,
            halo_control,
            halo,
            halo_control,
            pl.BlockSpec((group, rows, chans, width), lambda i: (i, 0, 0, 0)),
            pl.BlockSpec((rows, chans, width), lambda i: (0, 0, 0)),
            pl.BlockSpec((chans, LANES), lambda i: (0, 0)),
            pl.BlockSpec(pair.shape, lambda i: (0, 0, 0)),
            pl.BlockSpec(single.shape, lambda i: (0, 0, 0)),
        ],
        out_specs=[pl.BlockSpec(half, lambda i: (0, 0, 0, 0))] * 2,
        out_shape=[jax.ShapeDtypeStruct(half, jnp.float32)] * 2,
        scratch_shapes=[
            pltpu.VMEM((12, chans, width), jnp.float32),
            pltpu.VMEM((span, 4 * LANES), jnp.bfloat16),
            pltpu.VMEM((span, 4 * LANES), jnp.bfloat16),
            pltpu.VMEM((2 * span, 2 * LANES), jnp.bfloat16),
            pltpu.VMEM((2 * span, 2 * LANES), jnp.bfloat16),
            pltpu.VMEM((2, span, 4 * LANES), jnp.float32),
            pltpu.VMEM((2, 2 * span, 2 * LANES), jnp.float32),
        ],
        name="cross_part",
    )(place, share, a, a, b, b, near, control_near, blend, pair, single)


def sent_kernel(
    place_ref, own_ref, got_ref, last_ref, cross_ref, cross_got_ref, cross_last_ref, a_ref, b_ref, turned
):
    chans, _, width = last_ref.shape
    whole = own_ref[0] + got_ref[0] + last_ref[...]
    for part in range(width // LANES):
        lanes = slice(part * LANES, (part + 1) * LANES)
        for chan in range(chans):
            turned[chan * PITCH : chan * PITCH + 8] = whole[chan, :8, lanes]
        first = turned[pl.ds(0, chans, stride=PITCH), :]

        def crossed(i):
            return cross_ref[0, i, :, lanes] + cross_got_ref[0, i, :, lanes] + cross_last_ref[i, :, lanes]

        first += crossed(6 * (1 - place_ref[3]))
        for side, ref in enumerate((a_ref, b_ref)):
            for i in range(2):
                ref[i, :, lanes] = crossed(6 * side + 4 + i)
            ref[2, :, lanes] = first


def sent_rows(place, own, got, last, cross, cross_got, cross_last):
    chans, _, width = last.shape
    one = lambda x: pl.BlockSpec((1,) + x.shape[1:], lambda i: (0, 0, 0, 0))
    vmem = pl.BlockSpec(memory_space=pltpu.VMEM)
    return pl.pallas_call(
        sent_kernel,
        grid=(1,),
        in_specs=[
            pl.BlockSpec(memory_space=pltpu.SMEM),
            one(own), one(got), vmem, one(cross), one(cross_got), vmem,
        ],
        out_specs=[vmem, vmem],
        out_shape=[jax.ShapeDtypeStruct((3, chans, width), jnp.float32)] * 2,
        scratch_shapes=[pltpu.VMEM((chans * PITCH, LANES), jnp.float32)],
        name="sent_rows",
    )(place, own, got, last, cross, cross_got, cross_last)


def answer_kernel(
    place_ref, asked_ref, own_ref, got_ref, last_ref, cross_ref, cross_got_ref, cross_last_ref,
    a_ref, b_ref, out_ref, turned, pairs,
):
    chans, rows, width = last_ref.shape
    parts = width // LANES
    capacity = out_ref.shape[0] // asked_ref.shape[0]
    keep_high = (place_ref[2] != 0).astype(jnp.float32)
    odd = place_ref[3]
    whole = own_ref[0] + got_ref[0] + last_ref[...]
    for part in range(parts):
        for chan in range(chans):
            turned[part, chan * PITCH : chan * PITCH + rows] = whole[
                chan, :, part * LANES : (part + 1) * LANES
            ]

    def crossed(i, lanes):
        return cross_ref[0, i, :, lanes] + cross_got_ref[0, i, :, lanes] + cross_last_ref[i, :, lanes]

    def from_next(i, lanes):
        return jnp.where(odd == 0, a_ref[i, :, lanes], b_ref[i, :, lanes])

    def from_before(i, lanes):
        return jnp.where(odd == 0, b_ref[i, :, lanes], a_ref[i, :, lanes])

    for part in range(parts):
        lanes = slice(part * LANES, (part + 1) * LANES)
        for row in range(rows + 1):
            if row < rows:
                value = turned[part, pl.ds(row, chans, stride=PITCH), :]
            else:
                value = keep_high * (from_next(2, lanes) + crossed(6 * odd + 4, lanes))
            if row < 4:
                value += crossed(6 * (1 - odd) + row, lanes)
            if rows - 4 <= row < rows:
                value += crossed(6 * odd + rows - 1 - row, lanes)
            if row < 2:
                value += from_before(row, lanes)
            if rows - 2 <= row < rows:
                value += from_next(rows - 1 - row, lanes)
            if row < rows:
                pairs[part, pl.ds(row * 2 * chans, chans, stride=2), :] = value
            if row > 0:
                pairs[part, pl.ds((row - 1) * 2 * chans + 1, chans, stride=2), :] = value

    def one(device, carry):
        for slot in range(capacity):
            row = asked_ref[device, 0, slot]
            at = pl.ds(pl.multiple_of(row * (2 * chans), 2 * chans), 2 * chans)
            for part in range(parts):
                out_ref[device * capacity + slot, :, part * LANES : (part + 1) * LANES] = pairs[
                    part, at, :
                ]
        return carry

    lax.fori_loop(0, asked_ref.shape[0], one, 0, unroll=4)


def answers(place, asked, capacity, own, got, last, cross, cross_got, cross_last, a, b):
    chans, rows, width = last.shape
    slots = asked.shape[0] * capacity
    smem = pl.BlockSpec(memory_space=pltpu.SMEM)
    vmem = pl.BlockSpec(memory_space=pltpu.VMEM)
    one = lambda x: pl.BlockSpec((1,) + x.shape[1:], lambda i: (0, 0, 0, 0))
    return pl.pallas_call(
        answer_kernel,
        grid=(1,),
        in_specs=[smem, smem, one(own), one(got), vmem, one(cross), one(cross_got), vmem, vmem, vmem],
        out_specs=vmem,
        out_shape=jax.ShapeDtypeStruct((slots, 2 * chans, width), jnp.float32),
        scratch_shapes=[
            pltpu.VMEM((width // LANES, chans * PITCH, LANES), jnp.float32),
            pltpu.VMEM((width // LANES, rows * 2 * chans, LANES), jnp.float32),
        ],
        name="answers",
    )(place, asked, own, got, last, cross, cross_got, cross_last, a, b)


def fine_kernel(slot_ref, arrived_ref, index_ref, weight_ref, out_ref):
    blocks = index_ref.shape[0]
    pairs, _ = arrived_ref.shape[1:]
    fine = index_ref.shape[2]
    half = LANES // 2
    quarter = half // 2
    lane = lax.broadcasted_iota(jnp.int32, (8, LANES), 1)
    even = lax.broadcasted_iota(jnp.int32, (8, LANES), 0) % 2 == 0

    def one(block, carry):
        slot = slot_ref[block]
        windows = []
        for group in range(pairs // 8):
            parts = []
            for part in split_lanes(arrived_ref[slot, pl.ds(group * 8, 8), :]):
                other = jnp.where(even, pltpu.roll(part, 7, 0), pltpu.roll(part, 1, 0))
                parts.append(0.75 * part + 0.25 * other)
            turned = {
                shift: [pltpu.roll(p, shift, 1) for p in parts]
                for shift in (quarter, LANES - quarter)
            }
            found = []
            for chunk in range(fine // LANES):
                part, ahead = divmod(chunk * half - quarter, LANES)
                rolled = turned[LANES - ahead]
                if part < 0:
                    found.append(rolled[part + 1])
                elif part + 1 == len(parts):
                    found.append(rolled[part])
                else:
                    found.append(
                        jnp.where(lane < LANES - ahead, rolled[part], rolled[part + 1])
                    )
            windows.append(found)
        for chunk in range(fine // LANES):
            lanes = slice(chunk * LANES, (chunk + 1) * LANES)
            index = index_ref[block, :, lanes]
            weight = weight_ref[block, :, lanes]
            for group in range(pairs // 8):
                near = windows[group][chunk]
                left = jnp.take_along_axis(near, index, axis=1)
                right = jnp.take_along_axis(near, index + 1, axis=1)
                value = (1.0 - weight) * left + weight * right
                out_ref[block, group * 4 : (group + 1) * 4, :, lanes] = value.reshape(4, 2, LANES)
        return carry

    lax.fori_loop(0, blocks, one, 0, unroll=4)


def fine_part(slot, arrived, index, weight):
    blocks, _, fine = index.shape
    chans = arrived.shape[1] // 2
    smem = pl.BlockSpec(memory_space=pltpu.SMEM)
    vmem = pl.BlockSpec(memory_space=pltpu.VMEM)
    return pl.pallas_call(
        fine_kernel,
        in_specs=[smem, vmem, vmem, vmem],
        out_specs=vmem,
        out_shape=jax.ShapeDtypeStruct((blocks, chans, 2, fine), jnp.float32),
        name="fine_part",
    )(slot, arrived, index, weight)


def column_kernel(source_ref, code_ref, index_ref, weight_ref):
    blocks, fine = source_ref.shape
    column = lax.broadcasted_iota(jnp.int32, (1, fine), 1)
    first = (column // LANES) * (LANES // 2) - LANES // 4
    for block in range(blocks):
        shape = index_ref.shape[1:]
        index_ref[block] = jnp.broadcast_to(source_ref[block : block + 1] - first, shape)
        weight_ref[block] = jnp.broadcast_to(
            code_ref[block : block + 1].astype(jnp.float32) * (1.0 / 16.0), shape
        )


def columns(source, code):
    blocks, fine = source.shape
    return pl.pallas_call(
        column_kernel,
        out_shape=[
            jax.ShapeDtypeStruct((blocks, 8, fine), jnp.int32),
            jax.ShapeDtypeStruct((blocks, 8, fine), jnp.float32),
        ],
        name="columns",
    )(source, code)


def per_device(
    members,
    control,
    hybrid_weight,
    member_weights,
    source_device,
    source_row,
    column_source,
    column_code,
):
    member_count, chans, row_count, width = members.shape
    spaces = lax.axis_size("space")
    space_index = lax.axis_index("space")
    member_slot = lax.axis_index("member")

    place = jnp.stack(
        [
            member_slot,
            jnp.where(space_index == 0, 0, jnp.where(space_index == spaces - 1, 2, 1)),
            (space_index < spaces - 1).astype(jnp.int32),
            space_index % 2,
        ]
    ).astype(jnp.int32)
    to_a, to_b = edge_rows(place, members, control, 4)
    halo_b = paired(to_b, "space", 1)
    halo_a = paired(to_a, "space", 0)

    weight_codes = member_weights.astype(jnp.float32)
    share = lax.dynamic_slice_in_dim(
        weight_codes, member_slot * member_count, member_count
    ) / jnp.sum(weight_codes)
    blend = jnp.broadcast_to(hybrid_weight[:, None], (chans, LANES))
    source_index = source_device[:, 0]
    capacity = max(2, 2 * row_count // spaces)
    chosen = (source_index[:, None] == jnp.arange(spaces, dtype=jnp.int32)[None, :]).astype(
        jnp.int32
    )
    earlier = jnp.cumsum(chosen, axis=0) - chosen
    rank_within = jnp.sum(earlier * chosen, axis=1)
    slot_index = source_index * capacity + rank_within
    spread = slot_index[None, :] - capacity * jnp.arange(spaces, dtype=jnp.int32)[:, None]
    lane = jnp.arange(LANES, dtype=jnp.int32)
    taken = (spread[:, None, :] == lane[None, :, None]) & (lane < capacity)[None, :, None]
    request = jnp.sum(jnp.where(taken, source_row[None, None, :], 0), axis=2)[:, None, :]
    index, weight = columns(column_source, column_code)

    own_keep, own_give, near, control_near = own_part(place, share, members, control, blend)
    own_give, request = lax.optimization_barrier((own_give, request))
    asked = lax.all_to_all(request, "space", split_axis=0, concat_axis=0, tiled=True)
    own_got = swapped(own_give, "member", 1)
    own_last = swapped(own_keep[1] + own_got[1], "member", 2)
    near, index, weight, slot_index = lax.optimization_barrier((near, index, weight, slot_index))

    keep, give = cross_part(place, share, halo_a, halo_b, near, control_near, blend, 4)
    got = swapped(give, "member", 1)
    last = swapped(keep[1] + got[1], "member", 2)
    back_a, back_b = sent_rows(place, own_keep, own_got, own_last, keep, got, last)
    back_b = paired(back_b, "space", 1)
    back_a = paired(back_a, "space", 0)

    outgoing = answers(
        place, asked, capacity, own_keep, own_got, own_last, keep, got, last, back_a, back_b
    )
    pair_rows = outgoing.shape[1]
    arrived = lax.all_to_all(
        outgoing.reshape(spaces, capacity * pair_rows, width),
        "space",
        split_axis=0,
        concat_axis=0,
        tiled=True,
    ).reshape(spaces * capacity, pair_rows, width)
    return fine_part(slot_index, arrived, index, weight)


def solution(mesh):
    placed = (
        P("member", None, "space", None),
        P(None, "space", None),
        P(),
        P(),
        P("space", None),
        P("space"),
        P("space", None),
        P("space", None),
    )

    return jax.shard_map(
        per_device,
        mesh=mesh,
        in_specs=placed,
        out_specs=P("space", "member", None, None),
        check_vma=False,
    )
```

```python
import jax
import jax.numpy as jnp
import numpy as np
from jax import lax
from jax.experimental import pallas as pl
from jax.experimental.pallas import tpu as pltpu
from jax.sharding import PartitionSpec as P

SCALE = 1.0 / 625.0
LANES = 128
PITCH = 24
LIMIT = 67043328


def paired(x, axis, first):
    length = lax.axis_size(axis)
    pairs = []
    for low in range(first, length - 1, 2):
        pairs += [(low, low + 1), (low + 1, low)]
    return lax.ppermute(x, axis, pairs)


def swapped(x, axis, bit):
    length = lax.axis_size(axis)
    return lax.ppermute(x, axis, [(i, i ^ bit) for i in range(length)])


def split_lanes(x):
    return [x[:, i : i + LANES] for i in range(0, x.shape[-1], LANES)]


def side_sum(parts, lane):
    ahead = [pltpu.roll(p, 1, 1) for p in parts]
    behind = [pltpu.roll(p, LANES - 1, 1) for p in parts]
    out = []
    for i in range(len(parts)):
        left = jnp.where(lane == 0, ahead[i - 1] if i else 0.0, ahead[i])
        right = jnp.where(
            lane == LANES - 1, behind[i + 1] if i + 1 < len(parts) else 0.0, behind[i]
        )
        out.append(left + right)
    return out


def inverse_total(weights_ref, rows):
    total = weights_ref[0]
    for i in range(1, weights_ref.shape[0]):
        total += weights_ref[i]
    return 1.0 / jnp.full((rows, LANES), total.astype(jnp.float32))


def plus(a, b):
    return [p + q for p, q in zip(a, b)]


def scaled(factor, a):
    return [factor * p for p in a]


def widen(parts, lane):
    return plus(parts, side_sum(parts, lane))


def edges_kernel(place_ref, members_ref, control_ref, a_ref, b_ref, scratch, stage, sems):
    step = pl.program_id(0)
    steps = pl.num_programs(0)
    group = members_ref.shape[0]
    chans, rows = members_ref.shape[1:3]
    parts = scratch.shape[0]
    odd = place_ref[3]

    def copies(first, count, index):
        return [
            pltpu.make_async_copy(
                stage.at[side, pl.ds(first, count)], ref.at[pl.ds(first, count)], sems.at[side, index]
            )
            for side, ref in enumerate((a_ref, b_ref))
        ]

    def rows_out(wide, index):
        for part in range(parts):
            lanes = slice(part * LANES, (part + 1) * LANES)
            for chan in range(chans):
                scratch[part, chan * PITCH : chan * PITCH + rows] = wide[chan, :, lanes]
            for slot in range(2):
                for which, side in ((slot, 1 - odd), (rows - 1 - slot, odd)):
                    stage[side, index, slot, :, lanes] = scratch[
                        part, pl.ds(which, chans, stride=PITCH), :
                    ]

    for one in range(group):
        rows_out(members_ref[one].astype(jnp.float32), step * group + one)
    for copy in copies(step * group, group, step):
        copy.start()

    @pl.when(step == steps - 1)
    def _():
        count = a_ref.shape[0] - 1
        rows_out(control_ref[...], count)
        for copy in copies(count, 1, count // group):
            copy.start()
        for index in range(count // group):
            for copy in copies(index * group, group, index):
                copy.wait()
        for copy in copies(count, 1, count // group):
            copy.wait()


def edge_rows(place, members, control, group):
    count, chans, rows, width = members.shape
    shape = (count + 1, 2, chans, width)
    out = jax.ShapeDtypeStruct(shape, jnp.float32)
    return pl.pallas_call(
        edges_kernel,
        grid=(count // group,),
        in_specs=[
            pl.BlockSpec(memory_space=pltpu.SMEM),
            pl.BlockSpec((group, chans, rows, width), lambda i: (i, 0, 0, 0)),
            pl.BlockSpec((chans, rows, width), lambda i: (0, 0, 0)),
        ],
        out_specs=[pl.BlockSpec(memory_space=pl.ANY)] * 2,
        out_shape=[out, out],
        scratch_shapes=[
            pltpu.VMEM((width // LANES, chans * PITCH, LANES), jnp.float32),
            pltpu.VMEM((2,) + shape, jnp.float32),
            pltpu.SemaphoreType.DMA((2, count // group + 1)),
        ],
        name="edge_rows",
    )(place, members, control)


def column_operators(width):
    q = np.eye(width) + np.eye(width, k=1) + np.eye(width, k=-1)
    q2 = q @ q
    q3 = q2 @ q
    eye = np.eye(width)
    return q2 @ q2 + 12 * q2 + 6 * eye, 4 * q3 + 12 * q, 6 * q2 + 4 * eye, 4 * q


def windowed(operator):
    first = operator[:256, :256]
    second = operator[128:, 128:].copy()
    second[:128, :128] = 0.0
    return first, second


def stacked(operators):
    first, second = zip(*[windowed(op) for op in operators])
    return np.stack([np.concatenate(first), np.concatenate(second)]).astype(jnp.bfloat16)


def own_kernel(
    place_ref, share_ref, members_ref, control_ref, blend_ref, operator_ref,
    keep_ref, give_ref, near_ref, control_near_ref,
    total, scratch, *work,
):
    step = pl.program_id(0)
    both, chans, rows, width = members_ref.shape
    parts = width // LANES
    last = pl.num_programs(0) - 1
    static = step == last
    fields, firsts, seconds, mixes = [work[i * both : (i + 1) * both] for i in range(4)]
    odd = place_ref[3]
    ends = [(4 * (1 - odd) + i, i) for i in range(4)]
    ends += [(4 * odd + i, rows - 1 - i) for i in range(4)]

    def lanes(part):
        return slice(part * LANES, (part + 1) * LANES)

    @pl.when(step == 0)
    def _():
        total[...] = jnp.zeros(total.shape, jnp.float32)
        for field in fields:
            field[...] = jnp.zeros(field.shape, jnp.float32)

    @pl.when(step < last)
    def _():
        for which, field in enumerate(fields):

            def fill(chan, carry):
                for part in range(parts):
                    state = members_ref[which, chan, :, lanes(part)].astype(jnp.float32)
                    field[part, chan, 8 : 8 + rows] = state * control_ref[chan, :, lanes(part)]
                    scratch[part, pl.ds(pl.multiple_of(chan * PITCH, 8), rows), :] = state
                return carry

            lax.fori_loop(0, chans, fill, 0, unroll=4)
            for place, row in ends:
                for part in range(parts):
                    near_ref[which, place, :, lanes(part)] = scratch[
                        part, pl.ds(row, chans, stride=PITCH), :
                    ].astype(jnp.bfloat16)

    @pl.when(static)
    def _():
        def fill(chan, carry):
            for part in range(parts):
                block = control_ref[chan, :, lanes(part)]
                for field in fields:
                    field[part, chan, 8 : 8 + rows] = block
                scratch[part, pl.ds(pl.multiple_of(chan * PITCH, 8), rows), :] = block
            return carry

        lax.fori_loop(0, chans, fill, 0, unroll=4)
        for place, row in ends:
            for part in range(parts):
                control_near_ref[place, :, lanes(part)] = scratch[
                    part, pl.ds(row, chans, stride=PITCH), :
                ]

    @pl.when(place_ref[1] == 0)
    def _():
        def image(chan, carry):
            for field in fields:
                for part in range(parts):
                    for row in range(3):
                        field[part, chan, 6 - row : 7 - row] = -field[
                            part, chan, 8 + row : 9 + row
                        ]
            return carry

        lax.fori_loop(0, chans, image, 0, unroll=4)

    @pl.when(place_ref[1] == 2)
    def _():
        def image(chan, carry):
            for field in fields:
                for part in range(parts):
                    for row in range(3):
                        field[part, chan, 9 + rows + row : 10 + rows + row] = -field[
                            part, chan, 7 + rows - row : 8 + rows - row
                        ]
            return carry

        lax.fori_loop(0, chans, image, 0, unroll=4)

    def at_distance(field, part, chan, distance):
        if distance == 0:
            return field[part, chan, 8 : 8 + rows]
        return (
            field[part, chan, 8 - distance : 8 - distance + rows]
            + field[part, chan, 8 + distance : 8 + distance + rows]
        )

    refine = jnp.where(static, 1.0, 0.0)

    def gather(which, chan):
        start = chan * rows
        at = pl.ds(start if isinstance(chan, int) else pl.multiple_of(start, rows), rows)
        for distance in range(4):
            base = distance * 2 * LANES
            for part in range(parts):
                value = at_distance(fields[which], part, chan, distance)
                if which:
                    value -= refine * value.astype(jnp.bfloat16).astype(jnp.float32)
                value = value.astype(jnp.bfloat16)
                if part < 2:
                    firsts[which][at, base + part * LANES : base + (part + 1) * LANES] = value
                if part > 0:
                    seconds[which][at, base + (part - 1) * LANES : base + part * LANES] = value

    inverse = inverse_total(share_ref, 1)

    def multiply(which):
        for window, ref in enumerate((firsts[which], seconds[which])):
            mixes[which][window] = jnp.dot(
                ref[...], operator_ref[window], preferred_element_type=jnp.float32
            )

    def collect(which, chan):
        at = pl.ds(chan * rows, rows)
        mixed = mixes[which]
        low = [mixed[0, at, lanes(0)], mixed[0, at, lanes(1)]]
        high = [mixed[1, at, lanes(0)], mixed[1, at, lanes(1)]]
        found = [low[0], low[1] + high[0], high[1]]
        blend = blend_ref[chan : chan + 1, :]
        member = jnp.minimum(step, last - 1) * both + which
        share = share_ref[place_ref[0] * (last * both) + member].astype(jnp.float32)
        factor = jnp.where(static, 0.25 * blend, share)
        for part in range(parts):
            far = at_distance(fields[which], part, chan, 4)
            value = found[part] + (far if which == 0 else (1.0 - refine) * far)
            state = members_ref[which, chan, :, lanes(part)].astype(jnp.float32)
            state = jnp.where(static, 1.0, state)
            before = total[chan, :, lanes(part)]
            if which == 0:
                before = jnp.where(static, (1.0 - blend) * inverse, 1.0) * before
            total[chan, :, lanes(part)] = before + (factor * state) * value

    def gather_four(group, carry):
        for inner in range(4):
            gather(0, group * 4 + inner)
        return carry

    lax.fori_loop(0, chans // 4, gather_four, 0)
    multiply(0)
    for chan in range(chans):
        gather(1, chan)
    multiply(1)
    for chan in range(chans):
        collect(0, chan)
    for chan in range(chans):
        collect(1, chan)

    @pl.when(static)
    def _():
        def one_group(group, carry):
            slot = jnp.bitwise_xor(group, place_ref[0])
            done = SCALE * total[pl.ds(pl.multiple_of(group * 8, 8), 8)]

            @pl.when(jnp.bitwise_and(slot, 1) == 0)
            def _():
                keep_ref[slot // 2] = done

            @pl.when(jnp.bitwise_and(slot, 1) == 1)
            def _():
                give_ref[slot // 2] = done

            return carry

        lax.fori_loop(0, chans // 8, one_group, 0)


def own_part(place, share, members, control, blend):
    count, chans, rows, width = members.shape
    parts = width // LANES
    both = 2
    steps = count // both
    operators = jnp.asarray(stacked(column_operators(width)))
    depth = operators.shape[1]
    half = (chans // 16, 8, rows, width)
    return pl.pallas_call(
        own_kernel,
        grid_spec=pltpu.PrefetchScalarGridSpec(
            num_scalar_prefetch=2,
            grid=(steps + 1,),
            in_specs=[
                pl.BlockSpec(
                    (both, chans, rows, width),
                    lambda i, place, share: (jnp.minimum(i, steps - 1), 0, 0, 0),
                ),
                pl.BlockSpec((chans, rows, width), lambda i, place, share: (0, 0, 0)),
                pl.BlockSpec((chans, LANES), lambda i, place, share: (0, 0)),
                pl.BlockSpec(operators.shape, lambda i, place, share: (0, 0, 0)),
            ],
            out_specs=[
                pl.BlockSpec(half, lambda i, place, share: (0, 0, 0, 0)),
                pl.BlockSpec(half, lambda i, place, share: (0, 0, 0, 0)),
                pl.BlockSpec(
                    (both, 8, chans, width),
                    lambda i, place, share: (jnp.minimum(i, steps - 1), 0, 0, 0),
                ),
                pl.BlockSpec((8, chans, width), lambda i, place, share: (0, 0, 0)),
            ],
            scratch_shapes=[
                pltpu.VMEM((chans, rows, width), jnp.float32),
                pltpu.VMEM((parts, chans * PITCH, LANES), jnp.float32),
            ]
            + [pltpu.VMEM((parts, chans, rows + 16, LANES), jnp.float32)] * both
            + [pltpu.VMEM((chans * rows, depth), jnp.bfloat16)] * (2 * both)
            + [pltpu.VMEM((2, chans * rows, 2 * LANES), jnp.float32)] * both,
        ),
        out_shape=[
            jax.ShapeDtypeStruct(half, jnp.float32),
            jax.ShapeDtypeStruct(half, jnp.float32),
            jax.ShapeDtypeStruct((count, 8, chans, width), jnp.bfloat16),
            jax.ShapeDtypeStruct((8, chans, width), jnp.float32),
        ],
        compiler_params=pltpu.CompilerParams(vmem_limit_bytes=LIMIT),
        name="own_part",
    )(place, share, members, control, blend, operators)


def cross_kernel(
    place_ref, share_ref, a_ref, a_control_ref, b_ref, b_control_ref,
    near_ref, control_ref, blend_ref, pair_ref, single_ref,
    keep_ref, give_ref, sums, first, second, third, fourth, mixed, alone,
):
    step = pl.program_id(0)
    group = near_ref.shape[0]
    chans, width = near_ref.shape[2:]
    parts = width // LANES
    lane = lax.broadcasted_iota(jnp.int32, (8, LANES), 1)
    final = step == pl.num_programs(0) - 1
    span = group * chans
    first_member = (place_ref[0] * pl.num_programs(0) + step) * group
    sides = (
        (a_ref, a_control_ref, (0, 1), (0, 1, 2, 3)),
        (b_ref, b_control_ref, (0, 1), (4, 5, 6, 7)),
    )

    def lanes(part, base=0):
        return slice(base + part * LANES, base + (part + 1) * LANES)

    for side, (halo, halo_control, order, own) in enumerate(sides):
        for one in range(group):
            share = share_ref[first_member + one].astype(jnp.float32)
            at = slice(side * span + one * chans, side * span + (one + 1) * chans)
            below = slice(2 * span + at.start, 2 * span + at.stop)
            for part in range(parts):
                y1, y2 = [
                    (
                        halo[one, slot, :, lanes(part)]
                        * (share * halo_control[0, slot, :, lanes(part)])
                    ).astype(jnp.bfloat16)
                    for slot in order
                ]
                y3 = (
                    near_ref[one, own[2], :, lanes(part)].astype(jnp.float32)
                    * (share * control_ref[own[2], :, lanes(part)])
                ).astype(jnp.bfloat16)
                if part < 2:
                    first[at, lanes(part)] = y1
                    first[at, lanes(part, 2 * LANES)] = y2
                    third[at, lanes(part)] = y1
                    third[below, lanes(part)] = y3
                if part > 0:
                    second[at, lanes(part - 1)] = y1
                    second[at, lanes(part - 1, 2 * LANES)] = y2
                    fourth[at, lanes(part - 1)] = y1
                    fourth[below, lanes(part - 1)] = y3
    mixed[0] = jnp.dot(first[...], pair_ref[0], preferred_element_type=jnp.float32)
    mixed[1] = jnp.dot(second[...], pair_ref[1], preferred_element_type=jnp.float32)
    alone[0] = jnp.dot(third[...], single_ref[0], preferred_element_type=jnp.float32)
    alone[1] = jnp.dot(fourth[...], single_ref[1], preferred_element_type=jnp.float32)

    def piece(ref, at, part, base):
        if part == 0:
            return ref[0, at, lanes(0, base)]
        if part == parts - 1:
            return ref[1, at, lanes(1, base)]
        return ref[0, at, lanes(1, base)] + ref[1, at, lanes(0, base)]

    def per_chans(eight, carry):
        here = pl.ds(pl.multiple_of(eight * 8, 8), 8)
        for side, (halo, halo_control, order, own) in enumerate(sides):
            for part in range(parts):
                totals = [None] * 6
                c = [
                    halo_control[0, order[0], here, lanes(part)],
                    halo_control[0, order[1], here, lanes(part)],
                    control_ref[own[2], here, lanes(part)],
                    control_ref[own[3], here, lanes(part)],
                ]
                for one in range(group):
                    share = share_ref[first_member + one].astype(jnp.float32)
                    start = side * span + one * chans + eight * 8
                    at = pl.ds(pl.multiple_of(start, 8), 8)
                    below = pl.ds(pl.multiple_of(2 * span + start, 8), 8)
                    b1 = halo[one, order[0], here, lanes(part)]
                    b2 = halo[one, order[1], here, lanes(part)]
                    a = [
                        near_ref[one, row, here, lanes(part)].astype(jnp.float32) for row in own
                    ]
                    y = [x * (share * k) for x, k in zip((b1, b2, a[2], a[3]), c)]
                    terms = (
                        a[0] * piece(mixed, at, part, 0),
                        a[1] * piece(mixed, at, part, 2 * LANES),
                        a[2] * (piece(alone, at, part, 0) + y[1]),
                        a[3] * y[0],
                        b1 * (piece(alone, below, part, 0) + y[3]),
                        b2 * y[2],
                    )
                    totals = [t if s is None else s + t for s, t in zip(totals, terms)]
                for i, value in enumerate(totals):
                    place = side * 6 + i
                    before = jnp.where(step == 0, 0.0, sums[place, here, lanes(part)])
                    sums[place, here, lanes(part)] = before + value
        return carry

    lax.fori_loop(0, chans // 8, per_chans, 0)

    def exact(y1, y2, y3, y4):
        wide = scaled(4.0, widen(y1, lane))
        inner = plus(widen(plus(wide, scaled(6.0, y2)), lane), scaled(12.0, y1))
        top = plus(widen(inner, lane), scaled(4.0, y2))
        next_row = plus(
            widen(plus(scaled(1.5, wide), scaled(4.0, y2)), lane), scaled(4.0, y1)
        )
        return top, next_row, plus(wide, y2), y1, plus(scaled(4.0, widen(y3, lane)), y4), y3

    @pl.when(final)
    def _():
        inverse = inverse_total(share_ref, 8)

        def finish(eight, carry):
            at = pl.ds(pl.multiple_of(eight * 8, 8), 8)
            slot = jnp.bitwise_xor(eight, place_ref[0])
            blend = blend_ref[at, :]
            for side, (halo, halo_control, order, own) in enumerate(sides):
                found = exact(
                    split_lanes(halo_control[0, order[0], at, :]),
                    split_lanes(halo_control[0, order[1], at, :]),
                    split_lanes(control_ref[own[2], at, :]),
                    split_lanes(control_ref[own[3], at, :]),
                )
                for i, value in enumerate(found):
                    place = side * 6 + i
                    for part in range(parts):
                        sums[place, at, lanes(part)] = SCALE * (
                            ((1.0 - blend) * inverse) * sums[place, at, lanes(part)]
                            + (0.25 * blend) * value[part]
                        )

            @pl.when(jnp.bitwise_and(slot, 1) == 0)
            def _():
                keep_ref[slot // 2] = sums[:, at, :]

            @pl.when(jnp.bitwise_and(slot, 1) == 1)
            def _():
                give_ref[slot // 2] = sums[:, at, :]

            return carry

        lax.fori_loop(0, chans // 8, finish, 0, unroll=2)


def cross_part(place, share, a, b, near, control_near, blend, group):
    count, rows, chans, width = near.shape
    halo = pl.BlockSpec((group, 2, chans, width), lambda i: (i, 0, 0, 0))
    halo_control = pl.BlockSpec((1, 2, chans, width), lambda i: (count, 0, 0, 0))
    half = (chans // 16, 12, 8, width)
    _, p1, p2, p3 = column_operators(width)
    left, right = stacked([p1, p2]), stacked([p2, p3])
    pair = jnp.asarray(np.concatenate([left, right], axis=2))
    single = jnp.asarray(stacked([p3]))
    span = 2 * group * chans
    return pl.pallas_call(
        cross_kernel,
        grid=(count // group,),
        in_specs=[
            pl.BlockSpec(memory_space=pltpu.SMEM),
            pl.BlockSpec(memory_space=pltpu.SMEM),
            halo,
            halo_control,
            halo,
            halo_control,
            pl.BlockSpec((group, rows, chans, width), lambda i: (i, 0, 0, 0)),
            pl.BlockSpec((rows, chans, width), lambda i: (0, 0, 0)),
            pl.BlockSpec((chans, LANES), lambda i: (0, 0)),
            pl.BlockSpec(pair.shape, lambda i: (0, 0, 0)),
            pl.BlockSpec(single.shape, lambda i: (0, 0, 0)),
        ],
        out_specs=[pl.BlockSpec(half, lambda i: (0, 0, 0, 0))] * 2,
        out_shape=[jax.ShapeDtypeStruct(half, jnp.float32)] * 2,
        scratch_shapes=[
            pltpu.VMEM((12, chans, width), jnp.float32),
            pltpu.VMEM((span, 4 * LANES), jnp.bfloat16),
            pltpu.VMEM((span, 4 * LANES), jnp.bfloat16),
            pltpu.VMEM((2 * span, 2 * LANES), jnp.bfloat16),
            pltpu.VMEM((2 * span, 2 * LANES), jnp.bfloat16),
            pltpu.VMEM((2, span, 4 * LANES), jnp.float32),
            pltpu.VMEM((2, 2 * span, 2 * LANES), jnp.float32),
        ],
        name="cross_part",
    )(place, share, a, a, b, b, near, control_near, blend, pair, single)


def sent_kernel(
    place_ref, own_ref, got_ref, last_ref, cross_ref, cross_got_ref, cross_last_ref, a_ref, b_ref, turned
):
    chans, _, width = last_ref.shape
    whole = own_ref[0] + got_ref[0] + last_ref[...]
    for part in range(width // LANES):
        lanes = slice(part * LANES, (part + 1) * LANES)
        for chan in range(chans):
            turned[chan * PITCH : chan * PITCH + 8] = whole[chan, :8, lanes]
        first = turned[pl.ds(0, chans, stride=PITCH), :]

        def crossed(i):
            return cross_ref[0, i, :, lanes] + cross_got_ref[0, i, :, lanes] + cross_last_ref[i, :, lanes]

        first += crossed(6 * (1 - place_ref[3]))
        for side, ref in enumerate((a_ref, b_ref)):
            for i in range(2):
                ref[i, :, lanes] = crossed(6 * side + 4 + i)
            ref[2, :, lanes] = first


def sent_rows(place, own, got, last, cross, cross_got, cross_last):
    chans, _, width = last.shape
    one = lambda x: pl.BlockSpec((1,) + x.shape[1:], lambda i: (0, 0, 0, 0))
    vmem = pl.BlockSpec(memory_space=pltpu.VMEM)
    return pl.pallas_call(
        sent_kernel,
        grid=(1,),
        in_specs=[
            pl.BlockSpec(memory_space=pltpu.SMEM),
            one(own), one(got), vmem, one(cross), one(cross_got), vmem,
        ],
        out_specs=[vmem, vmem],
        out_shape=[jax.ShapeDtypeStruct((3, chans, width), jnp.float32)] * 2,
        scratch_shapes=[pltpu.VMEM((chans * PITCH, LANES), jnp.float32)],
        name="sent_rows",
    )(place, own, got, last, cross, cross_got, cross_last)


def answer_kernel(
    place_ref, asked_ref, own_ref, got_ref, last_ref, cross_ref, cross_got_ref, cross_last_ref,
    a_ref, b_ref, out_ref, turned, pairs,
):
    chans, rows, width = last_ref.shape
    parts = width // LANES
    capacity = out_ref.shape[0] // asked_ref.shape[0]
    keep_high = (place_ref[2] != 0).astype(jnp.float32)
    odd = place_ref[3]
    whole = own_ref[0] + got_ref[0] + last_ref[...]
    for part in range(parts):
        for chan in range(chans):
            turned[part, chan * PITCH : chan * PITCH + rows] = whole[
                chan, :, part * LANES : (part + 1) * LANES
            ]

    def crossed(i, lanes):
        return cross_ref[0, i, :, lanes] + cross_got_ref[0, i, :, lanes] + cross_last_ref[i, :, lanes]

    def from_next(i, lanes):
        return jnp.where(odd == 0, a_ref[i, :, lanes], b_ref[i, :, lanes])

    def from_before(i, lanes):
        return jnp.where(odd == 0, b_ref[i, :, lanes], a_ref[i, :, lanes])

    for part in range(parts):
        lanes = slice(part * LANES, (part + 1) * LANES)
        for row in range(rows + 1):
            if row < rows:
                value = turned[part, pl.ds(row, chans, stride=PITCH), :]
            else:
                value = keep_high * (from_next(2, lanes) + crossed(6 * odd + 4, lanes))
            if row < 4:
                value += crossed(6 * (1 - odd) + row, lanes)
            if rows - 4 <= row < rows:
                value += crossed(6 * odd + rows - 1 - row, lanes)
            if row < 2:
                value += from_before(row, lanes)
            if rows - 2 <= row < rows:
                value += from_next(rows - 1 - row, lanes)
            if row < rows:
                pairs[part, pl.ds(row * 2 * chans, chans, stride=2), :] = value
            if row > 0:
                pairs[part, pl.ds((row - 1) * 2 * chans + 1, chans, stride=2), :] = value

    def one(device, carry):
        for slot in range(capacity):
            row = asked_ref[device, 0, slot]
            at = pl.ds(pl.multiple_of(row * (2 * chans), 2 * chans), 2 * chans)
            for part in range(parts):
                out_ref[device * capacity + slot, :, part * LANES : (part + 1) * LANES] = pairs[
                    part, at, :
                ]
        return carry

    lax.fori_loop(0, asked_ref.shape[0], one, 0, unroll=4)


def answers(place, asked, capacity, own, got, last, cross, cross_got, cross_last, a, b):
    chans, rows, width = last.shape
    slots = asked.shape[0] * capacity
    smem = pl.BlockSpec(memory_space=pltpu.SMEM)
    vmem = pl.BlockSpec(memory_space=pltpu.VMEM)
    one = lambda x: pl.BlockSpec((1,) + x.shape[1:], lambda i: (0, 0, 0, 0))
    return pl.pallas_call(
        answer_kernel,
        grid=(1,),
        in_specs=[smem, smem, one(own), one(got), vmem, one(cross), one(cross_got), vmem, vmem, vmem],
        out_specs=vmem,
        out_shape=jax.ShapeDtypeStruct((slots, 2 * chans, width), jnp.float32),
        scratch_shapes=[
            pltpu.VMEM((width // LANES, chans * PITCH, LANES), jnp.float32),
            pltpu.VMEM((width // LANES, rows * 2 * chans, LANES), jnp.float32),
        ],
        name="answers",
    )(place, asked, own, got, last, cross, cross_got, cross_last, a, b)


def fine_kernel(slot_ref, arrived_ref, index_ref, weight_ref, out_ref):
    blocks = index_ref.shape[0]
    pairs, _ = arrived_ref.shape[1:]
    fine = index_ref.shape[2]
    half = LANES // 2
    quarter = half // 2
    lane = lax.broadcasted_iota(jnp.int32, (8, LANES), 1)
    even = lax.broadcasted_iota(jnp.int32, (8, LANES), 0) % 2 == 0

    def one(block, carry):
        slot = slot_ref[pl.program_id(0) * blocks + block]
        windows = []
        for group in range(pairs // 8):
            parts = []
            for part in split_lanes(arrived_ref[slot, pl.ds(group * 8, 8), :]):
                other = jnp.where(even, pltpu.roll(part, 7, 0), pltpu.roll(part, 1, 0))
                parts.append(0.75 * part + 0.25 * other)
            turned = {
                shift: [pltpu.roll(p, shift, 1) for p in parts]
                for shift in (quarter, LANES - quarter)
            }
            found = []
            for chunk in range(fine // LANES):
                part, ahead = divmod(chunk * half - quarter, LANES)
                rolled = turned[LANES - ahead]
                if part < 0:
                    found.append(rolled[part + 1])
                elif part + 1 == len(parts):
                    found.append(rolled[part])
                else:
                    found.append(
                        jnp.where(lane < LANES - ahead, rolled[part], rolled[part + 1])
                    )
            windows.append(found)
        for chunk in range(fine // LANES):
            lanes = slice(chunk * LANES, (chunk + 1) * LANES)
            index = index_ref[block, :, lanes]
            weight = weight_ref[block, :, lanes]
            for group in range(pairs // 8):
                near = windows[group][chunk]
                left = jnp.take_along_axis(near, index, axis=1)
                right = jnp.take_along_axis(near, index + 1, axis=1)
                value = (1.0 - weight) * left + weight * right
                out_ref[block, group * 4 : (group + 1) * 4, :, lanes] = value.reshape(4, 2, LANES)
        return carry

    lax.fori_loop(0, blocks, one, 0, unroll=4)


def fine_part(slot, arrived, index, weight, group):
    blocks, lines, fine = index.shape
    slots, pairs, width = arrived.shape
    return pl.pallas_call(
        fine_kernel,
        grid=(blocks // group,),
        in_specs=[
            pl.BlockSpec(memory_space=pltpu.SMEM),
            pl.BlockSpec((slots, pairs, width), lambda i: (0, 0, 0)),
            pl.BlockSpec((group, lines, fine), lambda i: (i, 0, 0)),
            pl.BlockSpec((group, lines, fine), lambda i: (i, 0, 0)),
        ],
        out_specs=pl.BlockSpec((group, pairs // 2, 2, fine), lambda i: (i, 0, 0, 0)),
        out_shape=jax.ShapeDtypeStruct((blocks, pairs // 2, 2, fine), jnp.float32),
        name="fine_part",
    )(slot, arrived, index, weight)


def column_kernel(source_ref, code_ref, index_ref, weight_ref):
    blocks, fine = source_ref.shape
    column = lax.broadcasted_iota(jnp.int32, (1, fine), 1)
    first = (column // LANES) * (LANES // 2) - LANES // 4
    for block in range(blocks):
        shape = index_ref.shape[1:]
        index_ref[block] = jnp.broadcast_to(source_ref[block : block + 1] - first, shape)
        weight_ref[block] = jnp.broadcast_to(
            code_ref[block : block + 1].astype(jnp.float32) * (1.0 / 16.0), shape
        )


def columns(source, code):
    blocks, fine = source.shape
    return pl.pallas_call(
        column_kernel,
        out_shape=[
            jax.ShapeDtypeStruct((blocks, 8, fine), jnp.int32),
            jax.ShapeDtypeStruct((blocks, 8, fine), jnp.float32),
        ],
        name="columns",
    )(source, code)


def per_device(
    members,
    control,
    hybrid_weight,
    member_weights,
    source_device,
    source_row,
    column_source,
    column_code,
):
    _, chans, row_count, width = members.shape
    spaces = lax.axis_size("space")
    space_index = lax.axis_index("space")
    member_slot = lax.axis_index("member")

    place = jnp.stack(
        [
            member_slot,
            jnp.where(space_index == 0, 0, jnp.where(space_index == spaces - 1, 2, 1)),
            (space_index < spaces - 1).astype(jnp.int32),
            space_index % 2,
        ]
    ).astype(jnp.int32)
    to_a, to_b = edge_rows(place, members, control, 4)
    halo_b = paired(to_b, "space", 1)
    halo_a = paired(to_a, "space", 0)

    blend = jnp.broadcast_to(hybrid_weight[:, None], (chans, LANES))
    source_index = source_device[:, 0]
    capacity = max(2, 2 * row_count // spaces)
    chosen = (source_index[:, None] == jnp.arange(spaces, dtype=jnp.int32)[None, :]).astype(
        jnp.int32
    )
    earlier = jnp.cumsum(chosen, axis=0) - chosen
    rank_within = jnp.sum(earlier * chosen, axis=1)
    slot_index = source_index * capacity + rank_within
    spread = slot_index[None, :] - capacity * jnp.arange(spaces, dtype=jnp.int32)[:, None]
    lane = jnp.arange(LANES, dtype=jnp.int32)
    taken = (spread[:, None, :] == lane[None, :, None]) & (lane < capacity)[None, :, None]
    request = jnp.sum(jnp.where(taken, source_row[None, None, :], 0), axis=2)[:, None, :]
    index, weight = columns(column_source, column_code)

    own_keep, own_give, near, control_near = own_part(
        place, member_weights, members, control, blend
    )
    own_give, request = lax.optimization_barrier((own_give, request))
    asked = lax.all_to_all(request, "space", split_axis=0, concat_axis=0, tiled=True)
    own_got = swapped(own_give, "member", 1)
    own_last = swapped(own_keep[1] + own_got[1], "member", 2)
    near, index, weight, slot_index = lax.optimization_barrier((near, index, weight, slot_index))

    keep, give = cross_part(place, member_weights, halo_a, halo_b, near, control_near, blend, 4)
    got = swapped(give, "member", 1)
    last = swapped(keep[1] + got[1], "member", 2)
    back_a, back_b = sent_rows(place, own_keep, own_got, own_last, keep, got, last)
    back_b = paired(back_b, "space", 1)
    back_a = paired(back_a, "space", 0)

    outgoing = answers(
        place, asked, capacity, own_keep, own_got, own_last, keep, got, last, back_a, back_b
    )
    pair_rows = outgoing.shape[1]
    arrived = lax.all_to_all(
        outgoing.reshape(spaces, capacity * pair_rows, width),
        "space",
        split_axis=0,
        concat_axis=0,
        tiled=True,
    ).reshape(spaces * capacity, pair_rows, width)
    return fine_part(slot_index, arrived, index, weight, 4)


def solution(mesh):
    placed = (
        P("member", None, "space", None),
        P(None, "space", None),
        P(),
        P(),
        P("space", None),
        P("space"),
        P("space", None),
        P("space", None),
    )

    return jax.shard_map(
        per_device,
        mesh=mesh,
        in_specs=placed,
        out_specs=P("space", "member", None, None),
        check_vma=False,
    )
```

```python
import functools

import jax
import jax.numpy as jnp
import numpy as np
from jax import lax
from jax.experimental import pallas as pl
from jax.experimental.pallas import tpu as pltpu
from jax.sharding import PartitionSpec as P

SCALE = 1.0 / 625.0
LANES = 128
PITCH = 24
LIMIT = 67043328


def paired(x, axis, first):
    length = lax.axis_size(axis)
    pairs = []
    for low in range(first, length - 1, 2):
        pairs += [(low, low + 1), (low + 1, low)]
    return lax.ppermute(x, axis, pairs)


def swapped(x, axis, bit):
    length = lax.axis_size(axis)
    return lax.ppermute(x, axis, [(i, i ^ bit) for i in range(length)])


def split_lanes(x):
    return [x[:, i : i + LANES] for i in range(0, x.shape[-1], LANES)]


def side_sum(parts, lane):
    ahead = [pltpu.roll(p, 1, 1) for p in parts]
    behind = [pltpu.roll(p, LANES - 1, 1) for p in parts]
    out = []
    for i in range(len(parts)):
        left = jnp.where(lane == 0, ahead[i - 1] if i else 0.0, ahead[i])
        right = jnp.where(
            lane == LANES - 1, behind[i + 1] if i + 1 < len(parts) else 0.0, behind[i]
        )
        out.append(left + right)
    return out


def inverse_total(weights_ref, rows):
    total = weights_ref[0]
    for i in range(1, weights_ref.shape[0]):
        total += weights_ref[i]
    return 1.0 / jnp.full((rows, LANES), total.astype(jnp.float32))


def plus(a, b):
    return [p + q for p, q in zip(a, b)]


def scaled(factor, a):
    return [factor * p for p in a]


def widen(parts, lane):
    return plus(parts, side_sum(parts, lane))


def edges_kernel(place_ref, members_ref, control_ref, a_ref, b_ref, scratch, stage, sems):
    step = pl.program_id(0)
    steps = pl.num_programs(0)
    group = members_ref.shape[0]
    chans, rows = members_ref.shape[1:3]
    parts = scratch.shape[0]
    odd = place_ref[3]

    def copies(first, count, index):
        return [
            pltpu.make_async_copy(
                stage.at[side, pl.ds(first, count)], ref.at[pl.ds(first, count)], sems.at[side, index]
            )
            for side, ref in enumerate((a_ref, b_ref))
        ]

    def rows_out(wide, index):
        for part in range(parts):
            lanes = slice(part * LANES, (part + 1) * LANES)
            for chan in range(chans):
                scratch[part, chan * PITCH : chan * PITCH + rows] = wide[chan, :, lanes]
            for slot in range(2):
                for which, side in ((slot, 1 - odd), (rows - 1 - slot, odd)):
                    stage[side, index, slot, :, lanes] = scratch[
                        part, pl.ds(which, chans, stride=PITCH), :
                    ]

    for one in range(group):
        rows_out(members_ref[one].astype(jnp.float32), step * group + one)
    for copy in copies(step * group, group, step):
        copy.start()

    @pl.when(step == steps - 1)
    def _():
        count = a_ref.shape[0] - 1
        rows_out(control_ref[...], count)
        for copy in copies(count, 1, count // group):
            copy.start()
        for index in range(count // group):
            for copy in copies(index * group, group, index):
                copy.wait()
        for copy in copies(count, 1, count // group):
            copy.wait()


def edge_rows(place, members, control, group):
    count, chans, rows, width = members.shape
    shape = (count + 1, 2, chans, width)
    out = jax.ShapeDtypeStruct(shape, jnp.float32)
    return pl.pallas_call(
        edges_kernel,
        grid=(count // group,),
        in_specs=[
            pl.BlockSpec(memory_space=pltpu.SMEM),
            pl.BlockSpec((group, chans, rows, width), lambda i: (i, 0, 0, 0)),
            pl.BlockSpec((chans, rows, width), lambda i: (0, 0, 0)),
        ],
        out_specs=[pl.BlockSpec(memory_space=pl.ANY)] * 2,
        out_shape=[out, out],
        scratch_shapes=[
            pltpu.VMEM((width // LANES, chans * PITCH, LANES), jnp.float32),
            pltpu.VMEM((2,) + shape, jnp.float32),
            pltpu.SemaphoreType.DMA((2, count // group + 1)),
        ],
        name="edge_rows",
    )(place, members, control)


def column_operators(width):
    q = np.eye(width) + np.eye(width, k=1) + np.eye(width, k=-1)
    q2 = q @ q
    q3 = q2 @ q
    eye = np.eye(width)
    return q2 @ q2 + 12 * q2 + 6 * eye, 4 * q3 + 12 * q, 6 * q2 + 4 * eye, 4 * q


def windowed(operator):
    first = operator[:256, :256]
    second = operator[128:, 128:].copy()
    second[:128, :128] = 0.0
    return first, second


def stacked(operators):
    first, second = zip(*[windowed(op) for op in operators])
    return np.stack([np.concatenate(first), np.concatenate(second)]).astype(jnp.bfloat16)


def own_kernel(
    place_ref, share_ref, members_ref, control_ref, blend_ref, operator_ref,
    keep_ref, give_ref, near_ref, control_near_ref,
    total, scratch, *work,
):
    step = pl.program_id(0)
    both, chans, rows, width = members_ref.shape
    parts = width // LANES
    last = pl.num_programs(0) - 1
    static = step == last
    fields, firsts, seconds, mixes = [work[i * both : (i + 1) * both] for i in range(4)]
    odd = place_ref[3]
    ends = [(4 * (1 - odd) + i, i) for i in range(4)]
    ends += [(4 * odd + i, rows - 1 - i) for i in range(4)]

    def lanes(part):
        return slice(part * LANES, (part + 1) * LANES)

    @pl.when(step == 0)
    def _():
        total[...] = jnp.zeros(total.shape, jnp.float32)
        for field in fields:
            field[...] = jnp.zeros(field.shape, jnp.float32)

    @pl.when(step < last)
    def _():
        for which, field in enumerate(fields):

            def fill(chan, carry):
                for part in range(parts):
                    state = members_ref[which, chan, :, lanes(part)].astype(jnp.float32)
                    field[part, chan, 8 : 8 + rows] = state * control_ref[chan, :, lanes(part)]
                    scratch[part, pl.ds(pl.multiple_of(chan * PITCH, 8), rows), :] = state
                return carry

            lax.fori_loop(0, chans, fill, 0, unroll=4)
            for place, row in ends:
                for part in range(parts):
                    near_ref[which, place, :, lanes(part)] = scratch[
                        part, pl.ds(row, chans, stride=PITCH), :
                    ].astype(jnp.bfloat16)

    @pl.when(static)
    def _():
        def fill(chan, carry):
            for part in range(parts):
                block = control_ref[chan, :, lanes(part)]
                for field in fields:
                    field[part, chan, 8 : 8 + rows] = block
                scratch[part, pl.ds(pl.multiple_of(chan * PITCH, 8), rows), :] = block
            return carry

        lax.fori_loop(0, chans, fill, 0, unroll=4)
        for place, row in ends:
            for part in range(parts):
                control_near_ref[place, :, lanes(part)] = scratch[
                    part, pl.ds(row, chans, stride=PITCH), :
                ]

    @pl.when(place_ref[1] == 0)
    def _():
        def image(chan, carry):
            for field in fields:
                for part in range(parts):
                    for row in range(3):
                        field[part, chan, 6 - row : 7 - row] = -field[
                            part, chan, 8 + row : 9 + row
                        ]
            return carry

        lax.fori_loop(0, chans, image, 0, unroll=4)

    @pl.when(place_ref[1] == 2)
    def _():
        def image(chan, carry):
            for field in fields:
                for part in range(parts):
                    for row in range(3):
                        field[part, chan, 9 + rows + row : 10 + rows + row] = -field[
                            part, chan, 7 + rows - row : 8 + rows - row
                        ]
            return carry

        lax.fori_loop(0, chans, image, 0, unroll=4)

    def at_distance(field, part, chan, distance):
        if distance == 0:
            return field[part, chan, 8 : 8 + rows]
        return (
            field[part, chan, 8 - distance : 8 - distance + rows]
            + field[part, chan, 8 + distance : 8 + distance + rows]
        )

    refine = jnp.where(static, 1.0, 0.0)

    def gather(which, chan):
        start = chan * rows
        at = pl.ds(start if isinstance(chan, int) else pl.multiple_of(start, rows), rows)
        for distance in range(4):
            base = distance * 2 * LANES
            for part in range(parts):
                value = at_distance(fields[which], part, chan, distance)
                if which:
                    value -= refine * value.astype(jnp.bfloat16).astype(jnp.float32)
                value = value.astype(jnp.bfloat16)
                if part < 2:
                    firsts[which][at, base + part * LANES : base + (part + 1) * LANES] = value
                if part > 0:
                    seconds[which][at, base + (part - 1) * LANES : base + part * LANES] = value

    inverse = inverse_total(share_ref, 1)

    def multiply(which):
        for window, ref in enumerate((firsts[which], seconds[which])):
            mixes[which][window] = jnp.dot(
                ref[...], operator_ref[window], preferred_element_type=jnp.float32
            )

    def collect(which, chan):
        at = pl.ds(chan * rows, rows)
        mixed = mixes[which]
        low = [mixed[0, at, lanes(0)], mixed[0, at, lanes(1)]]
        high = [mixed[1, at, lanes(0)], mixed[1, at, lanes(1)]]
        found = [low[0], low[1] + high[0], high[1]]
        blend = blend_ref[chan : chan + 1, :]
        member = jnp.minimum(step, last - 1) * both + which
        share = share_ref[place_ref[0] * (last * both) + member].astype(jnp.float32)
        factor = jnp.where(static, 0.25 * blend, share)
        for part in range(parts):
            far = at_distance(fields[which], part, chan, 4)
            value = found[part] + (far if which == 0 else (1.0 - refine) * far)
            state = members_ref[which, chan, :, lanes(part)].astype(jnp.float32)
            state = jnp.where(static, 1.0, state)
            before = total[chan, :, lanes(part)]
            if which == 0:
                before = jnp.where(static, (1.0 - blend) * inverse, 1.0) * before
            total[chan, :, lanes(part)] = before + (factor * state) * value

    def gather_four(group, carry):
        for inner in range(4):
            gather(0, group * 4 + inner)
        return carry

    lax.fori_loop(0, chans // 4, gather_four, 0)
    multiply(0)
    for chan in range(chans):
        gather(1, chan)
    multiply(1)
    for chan in range(chans):
        collect(0, chan)
    for chan in range(chans):
        collect(1, chan)

    @pl.when(static)
    def _():
        def one_group(group, carry):
            slot = jnp.bitwise_xor(group, place_ref[0])
            done = SCALE * total[pl.ds(pl.multiple_of(group * 8, 8), 8)]

            @pl.when(jnp.bitwise_and(slot, 1) == 0)
            def _():
                keep_ref[slot // 2] = done

            @pl.when(jnp.bitwise_and(slot, 1) == 1)
            def _():
                give_ref[slot // 2] = done

            return carry

        lax.fori_loop(0, chans // 8, one_group, 0)


def own_part(place, share, members, control, blend):
    count, chans, rows, width = members.shape
    parts = width // LANES
    both = 2
    steps = count // both
    operators = jnp.asarray(stacked(column_operators(width)))
    depth = operators.shape[1]
    half = (chans // 16, 8, rows, width)
    return pl.pallas_call(
        own_kernel,
        grid_spec=pltpu.PrefetchScalarGridSpec(
            num_scalar_prefetch=2,
            grid=(steps + 1,),
            in_specs=[
                pl.BlockSpec(
                    (both, chans, rows, width),
                    lambda i, place, share: (jnp.minimum(i, steps - 1), 0, 0, 0),
                ),
                pl.BlockSpec((chans, rows, width), lambda i, place, share: (0, 0, 0)),
                pl.BlockSpec((chans, LANES), lambda i, place, share: (0, 0)),
                pl.BlockSpec(operators.shape, lambda i, place, share: (0, 0, 0)),
            ],
            out_specs=[
                pl.BlockSpec(half, lambda i, place, share: (0, 0, 0, 0)),
                pl.BlockSpec(half, lambda i, place, share: (0, 0, 0, 0)),
                pl.BlockSpec(
                    (both, 8, chans, width),
                    lambda i, place, share: (jnp.minimum(i, steps - 1), 0, 0, 0),
                ),
                pl.BlockSpec((8, chans, width), lambda i, place, share: (0, 0, 0)),
            ],
            scratch_shapes=[
                pltpu.VMEM((chans, rows, width), jnp.float32),
                pltpu.VMEM((parts, chans * PITCH, LANES), jnp.float32),
            ]
            + [pltpu.VMEM((parts, chans, rows + 16, LANES), jnp.float32)] * both
            + [pltpu.VMEM((chans * rows, depth), jnp.bfloat16)] * (2 * both)
            + [pltpu.VMEM((2, chans * rows, 2 * LANES), jnp.float32)] * both,
        ),
        out_shape=[
            jax.ShapeDtypeStruct(half, jnp.float32),
            jax.ShapeDtypeStruct(half, jnp.float32),
            jax.ShapeDtypeStruct((count, 8, chans, width), jnp.bfloat16),
            jax.ShapeDtypeStruct((8, chans, width), jnp.float32),
        ],
        compiler_params=pltpu.CompilerParams(vmem_limit_bytes=LIMIT),
        name="own_part",
    )(place, share, members, control, blend, operators)


def cross_kernel(
    place_ref, share_ref, a_ref, a_control_ref, b_ref, b_control_ref,
    near_ref, control_ref, blend_ref, pair_ref, single_ref,
    keep_ref, give_ref, sums, first, second, third, fourth, mixed, alone,
):
    step = pl.program_id(0)
    group = near_ref.shape[0]
    chans, width = near_ref.shape[2:]
    parts = width // LANES
    lane = lax.broadcasted_iota(jnp.int32, (8, LANES), 1)
    final = step == pl.num_programs(0) - 1
    span = group * chans
    first_member = (place_ref[0] * pl.num_programs(0) + step) * group
    sides = (
        (a_ref, a_control_ref, (0, 1), (0, 1, 2, 3)),
        (b_ref, b_control_ref, (0, 1), (4, 5, 6, 7)),
    )

    def lanes(part, base=0):
        return slice(base + part * LANES, base + (part + 1) * LANES)

    for side, (halo, halo_control, order, own) in enumerate(sides):
        for one in range(group):
            share = share_ref[first_member + one].astype(jnp.float32)
            at = slice(side * span + one * chans, side * span + (one + 1) * chans)
            below = slice(2 * span + at.start, 2 * span + at.stop)
            for part in range(parts):
                y1, y2 = [
                    (
                        halo[one, slot, :, lanes(part)]
                        * (share * halo_control[0, slot, :, lanes(part)])
                    ).astype(jnp.bfloat16)
                    for slot in order
                ]
                y3 = (
                    near_ref[one, own[2], :, lanes(part)].astype(jnp.float32)
                    * (share * control_ref[own[2], :, lanes(part)])
                ).astype(jnp.bfloat16)
                if part < 2:
                    first[at, lanes(part)] = y1
                    first[at, lanes(part, 2 * LANES)] = y2
                    third[at, lanes(part)] = y1
                    third[below, lanes(part)] = y3
                if part > 0:
                    second[at, lanes(part - 1)] = y1
                    second[at, lanes(part - 1, 2 * LANES)] = y2
                    fourth[at, lanes(part - 1)] = y1
                    fourth[below, lanes(part - 1)] = y3
    mixed[0] = jnp.dot(first[...], pair_ref[0], preferred_element_type=jnp.float32)
    mixed[1] = jnp.dot(second[...], pair_ref[1], preferred_element_type=jnp.float32)
    alone[0] = jnp.dot(third[...], single_ref[0], preferred_element_type=jnp.float32)
    alone[1] = jnp.dot(fourth[...], single_ref[1], preferred_element_type=jnp.float32)

    def piece(ref, at, part, base):
        if part == 0:
            return ref[0, at, lanes(0, base)]
        if part == parts - 1:
            return ref[1, at, lanes(1, base)]
        return ref[0, at, lanes(1, base)] + ref[1, at, lanes(0, base)]

    def per_chans(eight, carry):
        here = pl.ds(pl.multiple_of(eight * 8, 8), 8)
        for side, (halo, halo_control, order, own) in enumerate(sides):
            for part in range(parts):
                totals = [None] * 6
                c = [
                    halo_control[0, order[0], here, lanes(part)],
                    halo_control[0, order[1], here, lanes(part)],
                    control_ref[own[2], here, lanes(part)],
                    control_ref[own[3], here, lanes(part)],
                ]
                for one in range(group):
                    share = share_ref[first_member + one].astype(jnp.float32)
                    start = side * span + one * chans + eight * 8
                    at = pl.ds(pl.multiple_of(start, 8), 8)
                    below = pl.ds(pl.multiple_of(2 * span + start, 8), 8)
                    b1 = halo[one, order[0], here, lanes(part)]
                    b2 = halo[one, order[1], here, lanes(part)]
                    a = [
                        near_ref[one, row, here, lanes(part)].astype(jnp.float32) for row in own
                    ]
                    y = [x * (share * k) for x, k in zip((b1, b2, a[2], a[3]), c)]
                    terms = (
                        a[0] * piece(mixed, at, part, 0),
                        a[1] * piece(mixed, at, part, 2 * LANES),
                        a[2] * (piece(alone, at, part, 0) + y[1]),
                        a[3] * y[0],
                        b1 * (piece(alone, below, part, 0) + y[3]),
                        b2 * y[2],
                    )
                    totals = [t if s is None else s + t for s, t in zip(totals, terms)]
                for i, value in enumerate(totals):
                    place = side * 6 + i
                    before = jnp.where(step == 0, 0.0, sums[place, here, lanes(part)])
                    sums[place, here, lanes(part)] = before + value
        return carry

    lax.fori_loop(0, chans // 8, per_chans, 0)

    def exact(y1, y2, y3, y4):
        wide = scaled(4.0, widen(y1, lane))
        inner = plus(widen(plus(wide, scaled(6.0, y2)), lane), scaled(12.0, y1))
        top = plus(widen(inner, lane), scaled(4.0, y2))
        next_row = plus(
            widen(plus(scaled(1.5, wide), scaled(4.0, y2)), lane), scaled(4.0, y1)
        )
        return top, next_row, plus(wide, y2), y1, plus(scaled(4.0, widen(y3, lane)), y4), y3

    @pl.when(final)
    def _():
        inverse = inverse_total(share_ref, 8)

        def finish(eight, carry):
            at = pl.ds(pl.multiple_of(eight * 8, 8), 8)
            slot = jnp.bitwise_xor(eight, place_ref[0])
            blend = blend_ref[at, :]
            for side, (halo, halo_control, order, own) in enumerate(sides):
                found = exact(
                    split_lanes(halo_control[0, order[0], at, :]),
                    split_lanes(halo_control[0, order[1], at, :]),
                    split_lanes(control_ref[own[2], at, :]),
                    split_lanes(control_ref[own[3], at, :]),
                )
                for i, value in enumerate(found):
                    place = side * 6 + i
                    for part in range(parts):
                        sums[place, at, lanes(part)] = SCALE * (
                            ((1.0 - blend) * inverse) * sums[place, at, lanes(part)]
                            + (0.25 * blend) * value[part]
                        )

            @pl.when(jnp.bitwise_and(slot, 1) == 0)
            def _():
                keep_ref[slot // 2] = sums[:, at, :]

            @pl.when(jnp.bitwise_and(slot, 1) == 1)
            def _():
                give_ref[slot // 2] = sums[:, at, :]

            return carry

        lax.fori_loop(0, chans // 8, finish, 0, unroll=2)


def cross_part(place, share, a, b, near, control_near, blend, group):
    count, rows, chans, width = near.shape
    halo = pl.BlockSpec((group, 2, chans, width), lambda i: (i, 0, 0, 0))
    halo_control = pl.BlockSpec((1, 2, chans, width), lambda i: (count, 0, 0, 0))
    half = (chans // 16, 12, 8, width)
    _, p1, p2, p3 = column_operators(width)
    left, right = stacked([p1, p2]), stacked([p2, p3])
    pair = jnp.asarray(np.concatenate([left, right], axis=2))
    single = jnp.asarray(stacked([p3]))
    span = 2 * group * chans
    return pl.pallas_call(
        cross_kernel,
        grid=(count // group,),
        in_specs=[
            pl.BlockSpec(memory_space=pltpu.SMEM),
            pl.BlockSpec(memory_space=pltpu.SMEM),
            halo,
            halo_control,
            halo,
            halo_control,
            pl.BlockSpec((group, rows, chans, width), lambda i: (i, 0, 0, 0)),
            pl.BlockSpec((rows, chans, width), lambda i: (0, 0, 0)),
            pl.BlockSpec((chans, LANES), lambda i: (0, 0)),
            pl.BlockSpec(pair.shape, lambda i: (0, 0, 0)),
            pl.BlockSpec(single.shape, lambda i: (0, 0, 0)),
        ],
        out_specs=[pl.BlockSpec(half, lambda i: (0, 0, 0, 0))] * 2,
        out_shape=[jax.ShapeDtypeStruct(half, jnp.float32)] * 2,
        scratch_shapes=[
            pltpu.VMEM((12, chans, width), jnp.float32),
            pltpu.VMEM((span, 4 * LANES), jnp.bfloat16),
            pltpu.VMEM((span, 4 * LANES), jnp.bfloat16),
            pltpu.VMEM((2 * span, 2 * LANES), jnp.bfloat16),
            pltpu.VMEM((2 * span, 2 * LANES), jnp.bfloat16),
            pltpu.VMEM((2, span, 4 * LANES), jnp.float32),
            pltpu.VMEM((2, 2 * span, 2 * LANES), jnp.float32),
        ],
        name="cross_part",
    )(place, share, a, a, b, b, near, control_near, blend, pair, single)


def sent_kernel(
    place_ref, own_ref, got_ref, last_ref, cross_ref, cross_got_ref, cross_last_ref, a_ref, b_ref, turned
):
    chans, _, width = last_ref.shape
    whole = own_ref[0] + got_ref[0] + last_ref[...]
    for part in range(width // LANES):
        lanes = slice(part * LANES, (part + 1) * LANES)
        for chan in range(chans):
            turned[chan * PITCH : chan * PITCH + 8] = whole[chan, :8, lanes]
        first = turned[pl.ds(0, chans, stride=PITCH), :]

        def crossed(i):
            return cross_ref[0, i, :, lanes] + cross_got_ref[0, i, :, lanes] + cross_last_ref[i, :, lanes]

        first += crossed(6 * (1 - place_ref[3]))
        for side, ref in enumerate((a_ref, b_ref)):
            for i in range(2):
                ref[i, :, lanes] = crossed(6 * side + 4 + i)
            ref[2, :, lanes] = first


def sent_rows(place, own, got, last, cross, cross_got, cross_last):
    chans, _, width = last.shape
    one = lambda x: pl.BlockSpec((1,) + x.shape[1:], lambda i: (0, 0, 0, 0))
    vmem = pl.BlockSpec(memory_space=pltpu.VMEM)
    return pl.pallas_call(
        sent_kernel,
        grid=(1,),
        in_specs=[
            pl.BlockSpec(memory_space=pltpu.SMEM),
            one(own), one(got), vmem, one(cross), one(cross_got), vmem,
        ],
        out_specs=[vmem, vmem],
        out_shape=[jax.ShapeDtypeStruct((3, chans, width), jnp.float32)] * 2,
        scratch_shapes=[pltpu.VMEM((chans * PITCH, LANES), jnp.float32)],
        name="sent_rows",
    )(place, own, got, last, cross, cross_got, cross_last)


def answer_kernel(
    place_ref, asked_ref, own_ref, got_ref, last_ref, cross_ref, cross_got_ref, cross_last_ref,
    a_ref, b_ref, out_ref, turned, pairs,
):
    chans, rows, width = last_ref.shape
    parts = width // LANES
    capacity = out_ref.shape[0] // asked_ref.shape[0]
    keep_high = (place_ref[2] != 0).astype(jnp.float32)
    odd = place_ref[3]
    whole = own_ref[0] + got_ref[0] + last_ref[...]
    for part in range(parts):
        for chan in range(chans):
            turned[part, chan * PITCH : chan * PITCH + rows] = whole[
                chan, :, part * LANES : (part + 1) * LANES
            ]

    def crossed(i, lanes):
        return cross_ref[0, i, :, lanes] + cross_got_ref[0, i, :, lanes] + cross_last_ref[i, :, lanes]

    def from_next(i, lanes):
        return jnp.where(odd == 0, a_ref[i, :, lanes], b_ref[i, :, lanes])

    def from_before(i, lanes):
        return jnp.where(odd == 0, b_ref[i, :, lanes], a_ref[i, :, lanes])

    for part in range(parts):
        lanes = slice(part * LANES, (part + 1) * LANES)
        for row in range(rows + 1):
            if row < rows:
                value = turned[part, pl.ds(row, chans, stride=PITCH), :]
            else:
                value = keep_high * (from_next(2, lanes) + crossed(6 * odd + 4, lanes))
            if row < 4:
                value += crossed(6 * (1 - odd) + row, lanes)
            if rows - 4 <= row < rows:
                value += crossed(6 * odd + rows - 1 - row, lanes)
            if row < 2:
                value += from_before(row, lanes)
            if rows - 2 <= row < rows:
                value += from_next(rows - 1 - row, lanes)
            if row < rows:
                pairs[part, pl.ds(row * 2 * chans, chans, stride=2), :] = value
            if row > 0:
                pairs[part, pl.ds((row - 1) * 2 * chans + 1, chans, stride=2), :] = value

    def one(device, carry):
        for slot in range(capacity):
            row = asked_ref[device, 0, slot]
            at = pl.ds(pl.multiple_of(row * (2 * chans), 2 * chans), 2 * chans)
            for part in range(parts):
                out_ref[device * capacity + slot, :, part * LANES : (part + 1) * LANES] = pairs[
                    part, at, :
                ]
        return carry

    lax.fori_loop(0, asked_ref.shape[0], one, 0, unroll=4)


def answers(place, asked, capacity, own, got, last, cross, cross_got, cross_last, a, b):
    chans, rows, width = last.shape
    slots = asked.shape[0] * capacity
    smem = pl.BlockSpec(memory_space=pltpu.SMEM)
    vmem = pl.BlockSpec(memory_space=pltpu.VMEM)
    one = lambda x: pl.BlockSpec((1,) + x.shape[1:], lambda i: (0, 0, 0, 0))
    return pl.pallas_call(
        answer_kernel,
        grid=(1,),
        in_specs=[smem, smem, one(own), one(got), vmem, one(cross), one(cross_got), vmem, vmem, vmem],
        out_specs=vmem,
        out_shape=jax.ShapeDtypeStruct((slots, 2 * chans, width), jnp.float32),
        scratch_shapes=[
            pltpu.VMEM((width // LANES, chans * PITCH, LANES), jnp.float32),
            pltpu.VMEM((width // LANES, rows * 2 * chans, LANES), jnp.float32),
        ],
        name="answers",
    )(place, asked, own, got, last, cross, cross_got, cross_last, a, b)


def fine_kernel(slot_ref, arrived_ref, index_ref, weight_ref, out_ref):
    blocks = index_ref.shape[0]
    pairs, _ = arrived_ref.shape[1:]
    fine = index_ref.shape[2]
    half = LANES // 2
    quarter = half // 2
    lane = lax.broadcasted_iota(jnp.int32, (8, LANES), 1)
    even = lax.broadcasted_iota(jnp.int32, (8, LANES), 0) % 2 == 0

    def one(block, carry):
        slot = slot_ref[pl.program_id(0) * blocks + block]
        windows = []
        for group in range(pairs // 8):
            parts = []
            for part in split_lanes(arrived_ref[slot, pl.ds(group * 8, 8), :]):
                other = jnp.where(even, pltpu.roll(part, 7, 0), pltpu.roll(part, 1, 0))
                parts.append(0.75 * part + 0.25 * other)
            turned = {
                shift: [pltpu.roll(p, shift, 1) for p in parts]
                for shift in (quarter, LANES - quarter)
            }
            found = []
            for chunk in range(fine // LANES):
                part, ahead = divmod(chunk * half - quarter, LANES)
                rolled = turned[LANES - ahead]
                if part < 0:
                    found.append(rolled[part + 1])
                elif part + 1 == len(parts):
                    found.append(rolled[part])
                else:
                    found.append(
                        jnp.where(lane < LANES - ahead, rolled[part], rolled[part + 1])
                    )
            windows.append(found)
        for chunk in range(fine // LANES):
            lanes = slice(chunk * LANES, (chunk + 1) * LANES)
            index = index_ref[block, :, lanes]
            weight = weight_ref[block, :, lanes]
            for group in range(pairs // 8):
                near = windows[group][chunk]
                left = jnp.take_along_axis(near, index, axis=1)
                right = jnp.take_along_axis(near, index + 1, axis=1)
                value = (1.0 - weight) * left + weight * right
                out_ref[block, group * 4 : (group + 1) * 4, :, lanes] = value.reshape(4, 2, LANES)
        return carry

    lax.fori_loop(0, blocks, one, 0, unroll=4)


def fine_part(slot, arrived, index, weight, group):
    blocks, lines, fine = index.shape
    slots, pairs, width = arrived.shape
    return pl.pallas_call(
        fine_kernel,
        grid=(blocks // group,),
        in_specs=[
            pl.BlockSpec(memory_space=pltpu.SMEM),
            pl.BlockSpec((slots, pairs, width), lambda i: (0, 0, 0)),
            pl.BlockSpec((group, lines, fine), lambda i: (i, 0, 0)),
            pl.BlockSpec((group, lines, fine), lambda i: (i, 0, 0)),
        ],
        out_specs=pl.BlockSpec((group, pairs // 2, 2, fine), lambda i: (i, 0, 0, 0)),
        out_shape=jax.ShapeDtypeStruct((blocks, pairs // 2, 2, fine), jnp.float32),
        name="fine_part",
    )(slot, arrived, index, weight)


def request_kernel(device_ref, row_ref, slot_ref, request_ref, *, capacity):
    blocks = device_ref.shape[0]
    lane = lax.broadcasted_iota(jnp.int32, (1, LANES), 1)
    request_ref[...] = jnp.zeros(request_ref.shape, jnp.int32)
    for block in range(blocks):
        device = device_ref[block]
        rank = jnp.int32(0)
        for earlier in range(block):
            rank += (device_ref[earlier] == device).astype(jnp.int32)
        slot_ref[block] = device * capacity + rank
        request_ref[device] = jnp.where(lane == rank, row_ref[block], request_ref[device])


def requests(device, row, spaces, capacity):
    smem = pl.BlockSpec(memory_space=pltpu.SMEM)
    return pl.pallas_call(
        functools.partial(request_kernel, capacity=capacity),
        in_specs=[smem, smem],
        out_specs=[smem, pl.BlockSpec(memory_space=pltpu.VMEM)],
        out_shape=[
            jax.ShapeDtypeStruct(device.shape, jnp.int32),
            jax.ShapeDtypeStruct((spaces, 1, LANES), jnp.int32),
        ],
        name="requests",
    )(device, row)


def column_kernel(source_ref, code_ref, index_ref, weight_ref):
    blocks, fine = source_ref.shape
    column = lax.broadcasted_iota(jnp.int32, (1, fine), 1)
    first = (column // LANES) * (LANES // 2) - LANES // 4
    for block in range(blocks):
        shape = index_ref.shape[1:]
        index_ref[block] = jnp.broadcast_to(source_ref[block : block + 1] - first, shape)
        weight_ref[block] = jnp.broadcast_to(
            code_ref[block : block + 1].astype(jnp.float32) * (1.0 / 16.0), shape
        )


def columns(source, code):
    blocks, fine = source.shape
    return pl.pallas_call(
        column_kernel,
        out_shape=[
            jax.ShapeDtypeStruct((blocks, 8, fine), jnp.int32),
            jax.ShapeDtypeStruct((blocks, 8, fine), jnp.float32),
        ],
        name="columns",
    )(source, code)


def per_device(
    members,
    control,
    hybrid_weight,
    member_weights,
    source_device,
    source_row,
    column_source,
    column_code,
):
    _, chans, row_count, width = members.shape
    spaces = lax.axis_size("space")
    space_index = lax.axis_index("space")
    member_slot = lax.axis_index("member")

    place = jnp.stack(
        [
            member_slot,
            jnp.where(space_index == 0, 0, jnp.where(space_index == spaces - 1, 2, 1)),
            (space_index < spaces - 1).astype(jnp.int32),
            space_index % 2,
        ]
    ).astype(jnp.int32)
    to_a, to_b = edge_rows(place, members, control, 2)
    halo_b = paired(to_b, "space", 1)
    halo_a = paired(to_a, "space", 0)

    blend = jnp.broadcast_to(hybrid_weight[:, None], (chans, LANES))
    source_index = source_device[:, 0]
    capacity = max(2, 2 * row_count // spaces)
    slot_index, request = requests(source_index, source_row, spaces, capacity)
    index, weight = columns(column_source, column_code)

    own_keep, own_give, near, control_near = own_part(
        place, member_weights, members, control, blend
    )
    own_give, request = lax.optimization_barrier((own_give, request))
    asked = lax.all_to_all(request, "space", split_axis=0, concat_axis=0, tiled=True)
    own_got = swapped(own_give, "member", 1)
    own_last = swapped(own_keep[1] + own_got[1], "member", 2)
    near, index, weight, slot_index = lax.optimization_barrier((near, index, weight, slot_index))

    keep, give = cross_part(place, member_weights, halo_a, halo_b, near, control_near, blend, 4)
    got = swapped(give, "member", 1)
    last = swapped(keep[1] + got[1], "member", 2)
    back_a, back_b = sent_rows(place, own_keep, own_got, own_last, keep, got, last)
    back_b = paired(back_b, "space", 1)
    back_a = paired(back_a, "space", 0)

    outgoing = answers(
        place, asked, capacity, own_keep, own_got, own_last, keep, got, last, back_a, back_b
    )
    pair_rows = outgoing.shape[1]
    arrived = lax.all_to_all(
        outgoing.reshape(spaces, capacity * pair_rows, width),
        "space",
        split_axis=0,
        concat_axis=0,
        tiled=True,
    ).reshape(spaces * capacity, pair_rows, width)
    return fine_part(slot_index, arrived, index, weight, 16)


def solution(mesh):
    placed = (
        P("member", None, "space", None),
        P(None, "space", None),
        P(),
        P(),
        P("space", None),
        P("space"),
        P("space", None),
        P("space", None),
    )

    return jax.shard_map(
        per_device,
        mesh=mesh,
        in_specs=placed,
        out_specs=P("space", "member", None, None),
        check_vma=False,
    )
```
